8 devices in a mesh: dp: 1 (over z), tp: 2 (over y), ep: 4 (over x, core).
Axes of the slice: x: 2, y: 2, z: 1, core: 2. Of those that a mesh axis runs over, the one named last changes fastest.
Arguments:
- tokens: bfloat16 [1024, 1024], P(('dp', 'ep'))
- grad_out: bfloat16 [1024, 1024], P(('dp', 'ep'))
- w_router: bfloat16 [1024, 8], replicated
- w_in: bfloat16 [8, 1024, 4096], P('ep', None, 'tp')
- w_out: bfloat16 [8, 4096, 1024], P('ep', 'tp')
- expert_ids: int32 [1024], P(('dp', 'ep'))
Outputs:
- output 1: bfloat16 [1024, 1024], P(('dp', 'ep'))
- output 2: bfloat16 [1024, 1024], P(('dp', 'ep'))
- output 3: float32 [8, 1024, 4096], P(('dp', 'ep'), None, 'tp')
- output 4: float32 [8, 4096, 1024], P(('dp', 'ep'), 'tp')
- output 5: float32 [1024, 8], P('dp')
All inputs are finite; a program needn't handle non-finite values.
Results may differ from the reference program's by a relative error of at most 0.00633399.
Values are sent between devices in bfloat16 or wider.
A program may use at most 1 GiB of HBM per device.

```python
import jax
import jax.numpy as jnp
from jax import lax

D_MODEL = 1024
D_FF = 4096
EXPERTS = 8
TOKENS_DEV = 256
EP_RANKS = 4

CAPACITY = (6 * TOKENS_DEV + 5 * EXPERTS - 1) // (5 * EXPERTS)
N_TOKENS = EP_RANKS * TOKENS_DEV
N_SLOTS = EXPERTS * CAPACITY


def draw_routes(route_key):
    key_hot, key_order, key_rest = jax.random.split(route_key, 3)
    hot_expert = jax.random.randint(key_hot, (EP_RANKS, 1), 0, EXPERTS)
    rest_ids = jax.random.randint(key_rest, (EP_RANKS, TOKENS_DEV), 0, EXPERTS)
    order_keys = jax.random.split(key_order, EP_RANKS)
    rank_of = jax.vmap(lambda one_key: jax.random.permutation(one_key, TOKENS_DEV))(order_keys)
    hot_count = CAPACITY + CAPACITY // 2 + 1
    cover_ids = (rank_of - hot_count) % EXPERTS
    route_ids = jnp.where(rank_of < hot_count, hot_expert, jnp.where(rank_of < hot_count + EXPERTS, cover_ids, rest_ids))
    return route_ids.reshape(N_TOKENS).astype(jnp.int32)


def setup_inputs(seed: int = 0, part: int = 0) -> dict:
    part_key = jax.random.fold_in(jax.random.key(seed), part)
    rand_keys = jax.random.split(part_key, 3)
    weight_keys = jax.random.split(jax.random.key(seed + 1), 3)
    tokens = jax.random.normal(rand_keys[0], (N_TOKENS, D_MODEL), jnp.float32)
    grad_out = jax.random.normal(rand_keys[1], (N_TOKENS, D_MODEL), jnp.float32)
    w_router = jax.random.normal(weight_keys[0], (D_MODEL, EXPERTS), jnp.float32) * D_MODEL ** -0.5
    w_in = jax.random.normal(weight_keys[1], (EXPERTS, D_MODEL, D_FF), jnp.float32) * D_MODEL ** -0.5
    w_out = jax.random.normal(weight_keys[2], (EXPERTS, D_FF, D_MODEL), jnp.float32) * D_FF ** -0.5
    return {
        "tokens": tokens.astype(jnp.bfloat16),
        "grad_out": grad_out.astype(jnp.bfloat16),
        "w_router": w_router.astype(jnp.bfloat16),
        "w_in": w_in.astype(jnp.bfloat16),
        "w_out": w_out.astype(jnp.bfloat16),
        "expert_ids": draw_routes(rand_keys[2]),
    }


def dispatch(rows, slot_index):
    slot_buf = jnp.zeros((N_SLOTS + 1, D_MODEL), rows.dtype).at[slot_index].set(rows)
    return slot_buf[:N_SLOTS]


def combine(slot_buf, slot_index):
    padded = jnp.concatenate([slot_buf, jnp.zeros((1, D_MODEL), slot_buf.dtype)], axis=0)
    return jnp.take(padded, slot_index, axis=0)


def by_expert(source_bufs):
    return source_bufs.reshape(EP_RANKS, EXPERTS, CAPACITY, D_MODEL).transpose(1, 0, 2, 3).reshape(EXPERTS, EP_RANKS * CAPACITY, D_MODEL)


def by_source(expert_bufs):
    return expert_bufs.reshape(EXPERTS, EP_RANKS, CAPACITY, D_MODEL).transpose(1, 0, 2, 3).reshape(EP_RANKS, N_SLOTS, D_MODEL)


def expert_step(operands):
    slot_rows, dy_rows, w_in_e, w_out_e = operands
    pre_act = jnp.dot(slot_rows, w_in_e, preferred_element_type=jnp.float32)
    act_val, act_vjp = jax.vjp(jax.nn.gelu, pre_act)
    hidden = act_val.astype(jnp.bfloat16)
    y_rows = jnp.dot(hidden, w_out_e, preferred_element_type=jnp.float32).astype(jnp.bfloat16)
    d_hidden = jnp.dot(dy_rows, w_out_e.T, preferred_element_type=jnp.float32)
    d_pre = act_vjp(d_hidden)[0].astype(jnp.bfloat16)
    grad_out_e = jnp.dot(hidden.T, dy_rows, preferred_element_type=jnp.float32)
    grad_in_e = jnp.dot(slot_rows.T, d_pre, preferred_element_type=jnp.float32)
    d_slot = jnp.dot(d_pre, w_in_e.T, preferred_element_type=jnp.float32).astype(jnp.bfloat16)
    return y_rows, d_slot, grad_in_e, grad_out_e


def reference(tokens, grad_out, w_router, w_in, w_out, expert_ids):
    route_ids = expert_ids.reshape(EP_RANKS, TOKENS_DEV)
    one_hot = (route_ids[:, :, None] == jnp.arange(EXPERTS)[None, None, :]).astype(jnp.int32)
    position = jnp.sum(jnp.cumsum(one_hot, axis=1) * one_hot, axis=2) - 1
    slot_index = jnp.where(position < CAPACITY, route_ids * CAPACITY + position, N_SLOTS)
    chosen = expert_ids[:, None] == jnp.arange(EXPERTS)[None, :]
    logits = jnp.dot(tokens, w_router, preferred_element_type=jnp.float32)
    router_prob = jax.nn.softmax(logits, axis=-1)
    gate_prob = jnp.sum(jnp.where(chosen, router_prob, 0.0), axis=1)
    dy_tok = (gate_prob[:, None] * grad_out.astype(jnp.float32)).astype(jnp.bfloat16)
    slot_rows = jax.vmap(dispatch)(tokens.reshape(EP_RANKS, TOKENS_DEV, D_MODEL), slot_index)
    dy_rows = jax.vmap(dispatch)(dy_tok.reshape(EP_RANKS, TOKENS_DEV, D_MODEL), slot_index)
    y_rows, d_slot, grad_w_in, grad_w_out = lax.map(expert_step, (by_expert(slot_rows), by_expert(dy_rows), w_in, w_out))
    y_tok = jax.vmap(combine)(by_source(y_rows), slot_index).reshape(N_TOKENS, D_MODEL)
    dx_moe = jax.vmap(combine)(by_source(d_slot), slot_index).reshape(N_TOKENS, D_MODEL)
    moe_out = (gate_prob[:, None] * y_tok.astype(jnp.float32)).astype(jnp.bfloat16)
    d_gate = jnp.sum(grad_out.astype(jnp.float32) * y_tok.astype(jnp.float32), axis=1)
    d_logits = (d_gate[:, None] * router_prob * (chosen.astype(jnp.float32) - gate_prob[:, None])).astype(jnp.bfloat16)
    router_grad = jnp.dot(d_logits, w_router.T, preferred_element_type=jnp.float32)
    grad_tokens = (dx_moe.astype(jnp.float32) + router_grad).astype(jnp.bfloat16)
    grad_w_router = jnp.dot(tokens.T, d_logits, preferred_element_type=jnp.float32)
    return moe_out, grad_tokens, grad_w_in, grad_w_out, grad_w_router
```

```python
import jax
import jax.numpy as jnp
from jax import lax
from jax.experimental import pallas as pl
from jax.experimental.pallas import tpu as pltpu
from jax.sharding import PartitionSpec as P

MESH = pl.DeviceIdType.MESH
F32, BF16 = jnp.float32, jnp.bfloat16
CONTRACT_LAST = (((1,), (1,)), ((), ()))
CONTRACT_FIRST = (((0,), (0,)), ((), ()))
GELU_C = 0.7978845608028654
GELU_K = 0.044715


def mm(a, b, dims=(((1,), (0,)), ((), ()))):
    return lax.dot_general(a, b, dims, preferred_element_type=F32)


def ep_partners():
    ep = lax.axis_index("ep")
    cx, cc = ep // 2, ep % 2
    return [ep, 2 * cx + (1 - cc), 2 * (1 - cx) + cc, 2 * (1 - cx) + (1 - cc)]


def route(idx_row, capacity, n_experts, stride):
    n = idx_row.shape[1]
    expert = lax.broadcasted_iota(jnp.int32, (n_experts, n), 0)
    hot = jnp.where(expert == idx_row, 1.0, 0.0)
    earlier = lax.broadcasted_iota(jnp.int32, (n, n), 0)
    later = lax.broadcasted_iota(jnp.int32, (n, n), 1)
    upto = jnp.where(earlier <= later, 1.0, 0.0).astype(BF16)
    count = mm(hot.astype(BF16), upto)
    position = jnp.sum(hot * count, axis=0, keepdims=True) - 1.0
    slot = jnp.where(position < capacity, idx_row.astype(F32) * stride + position, -1.0)
    return hot, slot


def pick(slot, first, rows):
    n = slot.shape[1]
    row = (lax.broadcasted_iota(jnp.int32, (rows, n), 0) + first).astype(F32)
    return jnp.where(row == slot, 1.0, 0.0).astype(BF16)


def gate_of(x, wgt, hot):
    n_experts = hot.shape[0]
    logits = mm(x, wgt, CONTRACT_LAST)
    e = jnp.exp(logits - jnp.max(logits, axis=1, keepdims=True))
    prob = e / jnp.sum(e, axis=1, keepdims=True)
    eye = jnp.where(
        lax.broadcasted_iota(jnp.int32, (n_experts, n_experts), 0)
        == lax.broadcasted_iota(jnp.int32, (n_experts, n_experts), 1), 1.0, 0.0)
    chosen = mm(hot.astype(BF16), eye.astype(BF16), CONTRACT_FIRST)
    gate = jnp.sum(chosen * prob, axis=1, keepdims=True)
    return prob, chosen, gate


def enter(peers, tp_peer):
    barrier = pltpu.get_barrier_semaphore()
    for r in (1, 2, 3):
        pl.semaphore_signal(barrier, inc=1, device_id={"ep": peers[r]}, device_id_type=MESH)
    pl.semaphore_signal(barrier, inc=1, device_id={"tp": tp_peer}, device_id_type=MESH)
    return barrier


def send(src, dst, ssem, rsem, device):
    copy = pltpu.make_async_remote_copy(
        src_ref=src, dst_ref=dst, send_sem=ssem, recv_sem=rsem, device_id=device, device_id_type=MESH)
    copy.start()
    return copy


def pair(lo, hi, e, cap):
    a = lo.astype(F32)[e * cap:(e + 1) * cap]
    b = hi.astype(F32)[e * cap:(e + 1) * cap]
    return jnp.concatenate([a, b], axis=0).astype(BF16)


def make_front(n_experts, capacity, cap):
    blk = 2 * cap

    def front(x_ref, gy_ref, wgt_ref, idx_ref, wi_hbm, wo_hbm,
              h_ref, da_ref, xs_ref, dys_ref, speer_ref, sown_ref, yr_ref,
              wi, wo, xsend, dysend, xrecv, dyrecv, gp, ypeer, yown, yrecv, yback, yland,
              wsem, x_s, x_r, d_s, d_r, y_s, y_r, b_s, b_r):
        tp = lax.axis_index("tp")
        tp_peer = 1 - tp
        peers = ep_partners()
        half = x_ref.shape[1] // 2
        d_ff = wi.shape[2]
        loads = {}
        for e in range(2):
            loads["i", e] = pltpu.make_async_copy(wi_hbm.at[e], wi.at[e], wsem.at[0, e])
            loads["o", e] = pltpu.make_async_copy(wo_hbm.at[e], wo.at[e], wsem.at[1, e])
        for e in range(2):
            loads["i", e].start()
            loads["o", e].start()
        barrier = enter(peers, tp_peer)

        x = x_ref[...]
        hot, slot = route(idx_ref[...], capacity, n_experts, cap)
        picks = [pick(slot, peers[r] * blk, blk) for r in range(4)]
        for r in (2, 3, 1, 0):
            xsend[r] = mm(picks[r], x).astype(BF16)
        pl.semaphore_wait(barrier, 4)
        sends = []
        xc, dc = {}, {}
        for r in (2, 3, 1):
            xc[r] = send(xsend.at[r], xrecv.at[r - 1], x_s.at[r - 1], x_r.at[r - 1], {"ep": peers[r]})
        _, _, gate = gate_of(x, wgt_ref[...], hot)
        dy = (gate * gy_ref[...].astype(F32)).astype(BF16)
        for r in (2, 3, 1, 0):
            dysend[r] = mm(picks[r], dy).astype(BF16)
            if r:
                dc[r] = send(dysend.at[r], dyrecv.at[r - 1], d_s.at[r - 1], d_r.at[r - 1], {"ep": peers[r]})

        yc = {}

        def forward(g):
            rows = slice(g * blk, (g + 1) * blk)
            for e in range(2):
                lo = xsend[0] if g == 0 else xrecv[1]
                hi = xrecv[0] if g == 0 else xrecv[2]
                xs_ref[e, rows, :] = pair(lo, hi, e, cap)
            for e in range(2):
                if g == 0:
                    loads["i", e].wait()
                xg = xs_ref[e, rows, :]
                step = d_ff // 2
                for c in range(2):
                    cols = slice(c * step, (c + 1) * step)
                    a = mm(xg, wi[e, :, cols])
                    t = jnp.tanh(GELU_C * (a + GELU_K * (a * a * a)))
                    cdf = 0.5 * (1.0 + t)
                    h_ref[e, rows, cols] = (a * cdf).astype(BF16)
                    gp[e, rows, cols] = cdf + (0.5 * a) * (1.0 - t * t) * (GELU_C + (3.0 * GELU_C * GELU_K) * (a * a))
                if g == 0:
                    loads["o", e].wait()
                hg = h_ref[e, rows, :]
                ypeer[g, e] = mm(hg, wo[e, :, pl.ds(pl.multiple_of(tp_peer * half, half), half)])
                yc[g, e] = send(ypeer.at[g, e], yrecv.at[g, e], y_s.at[g, e], y_r.at[g, e], {"tp": tp_peer})
                yown[g, e] = mm(hg, wo[e, :, pl.ds(pl.multiple_of(tp * half, half), half)])

        def backward(e):
            for g in range(2):
                lo = dysend[0] if g == 0 else dyrecv[1]
                hi = dyrecv[0] if g == 0 else dyrecv[2]
                dys_ref[e, g * blk:(g + 1) * blk, :] = pair(lo, hi, e, cap)
            dyg = dys_ref[e]
            step = d_ff // 4
            for c in range(4):
                cols = slice(c * step, (c + 1) * step)
                dh = mm(dyg, wo[e, cols, :], CONTRACT_LAST)
                da_ref[e, :, cols] = (dh * gp[e, :, cols]).astype(BF16)
            dag = da_ref[e]
            speer_ref[e] = mm(dag, wi[e, pl.ds(pl.multiple_of(tp_peer * half, half), half), :], CONTRACT_LAST)
            sown_ref[e] = mm(dag, wi[e, pl.ds(pl.multiple_of(tp * half, half), half), :], CONTRACT_LAST)

        bc = {}

        def give_back(g):
            for e in range(2):
                yc[g, e].wait()
            both = [yown[g, e] + yrecv[g, e] for e in range(2)]
            for q in range(2):
                r = 2 * g + q
                block = jnp.concatenate([both[e][q * cap:(q + 1) * cap] for e in range(2)], axis=0).astype(BF16)
                if r == 0:
                    yr_ref[0] = block
                else:
                    yback[r - 1] = block
                    bc[r] = send(yback.at[r - 1], yland.at[r - 1], b_s.at[r - 1], b_r.at[r - 1], {"ep": peers[r]})

        xc[1].wait()
        forward(0)
        xc[2].wait()
        xc[3].wait()
        forward(1)
        for r in (1, 2, 3):
            dc[r].wait()
        backward(0)
        give_back(0)
        backward(1)
        give_back(1)
        for r in (1, 2, 3):
            bc[r].wait()
            yr_ref[r] = yland[r - 1]

    return front


def grads_kernel(h_ref, dys_ref, xs_ref, da_ref, dwi_ref, dwo_ref):
    dwo_ref[0] = mm(h_ref[0], dys_ref[0], CONTRACT_FIRST)
    dwi_ref[0] = mm(xs_ref[0], da_ref[0], CONTRACT_FIRST)


def make_back(n_experts, capacity, cap):
    blk = 2 * cap

    def back(x_ref, gy_ref, wgt_ref, idx_ref, yr_ref, sown_ref, srecv_ref,
             out_ref, dx_ref, dwgt_ref,
             ysend, yland, sback, sland, dxsend, dxland, dwg,
             y_s, y_r, b_s, b_r, x_s, x_r, w_s, w_r):
        tp = lax.axis_index("tp")
        ep = lax.axis_index("ep")
        tp_peer = 1 - tp
        peers = ep_partners()
        half = x_ref.shape[1] // 2
        mine = pl.ds(pl.multiple_of(tp * half, half), half)
        theirs = pl.ds(pl.multiple_of(tp_peer * half, half), half)
        barrier = enter(peers, tp_peer)
        hot, slot = route(idx_ref[...], capacity, n_experts, cap)
        picks = jnp.concatenate([pick(slot, peers[r] * blk, blk) for r in range(4)], axis=0)
        ysend[...] = mm(picks, yr_ref[...], CONTRACT_FIRST).astype(BF16)
        pl.semaphore_wait(barrier, 4)
        yc = send(ysend, yland, y_s, y_r, {"tp": tp_peer})

        bc = {}
        for g in (1, 0):
            rows = slice(g * blk, (g + 1) * blk)
            both = [sown_ref[e, rows, :] + srecv_ref[e, rows, :] for e in range(2)]
            for q in range(2):
                r = 2 * g + q
                block = jnp.concatenate([both[e][q * cap:(q + 1) * cap] for e in range(2)], axis=0).astype(BF16)
                if r == 0:
                    sland[0:blk, :] = block
                else:
                    sback[r - 1] = block
                    bc[r] = send(sback.at[r - 1], sland.at[r * blk:(r + 1) * blk, :], b_s.at[r - 1], b_r.at[r - 1],
                                 {"ep": peers[r]})

        x = x_ref[...]
        prob, chosen, gate = gate_of(x, wgt_ref[...], hot)
        y_mine = ysend[...].astype(F32)
        out_ref[:, mine] = (gate * y_mine).astype(BF16)
        dgate = jnp.sum(gy_ref[:, mine].astype(F32) * y_mine, axis=1, keepdims=True)
        yc.wait()
        y_theirs = yland[...].astype(F32)
        out_ref[:, theirs] = (gate * y_theirs).astype(BF16)
        dgate = dgate + jnp.sum(gy_ref[:, theirs].astype(F32) * y_theirs, axis=1, keepdims=True)
        dlogits = (dgate * prob * (chosen - gate)).astype(BF16)
        dwg[ep] = mm(dlogits, x, CONTRACT_FIRST)
        wc = {}
        for r in (2, 3, 1):
            wc[r] = send(dwg.at[ep], dwg.at[ep], w_s.at[r - 1], w_r.at[r - 1], {"ep": peers[r]})
        rgrad = mm(dlogits, wgt_ref[:, mine])
        for r in (1, 2, 3):
            bc[r].wait()
        s_tok = mm(picks, sland[...], CONTRACT_FIRST).astype(BF16).astype(F32)
        dx_mine = (s_tok + rgrad).astype(BF16)
        dxsend[...] = dx_mine
        xc = send(dxsend, dxland, x_s, x_r, {"tp": tp_peer})
        dx_ref[:, mine] = dx_mine
        for r in (1, 2, 3):
            wc[r].wait()
        dwgt_ref[...] = (dwg[0] + dwg[1]) + (dwg[2] + dwg[3])
        xc.wait()
        dx_ref[:, theirs] = dxland[...]

    return back


def solution(mesh):
    row_spec = P(("dp", "ep"), None)
    vmem = pl.BlockSpec(memory_space=pltpu.VMEM)
    hbm = pl.BlockSpec(memory_space=pl.ANY)

    def local_block(tokens, grad_out, w_router, w_in, w_out, expert_ids):
        n, d_model = tokens.shape
        n_experts = w_router.shape[1]
        le, _, d_ff = w_in.shape
        capacity = (6 * n + 5 * n_experts - 1) // (5 * n_experts)
        cap = -(-capacity // 8) * 8
        blk = le * cap
        rows = 4 * cap
        half = d_model // 2
        wgt = w_router.T
        idx_row = expert_ids.reshape(1, n)
        sds = jax.ShapeDtypeStruct
        dma = pltpu.SemaphoreType.DMA

        h, da, xs, dys, speer, sown, yr = pl.pallas_call(
            make_front(n_experts, capacity, cap),
            out_shape=(sds((le, rows, d_ff), BF16), sds((le, rows, d_ff), BF16), sds((le, rows, d_model), BF16),
                       sds((le, rows, d_model), BF16), sds((le, rows, half), F32), sds((le, rows, half), F32),
                       sds((4, blk, half), BF16)),
            in_specs=[vmem, vmem, vmem, vmem, hbm, hbm],
            out_specs=(vmem,) * 7,
            scratch_shapes=[
                pltpu.VMEM((le, d_model, d_ff), BF16), pltpu.VMEM((le, d_ff, d_model), BF16),
                pltpu.VMEM((4, blk, d_model), BF16), pltpu.VMEM((4, blk, d_model), BF16),
                pltpu.VMEM((3, blk, d_model), BF16), pltpu.VMEM((3, blk, d_model), BF16),
                pltpu.VMEM((le, rows, d_ff), F32),
                pltpu.VMEM((2, le, blk, half), F32), pltpu.VMEM((2, le, blk, half), F32), pltpu.VMEM((2, le, blk, half), F32),
                pltpu.VMEM((3, blk, half), BF16), pltpu.VMEM((3, blk, half), BF16),
                dma((2, le)), dma((3,)), dma((3,)), dma((3,)), dma((3,)), dma((2, le)), dma((2, le)), dma((3,)), dma((3,)),
            ],
            compiler_params=pltpu.CompilerParams(collective_id=0, has_side_effects=True, vmem_limit_bytes=48 * 2**20),
            name="front",
        )(tokens, grad_out, wgt, idx_row, w_in, w_out)

        srecv = lax.ppermute(speer, "tp", [(0, 1), (1, 0)])

        steps = 4
        hs, ms = d_ff // steps, d_model // steps
        dwi, dwo = pl.pallas_call(
            grads_kernel,
            grid=(le, steps),
            out_shape=(sds((le, d_model, d_ff), F32), sds((le, d_ff, d_model), F32)),
            in_specs=[pl.BlockSpec((1, rows, hs), lambda e, c: (e, 0, c)), pl.BlockSpec((1, rows, d_model), lambda e, c: (e, 0, 0)),
                      pl.BlockSpec((1, rows, ms), lambda e, c: (e, 0, c)), pl.BlockSpec((1, rows, d_ff), lambda e, c: (e, 0, 0))],
            out_specs=(pl.BlockSpec((1, ms, d_ff), lambda e, c: (e, c, 0)), pl.BlockSpec((1, hs, d_model), lambda e, c: (e, c, 0))),
            cost_estimate=pl.CostEstimate(flops=4 * le * rows * d_model * d_ff, bytes_accessed=8 * le * d_model * d_ff,
                                          transcendentals=0),
            compiler_params=pltpu.CompilerParams(vmem_limit_bytes=24 * 2**20),
            name="weight_grads",
        )(h, dys, xs, da)

        out, dx, dwgt = pl.pallas_call(
            make_back(n_experts, capacity, cap),
            out_shape=(sds((n, d_model), BF16), sds((n, d_model), BF16), sds((n_experts, d_model), F32)),
            in_specs=[vmem] * 7,
            out_specs=(vmem,) * 3,
            scratch_shapes=[
                pltpu.VMEM((n, half), BF16), pltpu.VMEM((n, half), BF16),
                pltpu.VMEM((3, blk, half), BF16), pltpu.VMEM((4 * blk, half), BF16),
                pltpu.VMEM((n, half), BF16), pltpu.VMEM((n, half), BF16),
                pltpu.VMEM((4, n_experts, d_model), F32),
                dma, dma, dma((3,)), dma((3,)), dma, dma, dma((3,)), dma((3,)),
            ],
            compiler_params=pltpu.CompilerParams(collective_id=1, has_side_effects=True, vmem_limit_bytes=24 * 2**20),
            name="back",
        )(tokens, grad_out, wgt, idx_row, yr.reshape(4 * blk, half), sown, srecv)
        return out, dx, dwi, dwo, dwgt.T

    in_specs = (row_spec, row_spec, P(None, None), P("ep", None, "tp"), P("ep", "tp", None), P(("dp", "ep")))
    out_specs = (row_spec, row_spec, P(("dp", "ep"), None, "tp"), P(("dp", "ep"), "tp", None), P("dp", None))
    return jax.shard_map(local_block, mesh=mesh, in_specs=in_specs, out_specs=out_specs, check_vma=False)
```

```python
import jax
import jax.numpy as jnp
from jax import lax
from jax.experimental import pallas as pl
from jax.experimental.pallas import tpu as pltpu
from jax.sharding import PartitionSpec as P

MESH = pl.DeviceIdType.MESH
F32, BF16 = jnp.float32, jnp.bfloat16
CONTRACT_LAST = (((1,), (1,)), ((), ()))
CONTRACT_FIRST = (((0,), (0,)), ((), ()))
GELU_C = 0.7978845608028654
GELU_K = 0.044715


def mm(a, b, dims=(((1,), (0,)), ((), ()))):
    return lax.dot_general(a, b, dims, preferred_element_type=F32)


def ep_partners():
    ep = lax.axis_index("ep")
    cx, cc = ep // 2, ep % 2
    return [ep, 2 * cx + (1 - cc), 2 * (1 - cx) + cc, 2 * (1 - cx) + (1 - cc)]


def route(idx_row, capacity, n_experts, stride):
    n = idx_row.shape[1]
    expert = lax.broadcasted_iota(jnp.int32, (n_experts, n), 0)
    hot = jnp.where(expert == idx_row, 1.0, 0.0)
    earlier = lax.broadcasted_iota(jnp.int32, (n, n), 0)
    later = lax.broadcasted_iota(jnp.int32, (n, n), 1)
    upto = jnp.where(earlier <= later, 1.0, 0.0).astype(BF16)
    count = mm(hot.astype(BF16), upto)
    position = jnp.sum(hot * count, axis=0, keepdims=True) - 1.0
    slot = jnp.where(position < capacity, idx_row.astype(F32) * stride + position, -1.0)
    return hot, slot


def pick(slot, first, rows):
    n = slot.shape[1]
    row = (lax.broadcasted_iota(jnp.int32, (rows, n), 0) + first).astype(F32)
    return jnp.where(row == slot, 1.0, 0.0).astype(BF16)


def gate_of(x, wgt, hot):
    n_experts = hot.shape[0]
    logits = mm(x, wgt, CONTRACT_LAST)
    e = jnp.exp(logits - jnp.max(logits, axis=1, keepdims=True))
    prob = e / jnp.sum(e, axis=1, keepdims=True)
    eye = jnp.where(
        lax.broadcasted_iota(jnp.int32, (n_experts, n_experts), 0)
        == lax.broadcasted_iota(jnp.int32, (n_experts, n_experts), 1), 1.0, 0.0)
    chosen = mm(hot.astype(BF16), eye.astype(BF16), CONTRACT_FIRST)
    gate = jnp.sum(chosen * prob, axis=1, keepdims=True)
    return prob, chosen, gate


def enter(peers, tp_peer):
    barrier = pltpu.get_barrier_semaphore()
    for r in (1, 2, 3):
        pl.semaphore_signal(barrier, inc=1, device_id={"ep": peers[r]}, device_id_type=MESH)
    pl.semaphore_signal(barrier, inc=1, device_id={"tp": tp_peer}, device_id_type=MESH)
    return barrier


def send(src, dst, ssem, rsem, device):
    copy = pltpu.make_async_remote_copy(
        src_ref=src, dst_ref=dst, send_sem=ssem, recv_sem=rsem, device_id=device, device_id_type=MESH)
    copy.start()
    return copy


def pair(lo, hi, e, cap):
    a = lo.astype(F32)[e * cap:(e + 1) * cap]
    b = hi.astype(F32)[e * cap:(e + 1) * cap]
    return jnp.concatenate([a, b], axis=0).astype(BF16)


def make_front(n_experts, capacity, cap):
    blk = 2 * cap

    def front(x_hbm, gy_hbm, wgt_hbm, idx_hbm, wi_hbm, wo_hbm,
              h_ref, da_ref, xs_ref, dys_ref, speer_ref, sown_ref, yhalf_ref, sfirst_ref,
              x_ref, gy_ref, wgt_ref, idx_ref, wi, wo, xsend, dysend, xrecv, dyrecv, gp,
              ypeer, yown, yrecv, yback, yland, s0peer, s0own, s0recv, s0back, s0land,
              in_sem, wsem, x_s, x_r, d_s, d_r, y_s, y_r, b_s, b_r, s_s, s_r, t_s, t_r):
        tp = lax.axis_index("tp")
        tp_peer = 1 - tp
        peers = ep_partners()
        half = x_ref.shape[1] // 2
        mine = pl.ds(pl.multiple_of(tp * half, half), half)
        theirs = pl.ds(pl.multiple_of(tp_peer * half, half), half)
        d_ff = wi.shape[2]
        with jax.named_scope("enter"):
            barrier = enter(peers, tp_peer)
            small = [pltpu.make_async_copy(src, dst, in_sem.at[k]) for k, (src, dst) in enumerate(
                ((idx_hbm, idx_ref), (x_hbm, x_ref), (wgt_hbm, wgt_ref), (gy_hbm, gy_ref)))]
            for copy in small:
                copy.start()
            loads = {}
            for e in range(2):
                loads["i", e] = pltpu.make_async_copy(wi_hbm.at[e], wi.at[e], wsem.at[0, e])
                loads["o", e] = pltpu.make_async_copy(wo_hbm.at[e], wo.at[e], wsem.at[1, e])
            for e in range(2):
                loads["i", e].start()
                loads["o", e].start()

        with jax.named_scope("route"):
            small[0].wait()
            hot, slot = route(idx_ref[...], capacity, n_experts, cap)
            picks = [pick(slot, peers[r] * blk, blk) for r in range(4)]
            small[1].wait()
            x = x_ref[...]
            for r in (2, 3, 1, 0):
                xsend[r] = mm(picks[r], x).astype(BF16)
        with jax.named_scope("barrier"):
            pl.semaphore_wait(barrier, 4)
        xc, dc = {}, {}
        with jax.named_scope("dispatch"):
            for r in (2, 3, 1):
                xc[r] = send(xsend.at[r], xrecv.at[r - 1], x_s.at[r - 1], x_r.at[r - 1], {"ep": peers[r]})
            small[2].wait()
            small[3].wait()
            _, _, gate = gate_of(x, wgt_ref[...], hot)
            dy = (gate * gy_ref[...].astype(F32)).astype(BF16)
            for r in (2, 3, 1, 0):
                dysend[r] = mm(picks[r], dy).astype(BF16)
                if r:
                    dc[r] = send(dysend.at[r], dyrecv.at[r - 1], d_s.at[r - 1], d_r.at[r - 1], {"ep": peers[r]})

        yc = {}

        def forward(g):
            rows = slice(g * blk, (g + 1) * blk)
            for e in range(2):
                lo = xsend[0] if g == 0 else xrecv[1]
                hi = xrecv[0] if g == 0 else xrecv[2]
                xs_ref[e, rows, :] = pair(lo, hi, e, cap)
            for e in range(2):
                with jax.named_scope(f"act#g={g}#e={e}"):
                    if g == 0:
                        loads["i", e].wait()
                    xg = xs_ref[e, rows, :]
                    step = d_ff // 2
                    for c in range(2):
                        cols = slice(c * step, (c + 1) * step)
                        a = mm(xg, wi[e, :, cols])
                        t = jnp.tanh(GELU_C * (a + GELU_K * (a * a * a)))
                        cdf = 0.5 * (1.0 + t)
                        h_ref[e, rows, cols] = (a * cdf).astype(BF16)
                        gp[e, rows, cols] = cdf + (0.5 * a) * (1.0 - t * t) * (GELU_C + (3.0 * GELU_C * GELU_K) * (a * a))
                with jax.named_scope(f"ypeer#g={g}#e={e}"):
                    if g == 0:
                        loads["o", e].wait()
                    ypeer[g, e] = mm(h_ref[e, rows, :], wo[e, :, theirs])
                    yc[g, e] = send(ypeer.at[g, e], yrecv.at[g, e], y_s.at[g, e], y_r.at[g, e], {"tp": tp_peer})

        sc = []

        def backward(e):
            with jax.named_scope(f"dh#e={e}"):
                for g in range(2):
                    lo = dysend[0] if g == 0 else dyrecv[1]
                    hi = dyrecv[0] if g == 0 else dyrecv[2]
                    dys_ref[e, g * blk:(g + 1) * blk, :] = pair(lo, hi, e, cap)
                dyg = dys_ref[e]
                step = d_ff // 4
                for c in range(4):
                    cols = slice(c * step, (c + 1) * step)
                    dh = mm(dyg, wo[e, cols, :], CONTRACT_LAST)
                    da_ref[e, :, cols] = (dh * gp[e, :, cols]).astype(BF16)
            with jax.named_scope(f"s#e={e}"):
                dag = da_ref[e]
                if e == 0:
                    s0peer[...] = mm(dag, wi[e, theirs, :], CONTRACT_LAST)
                    sc.append(send(s0peer, s0recv, s_s, s_r, {"tp": tp_peer}))
                    s0own[...] = mm(dag, wi[e, mine, :], CONTRACT_LAST)
                else:
                    speer_ref[...] = mm(dag, wi[e, theirs, :], CONTRACT_LAST)
                    sown_ref[...] = mm(dag, wi[e, mine, :], CONTRACT_LAST)

        bc = {}

        def give_back(g):
            for e in range(2):
                yc[g, e].wait()
            rows = slice(g * blk, (g + 1) * blk)
            both = [yown[e, rows, :] + yrecv[g, e] for e in range(2)]
            for q in range(2):
                r = 2 * g + q
                block = jnp.concatenate([both[e][q * cap:(q + 1) * cap] for e in range(2)], axis=0).astype(BF16)
                if r == 0:
                    yland[0:blk, :] = block
                else:
                    yback[r - 1] = block
                    bc[r] = send(yback.at[r - 1], yland.at[r * blk:(r + 1) * blk, :], b_s.at[r - 1], b_r.at[r - 1],
                                 {"ep": peers[r]})

        with jax.named_scope("wait_near"):
            xc[1].wait()
        forward(0)
        with jax.named_scope("wait_far"):
            xc[2].wait()
            xc[3].wait()
        forward(1)
        with jax.named_scope("yown"):
            for e in range(2):
                yown[e] = mm(h_ref[e], wo[e, :, mine])
        with jax.named_scope("wait_dy"):
            for r in (1, 2, 3):
                dc[r].wait()
        backward(0)
        with jax.named_scope("give_back#g=0"):
            give_back(0)
        backward(1)
        with jax.named_scope("give_back#g=1"):
            give_back(1)
        with jax.named_scope("s0_back"):
            sc[0].wait()
            total = s0own[...] + s0recv[...]
            tc = {}
            sfirst_ref[0:cap, :] = total[0:cap].astype(BF16)
            for r in (2, 3, 1):
                s0back[r - 1] = total[r * cap:(r + 1) * cap].astype(BF16)
                tc[r] = send(s0back.at[r - 1], s0land.at[r - 1], t_s.at[r - 1], t_r.at[r - 1], {"ep": peers[r]})
        with jax.named_scope("y_tok"):
            for r in (1, 2, 3):
                bc[r].wait()
            yhalf_ref[...] = mm(jnp.concatenate(picks, axis=0), yland[...], CONTRACT_FIRST).astype(BF16)
        with jax.named_scope("s0_land"):
            for r in (1, 2, 3):
                tc[r].wait()
            sfirst_ref[...] = jnp.concatenate(
                [total[0:cap]] + [s0land[r - 1].astype(F32) for r in (1, 2, 3)], axis=0).astype(BF16)

    return front


def grads_kernel(h_ref, dys_ref, xs_ref, da_ref, dwi_ref, dwo_ref):
    dwo_ref[0] = mm(h_ref[0], dys_ref[0], CONTRACT_FIRST)
    dwi_ref[0] = mm(xs_ref[0], da_ref[0], CONTRACT_FIRST)


def make_back(n_experts, capacity, cap):
    blk = 2 * cap

    def back(x_ref, gy_ref, wgt_ref, idx_ref, ymine_ref, ytheirs_ref, sfirst_ref, sown_ref, srecv_ref,
             out_ref, dx_ref, dwgt_ref,
             sback, sland, dxsend, dxland, dwg,
             b_s, b_r, x_s, x_r, w_s, w_r):
        tp = lax.axis_index("tp")
        ep = lax.axis_index("ep")
        tp_peer = 1 - tp
        peers = ep_partners()
        half = x_ref.shape[1] // 2
        mine = pl.ds(pl.multiple_of(tp * half, half), half)
        theirs = pl.ds(pl.multiple_of(tp_peer * half, half), half)
        with jax.named_scope("enter"):
            barrier = enter(peers, tp_peer)
            total = sown_ref[...] + srecv_ref[...]
            for r in (2, 3, 1):
                sback[r - 1] = total[r * cap:(r + 1) * cap].astype(BF16)
            pl.semaphore_wait(barrier, 4)
        bc, wc = {}, {}
        with jax.named_scope("s_back"):
            for r in (2, 3, 1):
                bc[r] = send(sback.at[r - 1], sland.at[r - 1], b_s.at[r - 1], b_r.at[r - 1], {"ep": peers[r]})
        with jax.named_scope("router"):
            hot, slot = route(idx_ref[...], capacity, n_experts, cap)
            x = x_ref[...]
            prob, chosen, gate = gate_of(x, wgt_ref[...], hot)
            y_mine = ymine_ref[...].astype(F32)
            y_theirs = ytheirs_ref[...].astype(F32)
            dgate = (jnp.sum(gy_ref[:, mine].astype(F32) * y_mine, axis=1, keepdims=True)
                     + jnp.sum(gy_ref[:, theirs].astype(F32) * y_theirs, axis=1, keepdims=True))
            dlogits = (dgate * prob * (chosen - gate)).astype(BF16)
            dwg[ep] = mm(dlogits, x, CONTRACT_FIRST)
            for r in (2, 3, 1):
                wc[r] = send(dwg.at[ep], dwg.at[ep], w_s.at[r - 1], w_r.at[r - 1], {"ep": peers[r]})
            rgrad = mm(dlogits, wgt_ref[:, mine])
            even = jnp.concatenate([pick(slot, peers[r] * blk, cap) for r in range(4)], axis=0)
            odd = jnp.concatenate([pick(slot, peers[r] * blk + cap, cap) for r in range(4)], axis=0)
            s_even = mm(even, sfirst_ref[...], CONTRACT_FIRST)
        with jax.named_scope("s_wait"):
            for r in (1, 2, 3):
                bc[r].wait()
        with jax.named_scope("dx"):
            second = jnp.concatenate(
                [total[0:cap]] + [sland[r - 1].astype(F32) for r in (1, 2, 3)], axis=0).astype(BF16)
            dx_mine = (s_even + mm(odd, second, CONTRACT_FIRST) + rgrad).astype(BF16)
            dxsend[...] = dx_mine
            xc = send(dxsend, dxland, x_s, x_r, {"tp": tp_peer})
        with jax.named_scope("out"):
            dx_ref[:, mine] = dx_mine
            out_ref[:, mine] = (gate * y_mine).astype(BF16)
            out_ref[:, theirs] = (gate * y_theirs).astype(BF16)
            for r in (1, 2, 3):
                wc[r].wait()
            dwgt_ref[...] = (dwg[0] + dwg[1]) + (dwg[2] + dwg[3])
        with jax.named_scope("dx_wait"):
            xc.wait()
            dx_ref[:, theirs] = dxland[...]

    return back


def finish(out_ref, dx_ref, dwgt_ref, out_hbm, dx_hbm, dwgt_hbm, sem):
    copies = [pltpu.make_async_copy(src, dst, sem.at[k]) for k, (src, dst) in enumerate(
        ((out_ref, out_hbm), (dx_ref, dx_hbm), (dwgt_ref, dwgt_hbm)))]
    for copy in copies:
        copy.start()
    for copy in copies:
        copy.wait()


def solution(mesh):
    row_spec = P(("dp", "ep"), None)
    vmem = pl.BlockSpec(memory_space=pltpu.VMEM)
    hbm = pl.BlockSpec(memory_space=pltpu.HBM)

    def local_block(tokens, grad_out, w_router, w_in, w_out, expert_ids):
        n, d_model = tokens.shape
        n_experts = w_router.shape[1]
        le, _, d_ff = w_in.shape
        capacity = (6 * n + 5 * n_experts - 1) // (5 * n_experts)
        cap = -(-capacity // 8) * 8
        blk = le * cap
        rows = 4 * cap
        half = d_model // 2
        wgt = w_router.T
        idx_row = expert_ids.reshape(1, n)
        sds = jax.ShapeDtypeStruct
        dma = pltpu.SemaphoreType.DMA

        h, da, xs, dys, speer, sown, ymine, sfirst = pl.pallas_call(
            make_front(n_experts, capacity, cap),
            out_shape=(sds((le, rows, d_ff), BF16), sds((le, rows, d_ff), BF16), sds((le, rows, d_model), BF16),
                       sds((le, rows, d_model), BF16), sds((rows, half), F32), sds((rows, half), F32),
                       sds((n, half), BF16), sds((rows, half), BF16)),
            in_specs=[hbm] * 6,
            out_specs=(vmem,) * 8,
            scratch_shapes=[
                pltpu.VMEM((n, d_model), BF16), pltpu.VMEM((n, d_model), BF16), pltpu.VMEM((n_experts, d_model), BF16),
                pltpu.VMEM((1, n), jnp.int32),
                pltpu.VMEM((le, d_model, d_ff), BF16), pltpu.VMEM((le, d_ff, d_model), BF16),
                pltpu.VMEM((4, blk, d_model), BF16), pltpu.VMEM((4, blk, d_model), BF16),
                pltpu.VMEM((3, blk, d_model), BF16), pltpu.VMEM((3, blk, d_model), BF16),
                pltpu.VMEM((le, rows, d_ff), F32),
                pltpu.VMEM((2, le, blk, half), F32), pltpu.VMEM((le, rows, half), F32), pltpu.VMEM((2, le, blk, half), F32),
                pltpu.VMEM((3, blk, half), BF16), pltpu.VMEM((4 * blk, half), BF16),
                pltpu.VMEM((rows, half), F32), pltpu.VMEM((rows, half), F32), pltpu.VMEM((rows, half), F32),
                pltpu.VMEM((3, cap, half), BF16), pltpu.VMEM((3, cap, half), BF16),
                dma((4,)), dma((2, le)), dma((3,)), dma((3,)), dma((3,)), dma((3,)), dma((2, le)), dma((2, le)),
                dma((3,)), dma((3,)), dma, dma, dma((3,)), dma((3,)),
            ],
            compiler_params=pltpu.CompilerParams(collective_id=0, has_side_effects=True, vmem_limit_bytes=40 * 2**20),
            name="front",
        )(*[pltpu.with_memory_space_constraint(v, pltpu.HBM) for v in (tokens, grad_out, wgt, idx_row, w_in, w_out)])

        swap = [(0, 1), (1, 0)]
        srecv = lax.ppermute(speer, "tp", swap)
        ytheirs = lax.ppermute(ymine, "tp", swap)

        steps = 4
        hs, ms = d_ff // steps, d_model // steps
        dwi, dwo = pl.pallas_call(
            grads_kernel,
            grid=(le, steps),
            out_shape=(sds((le, d_model, d_ff), F32), sds((le, d_ff, d_model), F32)),
            in_specs=[pl.BlockSpec((1, rows, hs), lambda e, c: (e, 0, c)), pl.BlockSpec((1, rows, d_model), lambda e, c: (e, 0, 0)),
                      pl.BlockSpec((1, rows, ms), lambda e, c: (e, 0, c)), pl.BlockSpec((1, rows, d_ff), lambda e, c: (e, 0, 0))],
            out_specs=(pl.BlockSpec((1, ms, d_ff), lambda e, c: (e, c, 0)), pl.BlockSpec((1, hs, d_model), lambda e, c: (e, c, 0))),
            cost_estimate=pl.CostEstimate(flops=4 * le * rows * d_model * d_ff, bytes_accessed=8 * le * d_model * d_ff,
                                          transcendentals=0),
            compiler_params=pltpu.CompilerParams(vmem_limit_bytes=24 * 2**20),
            name="weight_grads",
        )(h, dys, xs, da)

        ends = (sds((n, d_model), BF16), sds((n, d_model), BF16), sds((n_experts, d_model), F32))
        parts = pl.pallas_call(
            make_back(n_experts, capacity, cap),
            out_shape=ends,
            in_specs=[vmem] * 9,
            out_specs=(vmem,) * 3,
            scratch_shapes=[
                pltpu.VMEM((3, cap, half), BF16), pltpu.VMEM((3, cap, half), BF16),
                pltpu.VMEM((n, half), BF16), pltpu.VMEM((n, half), BF16),
                pltpu.VMEM((4, n_experts, d_model), F32),
                dma((3,)), dma((3,)), dma, dma, dma((3,)), dma((3,)),
            ],
            compiler_params=pltpu.CompilerParams(collective_id=1, has_side_effects=True, vmem_limit_bytes=24 * 2**20),
            name="back",
        )(tokens, grad_out, wgt, idx_row, ymine, ytheirs, sfirst, sown, srecv)
        out, dx, dwgt = pl.pallas_call(
            finish, out_shape=ends, in_specs=[vmem] * 3, out_specs=(hbm,) * 3, scratch_shapes=[dma((3,))],
            compiler_params=pltpu.CompilerParams(vmem_limit_bytes=8 * 2**20), name="finish",
        )(*parts)
        return out, dx, dwi, dwo, dwgt.T

    in_specs = (row_spec, row_spec, P(None, None), P("ep", None, "tp"), P("ep", "tp", None), P(("dp", "ep")))
    out_specs = (row_spec, row_spec, P(("dp", "ep"), None, "tp"), P(("dp", "ep"), "tp", None), P("dp", None))
    return jax.shard_map(local_block, mesh=mesh, in_specs=in_specs, out_specs=out_specs, check_vma=False)
```

```python
import jax
import jax.numpy as jnp
from jax import lax
from jax.experimental import pallas as pl
from jax.experimental.pallas import tpu as pltpu
from jax.sharding import PartitionSpec as P

MESH = pl.DeviceIdType.MESH
F32, BF16 = jnp.float32, jnp.bfloat16
CONTRACT_LAST = (((1,), (1,)), ((), ()))
CONTRACT_FIRST = (((0,), (0,)), ((), ()))
GELU_C = 0.7978845608028654
GELU_K = 0.044715


def mm(a, b, dims=(((1,), (0,)), ((), ()))):
    return lax.dot_general(a, b, dims, preferred_element_type=F32)


def ep_partners():
    ep = lax.axis_index("ep")
    cx, cc = ep // 2, ep % 2
    return [ep, 2 * cx + (1 - cc), 2 * (1 - cx) + cc, 2 * (1 - cx) + (1 - cc)]


def route(idx_row, capacity, n_experts, stride):
    n = idx_row.shape[1]
    expert = lax.broadcasted_iota(jnp.int32, (n_experts, n), 0)
    hot = jnp.where(expert == idx_row, 1.0, 0.0)
    earlier = lax.broadcasted_iota(jnp.int32, (n, n), 0)
    later = lax.broadcasted_iota(jnp.int32, (n, n), 1)
    upto = jnp.where(earlier <= later, 1.0, 0.0).astype(BF16)
    count = mm(hot.astype(BF16), upto)
    position = jnp.sum(hot * count, axis=0, keepdims=True) - 1.0
    slot = jnp.where(position < capacity, idx_row.astype(F32) * stride + position, -1.0)
    return hot, slot


def pick(slot, first, rows):
    n = slot.shape[1]
    row = (lax.broadcasted_iota(jnp.int32, (rows, n), 0) + first).astype(F32)
    return jnp.where(row == slot, 1.0, 0.0).astype(BF16)


def gate_of(x, wgt, hot):
    n_experts = hot.shape[0]
    logits = mm(x, wgt, CONTRACT_LAST)
    e = jnp.exp(logits - jnp.max(logits, axis=1, keepdims=True))
    prob = e / jnp.sum(e, axis=1, keepdims=True)
    eye = jnp.where(
        lax.broadcasted_iota(jnp.int32, (n_experts, n_experts), 0)
        == lax.broadcasted_iota(jnp.int32, (n_experts, n_experts), 1), 1.0, 0.0)
    chosen = mm(hot.astype(BF16), eye.astype(BF16), CONTRACT_FIRST)
    gate = jnp.sum(chosen * prob, axis=1, keepdims=True)
    return prob, chosen, gate


def enter(peers, tp_peer):
    barrier = pltpu.get_barrier_semaphore()
    for r in (1, 2, 3):
        pl.semaphore_signal(barrier, inc=1, device_id={"ep": peers[r]}, device_id_type=MESH)
    pl.semaphore_signal(barrier, inc=1, device_id={"tp": tp_peer}, device_id_type=MESH)
    return barrier


def send(src, dst, ssem, rsem, device):
    copy = pltpu.make_async_remote_copy(
        src_ref=src, dst_ref=dst, send_sem=ssem, recv_sem=rsem, device_id=device, device_id_type=MESH)
    copy.start()
    return copy


def pair(lo, hi, e, cap):
    a = lo.astype(F32)[e * cap:(e + 1) * cap]
    b = hi.astype(F32)[e * cap:(e + 1) * cap]
    return jnp.concatenate([a, b], axis=0).astype(BF16)


def make_front(n_experts, capacity, cap):
    blk = 2 * cap

    def front(x_hbm, gy_hbm, wgt_hbm, idx_hbm, wi_hbm, wo_hbm,
              h_ref, da_ref, xs_ref, dys_ref, speer_ref, sown_ref, ynear_ref, yfar0_ref, yfar1_ref,
              x_ref, gy_ref, wgt_ref, idx_ref, wi, wo, xsend, dysend, xrecv, dyrecv, gp,
              ypeer, yown, yrecv, yback, yland,
              in_sem, wsem, x_s, x_r, d_s, d_r, y_s, y_r, b_s, b_r):
        tp = lax.axis_index("tp")
        tp_peer = 1 - tp
        peers = ep_partners()
        half = x_ref.shape[1] // 2
        mine = pl.ds(pl.multiple_of(tp * half, half), half)
        theirs = pl.ds(pl.multiple_of(tp_peer * half, half), half)
        d_ff = wi.shape[2]
        near, far = slice(0, blk), slice(blk, 2 * blk)
        with jax.named_scope("enter"):
            barrier = enter(peers, tp_peer)
            small = [pltpu.make_async_copy(src, dst, in_sem.at[k]) for k, (src, dst) in enumerate(
                ((idx_hbm, idx_ref), (x_hbm, x_ref), (wgt_hbm, wgt_ref), (gy_hbm, gy_ref)))]
            for copy in small:
                copy.start()
            loads = {}
            for e in range(2):
                loads["i", e] = pltpu.make_async_copy(wi_hbm.at[e], wi.at[e], wsem.at[0, e])
                loads["o", e] = pltpu.make_async_copy(wo_hbm.at[e], wo.at[e], wsem.at[1, e])
            for e in range(2):
                loads["i", e].start()
                loads["o", e].start()

        xc, dc, yc = {}, {}, {}

        def send_x(r):
            xc[r] = send(xsend.at[r], xrecv.at[r - 1], x_s.at[r - 1], x_r.at[r - 1], {"ep": peers[r]})

        with jax.named_scope("route"):
            small[0].wait()
            hot, slot = route(idx_ref[...], capacity, n_experts, cap)
            picks = [pick(slot, peers[r] * blk, blk) for r in range(4)]
            small[1].wait()
            x = x_ref[...]
            for r in (2, 3):
                xsend[r] = mm(picks[r], x).astype(BF16)
        with jax.named_scope("barrier"):
            pl.semaphore_wait(barrier, 4)
        with jax.named_scope("dispatch_x"):
            send_x(2)
            send_x(3)
            xsend[1] = mm(picks[1], x).astype(BF16)
            send_x(1)
            xsend[0] = mm(picks[0], x).astype(BF16)
        with jax.named_scope("gate"):
            small[2].wait()
            small[3].wait()
            _, _, gate = gate_of(x, wgt_ref[...], hot)
            dy = (gate * gy_ref[...].astype(F32)).astype(BF16)

        def dispatch_dy():
            for r in (2, 3, 1, 0):
                dysend[r] = mm(picks[r], dy).astype(BF16)
                if r:
                    dc[r] = send(dysend.at[r], dyrecv.at[r - 1], d_s.at[r - 1], d_r.at[r - 1], {"ep": peers[r]})

        def forward(g, e):
            rows = far if g else near
            if g == 0:
                loads["i", e].wait()
            xg = xs_ref[e, rows, :]
            step = d_ff // 2
            for c in range(2):
                cols = slice(c * step, (c + 1) * step)
                a = mm(xg, wi[e, :, cols])
                t = jnp.tanh(GELU_C * (a + GELU_K * (a * a * a)))
                cdf = 0.5 * (1.0 + t)
                h_ref[e, rows, cols] = (a * cdf).astype(BF16)
                gp[e, rows, cols] = cdf + (0.5 * a) * (1.0 - t * t) * (GELU_C + (3.0 * GELU_C * GELU_K) * (a * a))
            if g == 0:
                loads["o", e].wait()
            ypeer[g, e] = mm(h_ref[e, rows, :], wo[e, :, theirs])
            yc[g, e] = send(ypeer.at[g, e], yrecv.at[g, e], y_s.at[g, e], y_r.at[g, e], {"tp": tp_peer})

        def backward(g, e):
            rows = far if g else near
            dyg = dys_ref[e, rows, :]
            step = d_ff // 4
            for c in range(4):
                cols = slice(c * step, (c + 1) * step)
                dh = mm(dyg, wo[e, cols, :], CONTRACT_LAST)
                da_ref[e, rows, cols] = (dh * gp[e, rows, cols]).astype(BF16)
            dag = da_ref[e, rows, :]
            speer_ref[e, rows, :] = mm(dag, wi[e, theirs, :], CONTRACT_LAST)
            sown_ref[e, rows, :] = mm(dag, wi[e, mine, :], CONTRACT_LAST)

        def y_blocks(g):
            for e in range(2):
                yc[g, e].wait()
            both = [yown[e, far if g else near, :] + yrecv[g, e] for e in range(2)]
            return [jnp.concatenate([both[e][q * cap:(q + 1) * cap] for e in range(2)], axis=0).astype(BF16) for q in range(2)]

        with jax.named_scope("wait_near"):
            xc[1].wait()
            for e in range(2):
                xs_ref[e, near, :] = pair(xsend[0], xrecv[0], e, cap)
        with jax.named_scope("fwd#g=0#e=0"):
            forward(0, 0)
        with jax.named_scope("dispatch_dy"):
            dispatch_dy()
        with jax.named_scope("fwd#g=0#e=1"):
            forward(0, 1)
        with jax.named_scope("bwd#g=0#e=0"):
            dc[1].wait()
            for e in range(2):
                dys_ref[e, near, :] = pair(dysend[0], dyrecv[0], e, cap)
            backward(0, 0)
        with jax.named_scope("wait_far"):
            xc[2].wait()
            xc[3].wait()
            for e in range(2):
                xs_ref[e, far, :] = pair(xrecv[1], xrecv[2], e, cap)
        with jax.named_scope("fwd#g=1#e=0"):
            forward(1, 0)
        with jax.named_scope("fwd#g=1#e=1"):
            forward(1, 1)
        with jax.named_scope("bwd#g=0#e=1"):
            backward(0, 1)
        with jax.named_scope("yown"):
            for e in range(2):
                yown[e] = mm(h_ref[e], wo[e, :, mine])
        with jax.named_scope("y_near"):
            kept, away = y_blocks(0)
            ynear_ref[near, :] = kept
            yback[...] = away
            bc = send(yback, yland, b_s, b_r, {"ep": peers[1]})
        with jax.named_scope("wait_dy"):
            dc[2].wait()
            dc[3].wait()
            for e in range(2):
                dys_ref[e, far, :] = pair(dyrecv[1], dyrecv[2], e, cap)
        with jax.named_scope("bwd#g=1#e=0"):
            backward(1, 0)
        with jax.named_scope("bwd#g=1#e=1"):
            backward(1, 1)
        with jax.named_scope("y_far"):
            bc.wait()
            ynear_ref[far, :] = yland[...]
            yfar0_ref[...], yfar1_ref[...] = y_blocks(1)

    return front


def grads_kernel(h_ref, dys_ref, xs_ref, da_ref, dwi_ref, dwo_ref):
    dwo_ref[0] = mm(h_ref[0], dys_ref[0], CONTRACT_FIRST)
    dwi_ref[0] = mm(xs_ref[0], da_ref[0], CONTRACT_FIRST)


def make_back(n_experts, capacity, cap):
    blk = 2 * cap

    def back(x_ref, gy_ref, wgt_ref, idx_ref, ynear_ref, yfar0_ref, yfar1_ref, sown_ref, srecv_ref,
             out_ref, dx_ref, dwgt_ref,
             ysend, yland, sback, sland, stsend, stland, dwg,
             y_s, y_r, b_s, b_r, x_s, x_r, w_s, w_r):
        tp = lax.axis_index("tp")
        ep = lax.axis_index("ep")
        tp_peer = 1 - tp
        peers = ep_partners()
        half = x_ref.shape[1] // 2
        mine = pl.ds(pl.multiple_of(tp * half, half), half)
        theirs = pl.ds(pl.multiple_of(tp_peer * half, half), half)
        with jax.named_scope("enter"):
            barrier = enter(peers, tp_peer)
            hot, slot = route(idx_ref[...], capacity, n_experts, cap)
            picks = jnp.concatenate([pick(slot, peers[r] * blk, blk) for r in range(4)], axis=0)
            y_rows = jnp.concatenate([ynear_ref[...], yfar0_ref[...], yfar1_ref[...]], axis=0)
            ysend[...] = mm(picks, y_rows, CONTRACT_FIRST).astype(BF16)
            pl.semaphore_wait(barrier, 4)
            yc = send(ysend, yland, y_s, y_r, {"tp": tp_peer})
        with jax.named_scope("s_back"):
            bc = {}
            for g in (1, 0):
                rows = slice(g * blk, (g + 1) * blk)
                both = [sown_ref[e, rows, :] + srecv_ref[e, rows, :] for e in range(2)]
                for q in range(2):
                    r = 2 * g + q
                    block = jnp.concatenate([both[e][q * cap:(q + 1) * cap] for e in range(2)], axis=0).astype(BF16)
                    if r == 0:
                        sland[0:blk, :] = block
                    else:
                        sback[r - 1] = block
                        bc[r] = send(sback.at[r - 1], sland.at[r * blk:(r + 1) * blk, :], b_s.at[r - 1], b_r.at[r - 1],
                                     {"ep": peers[r]})
        with jax.named_scope("gate"):
            x = x_ref[...]
            prob, chosen, gate = gate_of(x, wgt_ref[...], hot)
            y_mine = ysend[...].astype(F32)
            out_ref[:, mine] = (gate * y_mine).astype(BF16)
            dgate = jnp.sum(gy_ref[:, mine].astype(F32) * y_mine, axis=1, keepdims=True)
        with jax.named_scope("s_wait"):
            for r in (1, 2, 3):
                bc[r].wait()
            stsend[...] = mm(picks, sland[...], CONTRACT_FIRST).astype(BF16)
            xc = send(stsend, stland, x_s, x_r, {"tp": tp_peer})
        with jax.named_scope("y_wait"):
            yc.wait()
        with jax.named_scope("router"):
            y_theirs = yland[...].astype(F32)
            out_ref[:, theirs] = (gate * y_theirs).astype(BF16)
            dgate = dgate + jnp.sum(gy_ref[:, theirs].astype(F32) * y_theirs, axis=1, keepdims=True)
            dlogits = (dgate * prob * (chosen - gate)).astype(BF16)
            dwg[ep] = mm(dlogits, x, CONTRACT_FIRST)
            wc = {}
            for r in (2, 3, 1):
                wc[r] = send(dwg.at[ep], dwg.at[ep], w_s.at[r - 1], w_r.at[r - 1], {"ep": peers[r]})
            dx_ref[:, mine] = (stsend[...].astype(F32) + mm(dlogits, wgt_ref[:, mine])).astype(BF16)
            rgrad = mm(dlogits, wgt_ref[:, theirs])
        with jax.named_scope("dwg"):
            for r in (1, 2, 3):
                wc[r].wait()
            dwgt_ref[...] = (dwg[0] + dwg[1]) + (dwg[2] + dwg[3])
        with jax.named_scope("dx_wait"):
            xc.wait()
        with jax.named_scope("dx"):
            dx_ref[:, theirs] = (stland[...].astype(F32) + rgrad).astype(BF16)

    return back


def finish(out_ref, dx_ref, dwgt_ref, out_hbm, dx_hbm, dwgt_hbm, sem):
    copies = [pltpu.make_async_copy(src, dst, sem.at[k]) for k, (src, dst) in enumerate(
        ((out_ref, out_hbm), (dx_ref, dx_hbm), (dwgt_ref, dwgt_hbm)))]
    for copy in copies:
        copy.start()
    for copy in copies:
        copy.wait()


def solution(mesh):
    row_spec = P(("dp", "ep"), None)
    vmem = pl.BlockSpec(memory_space=pltpu.VMEM)
    hbm = pl.BlockSpec(memory_space=pltpu.HBM)

    def local_block(tokens, grad_out, w_router, w_in, w_out, expert_ids):
        n, d_model = tokens.shape
        n_experts = w_router.shape[1]
        le, _, d_ff = w_in.shape
        capacity = (6 * n + 5 * n_experts - 1) // (5 * n_experts)
        cap = -(-capacity // 8) * 8
        blk = le * cap
        rows = 4 * cap
        half = d_model // 2
        wgt = w_router.T
        idx_row = expert_ids.reshape(1, n)
        sds = jax.ShapeDtypeStruct
        dma = pltpu.SemaphoreType.DMA

        h, da, xs, dys, speer, sown, ynear, yfar0, yfar1 = pl.pallas_call(
            make_front(n_experts, capacity, cap),
            out_shape=(sds((le, rows, d_ff), BF16), sds((le, rows, d_ff), BF16), sds((le, rows, d_model), BF16),
                       sds((le, rows, d_model), BF16), sds((le, rows, half), F32), sds((le, rows, half), F32),
                       sds((2 * blk, half), BF16), sds((blk, half), BF16), sds((blk, half), BF16)),
            in_specs=[hbm] * 6,
            out_specs=(vmem,) * 9,
            scratch_shapes=[
                pltpu.VMEM((n, d_model), BF16), pltpu.VMEM((n, d_model), BF16), pltpu.VMEM((n_experts, d_model), BF16),
                pltpu.VMEM((1, n), jnp.int32),
                pltpu.VMEM((le, d_model, d_ff), BF16), pltpu.VMEM((le, d_ff, d_model), BF16),
                pltpu.VMEM((4, blk, d_model), BF16), pltpu.VMEM((4, blk, d_model), BF16),
                pltpu.VMEM((3, blk, d_model), BF16), pltpu.VMEM((3, blk, d_model), BF16),
                pltpu.VMEM((le, rows, d_ff), F32),
                pltpu.VMEM((2, le, blk, half), F32), pltpu.VMEM((le, rows, half), F32), pltpu.VMEM((2, le, blk, half), F32),
                pltpu.VMEM((blk, half), BF16), pltpu.VMEM((blk, half), BF16),
                dma((4,)), dma((2, le)), dma((3,)), dma((3,)), dma((3,)), dma((3,)), dma((2, le)), dma((2, le)), dma, dma,
            ],
            compiler_params=pltpu.CompilerParams(collective_id=0, has_side_effects=True, vmem_limit_bytes=40 * 2**20),
            name="front",
        )(*[pltpu.with_memory_space_constraint(v, pltpu.HBM) for v in (tokens, grad_out, wgt, idx_row, w_in, w_out)])

        srecv = lax.ppermute(speer, "tp", [(0, 1), (1, 0)])
        yland0 = lax.ppermute(yfar0, "ep", [(0, 2), (2, 0), (1, 3), (3, 1)])
        yland1 = lax.ppermute(yfar1, "ep", [(0, 3), (3, 0), (1, 2), (2, 1)])

        steps = 4
        hs, ms = d_ff // steps, d_model // steps
        dwi, dwo = pl.pallas_call(
            grads_kernel,
            grid=(le, steps),
            out_shape=(sds((le, d_model, d_ff), F32), sds((le, d_ff, d_model), F32)),
            in_specs=[pl.BlockSpec((1, rows, hs), lambda e, c: (e, 0, c)), pl.BlockSpec((1, rows, d_model), lambda e, c: (e, 0, 0)),
                      pl.BlockSpec((1, rows, ms), lambda e, c: (e, 0, c)), pl.BlockSpec((1, rows, d_ff), lambda e, c: (e, 0, 0))],
            out_specs=(pl.BlockSpec((1, ms, d_ff), lambda e, c: (e, c, 0)), pl.BlockSpec((1, hs, d_model), lambda e, c: (e, c, 0))),
            cost_estimate=pl.CostEstimate(flops=4 * le * rows * d_model * d_ff, bytes_accessed=8 * le * d_model * d_ff,
                                          transcendentals=0),
            compiler_params=pltpu.CompilerParams(vmem_limit_bytes=24 * 2**20),
            name="weight_grads",
        )(h, dys, xs, da)

        ends = (sds((n, d_model), BF16), sds((n, d_model), BF16), sds((n_experts, d_model), F32))
        parts = pl.pallas_call(
            make_back(n_experts, capacity, cap),
            out_shape=ends,
            in_specs=[vmem] * 9,
            out_specs=(vmem,) * 3,
            scratch_shapes=[
                pltpu.VMEM((n, half), BF16), pltpu.VMEM((n, half), BF16),
                pltpu.VMEM((3, blk, half), BF16), pltpu.VMEM((4 * blk, half), BF16),
                pltpu.VMEM((n, half), BF16), pltpu.VMEM((n, half), BF16),
                pltpu.VMEM((4, n_experts, d_model), F32),
                dma, dma, dma((3,)), dma((3,)), dma, dma, dma((3,)), dma((3,)),
            ],
            compiler_params=pltpu.CompilerParams(collective_id=1, has_side_effects=True, vmem_limit_bytes=24 * 2**20),
            name="back",
        )(tokens, grad_out, wgt, idx_row, ynear, yland0, yland1, sown, srecv)
        out, dx, dwgt = pl.pallas_call(
            finish, out_shape=ends, in_specs=[vmem] * 3, out_specs=(hbm,) * 3, scratch_shapes=[dma((3,))],
            compiler_params=pltpu.CompilerParams(vmem_limit_bytes=8 * 2**20), name="finish",
        )(*parts)
        return out, dx, dwi, dwo, dwgt.T

    in_specs = (row_spec, row_spec, P(None, None), P("ep", None, "tp"), P("ep", "tp", None), P(("dp", "ep")))
    out_specs = (row_spec, row_spec, P(("dp", "ep"), None, "tp"), P(("dp", "ep"), "tp", None), P("dp", None))
    return jax.shard_map(local_block, mesh=mesh, in_specs=in_specs, out_specs=out_specs, check_vma=False)
```

```python
import jax
import jax.numpy as jnp
from jax import lax
from jax.experimental import pallas as pl
from jax.experimental.pallas import tpu as pltpu
from jax.sharding import PartitionSpec as P

MESH = pl.DeviceIdType.MESH
F32, BF16 = jnp.float32, jnp.bfloat16
CONTRACT_LAST = (((1,), (1,)), ((), ()))
CONTRACT_FIRST = (((0,), (0,)), ((), ()))
GELU_C = 0.7978845608028654
GELU_K = 0.044715


def mm(a, b, dims=(((1,), (0,)), ((), ()))):
    return lax.dot_general(a, b, dims, preferred_element_type=F32)


def ep_partners():
    ep = lax.axis_index("ep")
    cx, cc = ep // 2, ep % 2
    return [ep, 2 * cx + (1 - cc), 2 * (1 - cx) + cc, 2 * (1 - cx) + (1 - cc)]


def route(idx_row, capacity, n_experts, stride):
    n = idx_row.shape[1]
    expert = lax.broadcasted_iota(jnp.int32, (n_experts, n), 0)
    hot = jnp.where(expert == idx_row, 1.0, 0.0)
    earlier = lax.broadcasted_iota(jnp.int32, (n, n), 0)
    later = lax.broadcasted_iota(jnp.int32, (n, n), 1)
    upto = jnp.where(earlier <= later, 1.0, 0.0).astype(BF16)
    count = mm(hot.astype(BF16), upto)
    position = jnp.sum(hot * count, axis=0, keepdims=True) - 1.0
    slot = jnp.where(position < capacity, idx_row.astype(F32) * stride + position, -1.0)
    return hot, slot


def pick(slot, firsts, rows):
    n = slot.shape[1]
    row = lax.broadcasted_iota(jnp.int32, (rows, n), 0)
    parts = [jnp.where((row + first).astype(F32) == slot, 1.0, 0.0) for first in firsts]
    return jnp.concatenate(parts, axis=0).astype(BF16)


def gate_of(x, wgt, hot):
    n_experts = hot.shape[0]
    logits = mm(x, wgt, CONTRACT_LAST)
    e = jnp.exp(logits - jnp.max(logits, axis=1, keepdims=True))
    prob = e / jnp.sum(e, axis=1, keepdims=True)
    eye = jnp.where(
        lax.broadcasted_iota(jnp.int32, (n_experts, n_experts), 0)
        == lax.broadcasted_iota(jnp.int32, (n_experts, n_experts), 1), 1.0, 0.0)
    chosen = mm(hot.astype(BF16), eye.astype(BF16), CONTRACT_FIRST)
    gate = jnp.sum(chosen * prob, axis=1, keepdims=True)
    return prob, chosen, gate


def enter(peers, tp_peer):
    barrier = pltpu.get_barrier_semaphore()
    for r in (1, 2, 3):
        pl.semaphore_signal(barrier, inc=1, device_id={"ep": peers[r]}, device_id_type=MESH)
    pl.semaphore_signal(barrier, inc=1, device_id={"tp": tp_peer}, device_id_type=MESH)
    return barrier


def send(src, dst, ssem, rsem, device):
    copy = pltpu.make_async_remote_copy(
        src_ref=src, dst_ref=dst, send_sem=ssem, recv_sem=rsem, device_id=device, device_id_type=MESH)
    copy.start()
    return copy


def make_front(n_experts, capacity, cap):
    blk = 2 * cap

    def front(x_hbm, gy_hbm, wgt_hbm, idx_hbm, wi_hbm, wo_hbm,
              h_ref, da_ref, xs_ref, dys_ref, speer_ref, sown_ref, ynear_ref, yfar0_ref, yfar1_ref,
              picks_ref, prob_ref, chosen_ref,
              x_ref, gy_ref, wgt_ref, idx_ref, wi, wo, xsend, dysend, gp,
              ypeer, yown, yrecv, yback, yland,
              in_sem, wsem, x_s, x_r, d_s, d_r, y_s, y_r, b_s, b_r):
        tp = lax.axis_index("tp")
        tp_peer = 1 - tp
        peers = ep_partners()
        half = x_ref.shape[1] // 2
        mine = pl.ds(pl.multiple_of(tp * half, half), half)
        theirs = pl.ds(pl.multiple_of(tp_peer * half, half), half)
        d_ff = wi.shape[2]
        near, far, whole = slice(0, blk), slice(blk, 2 * blk), slice(0, 2 * blk)
        with jax.named_scope("enter"):
            small = [pltpu.make_async_copy(src, dst, in_sem.at[k]) for k, (src, dst) in enumerate(
                ((idx_hbm, idx_ref), (x_hbm, x_ref), (wgt_hbm, wgt_ref), (gy_hbm, gy_ref)))]
            for copy in small:
                copy.start()
            barrier = enter(peers, tp_peer)
            loads = {}
            for e in range(2):
                loads["i", e] = pltpu.make_async_copy(wi_hbm.at[e], wi.at[e], wsem.at[0, e])
                loads["o", e] = pltpu.make_async_copy(wo_hbm.at[e], wo.at[e], wsem.at[1, e])
            for e in range(2):
                loads["i", e].start()
                loads["o", e].start()

        xc, dc, yc = {}, {}, {}

        def dispatch(v, g, e, buf, rows_ref, ssem, rsem, made):
            first = [peers[2 * g + q] * blk + e * cap for q in range(2)]
            rows = mm(pick(slot, first, cap), v)
            for q in range(2):
                r = 2 * g + q
                part = rows[q * cap:(q + 1) * cap].astype(BF16)
                if r == 0:
                    rows_ref[e, 0:cap, :] = part
                else:
                    buf[r - 1, e] = part
            return lambda: [made.__setitem__((r, e), send(
                buf.at[r - 1, e], rows_ref.at[e, r * cap:(r + 1) * cap, :], ssem.at[r - 1, e], rsem.at[r - 1, e],
                {"ep": peers[r]})) for r in (2 * g, 2 * g + 1) if r]

        def dispatch_x(g, e):
            return dispatch(x_ref[...], g, e, xsend, xs_ref, x_s, x_r, xc)

        with jax.named_scope("route"):
            small[0].wait()
            hot, slot = route(idx_ref[...], capacity, n_experts, cap)
            small[1].wait()
            go = dispatch_x(1, 0)
        with jax.named_scope("barrier"):
            pl.semaphore_wait(barrier, 4)
        with jax.named_scope("dispatch_x"):
            go()
            for e in range(2):
                dispatch_x(0, e)()
            dispatch_x(1, 1)()
        with jax.named_scope("gate"):
            small[2].wait()
            prob, chosen, gate = gate_of(x_ref[...], wgt_ref[...], hot)
            prob_ref[...], chosen_ref[...] = prob, chosen

        def forward(g, e):
            rows = far if g else near
            if g == 0:
                loads["i", e].wait()
            xg = xs_ref[e, rows, :]
            step = d_ff // 2
            for c in range(2):
                cols = slice(c * step, (c + 1) * step)
                a = mm(xg, wi[e, :, cols])
                t = jnp.tanh(GELU_C * (a + GELU_K * (a * a * a)))
                cdf = 0.5 * (1.0 + t)
                h_ref[e, rows, cols] = (a * cdf).astype(BF16)
                gp[e, rows, cols] = cdf + (0.5 * a) * (1.0 - t * t) * (GELU_C + (3.0 * GELU_C * GELU_K) * (a * a))
            if g == 0:
                loads["o", e].wait()
            ypeer[g, e] = mm(h_ref[e, rows, :], wo[e, :, theirs])
            yc[g, e] = send(ypeer.at[g, e], yrecv.at[g, e], y_s.at[g, e], y_r.at[g, e], {"tp": tp_peer})

        def backward(rows, e):
            dyg = dys_ref[e, rows, :]
            step = d_ff // 4
            for c in range(4):
                cols = slice(c * step, (c + 1) * step)
                dh = mm(dyg, wo[e, cols, :], CONTRACT_LAST)
                da_ref[e, rows, cols] = (dh * gp[e, rows, cols]).astype(BF16)
            dag = da_ref[e, rows, :]
            speer_ref[e, rows, :] = mm(dag, wi[e, theirs, :], CONTRACT_LAST)
            sown_ref[e, rows, :] = mm(dag, wi[e, mine, :], CONTRACT_LAST)

        def y_blocks(g):
            for e in range(2):
                yc[g, e].wait()
            both = [yown[e, far if g else near, :] + yrecv[g, e] for e in range(2)]
            return [jnp.concatenate([both[e][q * cap:(q + 1) * cap] for e in range(2)], axis=0).astype(BF16) for q in range(2)]

        with jax.named_scope("wait_near"):
            xc[1, 0].wait()
        with jax.named_scope("fwd#g=0#e=0"):
            forward(0, 0)
        with jax.named_scope("dispatch_dy"):
            small[3].wait()
            dy = (gate * gy_ref[...].astype(F32)).astype(BF16)
            for g in (1, 0):
                for e in range(2):
                    dispatch(dy, g, e, dysend, dys_ref, d_s, d_r, dc)()
        with jax.named_scope("fwd#g=0#e=1"):
            xc[1, 1].wait()
            forward(0, 1)
        with jax.named_scope("picks"):
            picks_ref[...] = pick(slot, [peers[r] * blk for r in range(4)], blk)
        with jax.named_scope("wait_far#e=0"):
            xc[2, 0].wait()
            xc[3, 0].wait()
        with jax.named_scope("fwd#g=1#e=0"):
            forward(1, 0)
        with jax.named_scope("bwd#near#e=0"):
            dc[1, 0].wait()
            backward(near, 0)
        with jax.named_scope("wait_far#e=1"):
            xc[2, 1].wait()
            xc[3, 1].wait()
        with jax.named_scope("fwd#g=1#e=1"):
            forward(1, 1)
        with jax.named_scope("yown"):
            for e in range(2):
                yown[e] = mm(h_ref[e], wo[e, :, mine])
        with jax.named_scope("y_near"):
            kept, away = y_blocks(0)
            ynear_ref[near, :] = kept
            yback[...] = away
            bc = send(yback, yland, b_s, b_r, {"ep": peers[1]})
        with jax.named_scope("wait_dy#e=0"):
            dc[2, 0].wait()
            dc[3, 0].wait()
        with jax.named_scope("bwd#far#e=0"):
            backward(far, 0)
        with jax.named_scope("wait_dy#e=1"):
            for r in (1, 2, 3):
                dc[r, 1].wait()
        with jax.named_scope("bwd#e=1"):
            backward(whole, 1)
        with jax.named_scope("y_far"):
            bc.wait()
            ynear_ref[far, :] = yland[...]
            yfar0_ref[...], yfar1_ref[...] = y_blocks(1)

    return front


def grads_kernel(h_ref, dys_ref, xs_ref, da_ref, dwi_ref, dwo_ref):
    dwo_ref[0] = mm(h_ref[0], dys_ref[0], CONTRACT_FIRST)
    dwi_ref[0] = mm(xs_ref[0], da_ref[0], CONTRACT_FIRST)


def make_back(cap):
    blk = 2 * cap

    def back(x_ref, gy_ref, wgt_ref, picks_ref, prob_ref, chosen_ref, ynear_ref, yfar0_ref, yfar1_ref, sown_ref, srecv_ref,
             out_ref, dx_ref, dwgt_ref,
             ysend, yland, sback, sland, stsend, stland, dwg,
             y_s, y_r, b_s, b_r, x_s, x_r, w_s, w_r):
        tp = lax.axis_index("tp")
        ep = lax.axis_index("ep")
        tp_peer = 1 - tp
        peers = ep_partners()
        half = x_ref.shape[1] // 2
        mine = pl.ds(pl.multiple_of(tp * half, half), half)
        theirs = pl.ds(pl.multiple_of(tp_peer * half, half), half)
        with jax.named_scope("enter"):
            barrier = enter(peers, tp_peer)
            picks = picks_ref[...]
            y_rows = jnp.concatenate([ynear_ref[...], yfar0_ref[...], yfar1_ref[...]], axis=0)
            ysend[...] = mm(picks, y_rows, CONTRACT_FIRST).astype(BF16)
            pl.semaphore_wait(barrier, 4)
            yc = send(ysend, yland, y_s, y_r, {"tp": tp_peer})
        with jax.named_scope("s_back"):
            bc = {}
            for g in (1, 0):
                rows = slice(g * blk, (g + 1) * blk)
                both = [sown_ref[e, rows, :] + srecv_ref[e, rows, :] for e in range(2)]
                for q in range(2):
                    r = 2 * g + q
                    block = jnp.concatenate([both[e][q * cap:(q + 1) * cap] for e in range(2)], axis=0).astype(BF16)
                    if r == 0:
                        sland[0:blk, :] = block
                    else:
                        sback[r - 1] = block
                        bc[r] = send(sback.at[r - 1], sland.at[r * blk:(r + 1) * blk, :], b_s.at[r - 1], b_r.at[r - 1],
                                     {"ep": peers[r]})
        with jax.named_scope("gate"):
            x = x_ref[...]
            prob, chosen = prob_ref[...], chosen_ref[...]
            gate = jnp.sum(chosen * prob, axis=1, keepdims=True)
            y_mine = ysend[...].astype(F32)
            out_ref[:, mine] = (gate * y_mine).astype(BF16)
            dgate = jnp.sum(gy_ref[:, mine].astype(F32) * y_mine, axis=1, keepdims=True)
        with jax.named_scope("s_wait"):
            for r in (1, 2, 3):
                bc[r].wait()
            stsend[...] = mm(picks, sland[...], CONTRACT_FIRST).astype(BF16)
            xc = send(stsend, stland, x_s, x_r, {"tp": tp_peer})
        with jax.named_scope("y_wait"):
            yc.wait()
        with jax.named_scope("router"):
            y_theirs = yland[...].astype(F32)
            out_ref[:, theirs] = (gate * y_theirs).astype(BF16)
            dgate = dgate + jnp.sum(gy_ref[:, theirs].astype(F32) * y_theirs, axis=1, keepdims=True)
            dlogits = (dgate * prob * (chosen - gate)).astype(BF16)
            dwg[ep] = mm(dlogits, x, CONTRACT_FIRST)
            wc = {}
            for r in (2, 3, 1):
                wc[r] = send(dwg.at[ep], dwg.at[ep], w_s.at[r - 1], w_r.at[r - 1], {"ep": peers[r]})
            dx_ref[:, mine] = (stsend[...].astype(F32) + mm(dlogits, wgt_ref[:, mine])).astype(BF16)
            rgrad = mm(dlogits, wgt_ref[:, theirs])
        with jax.named_scope("dwg"):
            for r in (1, 2, 3):
                wc[r].wait()
            dwgt_ref[...] = (dwg[0] + dwg[1]) + (dwg[2] + dwg[3])
        with jax.named_scope("dx_wait"):
            xc.wait()
        with jax.named_scope("dx"):
            dx_ref[:, theirs] = (stland[...].astype(F32) + rgrad).astype(BF16)

    return back


def finish(out_ref, dx_ref, dwgt_ref, out_hbm, dx_hbm, dwgt_hbm, sem):
    copies = [pltpu.make_async_copy(src, dst, sem.at[k]) for k, (src, dst) in enumerate(
        ((out_ref, out_hbm), (dx_ref, dx_hbm), (dwgt_ref, dwgt_hbm)))]
    for copy in copies:
        copy.start()
    for copy in copies:
        copy.wait()


def solution(mesh):
    row_spec = P(("dp", "ep"), None)
    vmem = pl.BlockSpec(memory_space=pltpu.VMEM)
    hbm = pl.BlockSpec(memory_space=pltpu.HBM)

    def local_block(tokens, grad_out, w_router, w_in, w_out, expert_ids):
        n, d_model = tokens.shape
        n_experts = w_router.shape[1]
        le, _, d_ff = w_in.shape
        capacity = (6 * n + 5 * n_experts - 1) // (5 * n_experts)
        cap = -(-capacity // 8) * 8
        blk = le * cap
        rows = 4 * cap
        half = d_model // 2
        wgt = w_router.T
        idx_row = expert_ids.reshape(1, n)
        sds = jax.ShapeDtypeStruct
        dma = pltpu.SemaphoreType.DMA

        h, da, xs, dys, speer, sown, ynear, yfar0, yfar1, picks, prob, chosen = pl.pallas_call(
            make_front(n_experts, capacity, cap),
            out_shape=(sds((le, rows, d_ff), BF16), sds((le, rows, d_ff), BF16), sds((le, rows, d_model), BF16),
                       sds((le, rows, d_model), BF16), sds((le, rows, half), F32), sds((le, rows, half), F32),
                       sds((2 * blk, half), BF16), sds((blk, half), BF16), sds((blk, half), BF16),
                       sds((4 * blk, n), BF16), sds((n, n_experts), F32), sds((n, n_experts), F32)),
            in_specs=[hbm] * 6,
            out_specs=(vmem,) * 12,
            scratch_shapes=[
                pltpu.VMEM((n, d_model), BF16), pltpu.VMEM((n, d_model), BF16), pltpu.VMEM((n_experts, d_model), BF16),
                pltpu.VMEM((1, n), jnp.int32),
                pltpu.VMEM((le, d_model, d_ff), BF16), pltpu.VMEM((le, d_ff, d_model), BF16),
                pltpu.VMEM((3, le, cap, d_model), BF16), pltpu.VMEM((3, le, cap, d_model), BF16),
                pltpu.VMEM((le, rows, d_ff), F32),
                pltpu.VMEM((2, le, blk, half), F32), pltpu.VMEM((le, rows, half), F32), pltpu.VMEM((2, le, blk, half), F32),
                pltpu.VMEM((blk, half), BF16), pltpu.VMEM((blk, half), BF16),
                dma((4,)), dma((2, le)), dma((3, le)), dma((3, le)), dma((3, le)), dma((3, le)), dma((2, le)), dma((2, le)), dma, dma,
            ],
            compiler_params=pltpu.CompilerParams(collective_id=0, has_side_effects=True, vmem_limit_bytes=40 * 2**20),
            name="front",
        )(*[pltpu.with_memory_space_constraint(v, pltpu.HBM) for v in (tokens, grad_out, wgt, idx_row, w_in, w_out)])

        srecv = lax.ppermute(speer, "tp", [(0, 1), (1, 0)])
        yland0 = lax.ppermute(yfar0, "ep", [(0, 2), (2, 0), (1, 3), (3, 1)])
        yland1 = lax.ppermute(yfar1, "ep", [(0, 3), (3, 0), (1, 2), (2, 1)])

        steps = 4
        hs, ms = d_ff // steps, d_model // steps
        dwi, dwo = pl.pallas_call(
            grads_kernel,
            grid=(le, steps),
            out_shape=(sds((le, d_model, d_ff), F32), sds((le, d_ff, d_model), F32)),
            in_specs=[pl.BlockSpec((1, rows, hs), lambda e, c: (e, 0, c)), pl.BlockSpec((1, rows, d_model), lambda e, c: (e, 0, 0)),
                      pl.BlockSpec((1, rows, ms), lambda e, c: (e, 0, c)), pl.BlockSpec((1, rows, d_ff), lambda e, c: (e, 0, 0))],
            out_specs=(pl.BlockSpec((1, ms, d_ff), lambda e, c: (e, c, 0)), pl.BlockSpec((1, hs, d_model), lambda e, c: (e, c, 0))),
            cost_estimate=pl.CostEstimate(flops=4 * le * rows * d_model * d_ff, bytes_accessed=8 * le * d_model * d_ff,
                                          transcendentals=0),
            compiler_params=pltpu.CompilerParams(vmem_limit_bytes=24 * 2**20),
            name="weight_grads",
        )(h, dys, xs, da)

        ends = (sds((n, d_model), BF16), sds((n, d_model), BF16), sds((n_experts, d_model), F32))
        parts = pl.pallas_call(
            make_back(cap),
            out_shape=ends,
            in_specs=[vmem] * 11,
            out_specs=(vmem,) * 3,
            scratch_shapes=[
                pltpu.VMEM((n, half), BF16), pltpu.VMEM((n, half), BF16),
                pltpu.VMEM((3, blk, half), BF16), pltpu.VMEM((4 * blk, half), BF16),
                pltpu.VMEM((n, half), BF16), pltpu.VMEM((n, half), BF16),
                pltpu.VMEM((4, n_experts, d_model), F32),
                dma, dma, dma((3,)), dma((3,)), dma, dma, dma((3,)), dma((3,)),
            ],
            compiler_params=pltpu.CompilerParams(collective_id=1, has_side_effects=True, vmem_limit_bytes=24 * 2**20),
            name="back",
        )(tokens, grad_out, wgt, picks, prob, chosen, ynear, yland0, yland1, sown, srecv)
        out, dx, dwgt = pl.pallas_call(
            finish, out_shape=ends, in_specs=[vmem] * 3, out_specs=(hbm,) * 3, scratch_shapes=[dma((3,))],
            compiler_params=pltpu.CompilerParams(vmem_limit_bytes=8 * 2**20), name="finish",
        )(*parts)
        return out, dx, dwi, dwo, dwgt.T

    in_specs = (row_spec, row_spec, P(None, None), P("ep", None, "tp"), P("ep", "tp", None), P(("dp", "ep")))
    out_specs = (row_spec, row_spec, P(("dp", "ep"), None, "tp"), P(("dp", "ep"), "tp", None), P("dp", None))
    return jax.shard_map(local_block, mesh=mesh, in_specs=in_specs, out_specs=out_specs, check_vma=False)
```

```python
import jax
import jax.numpy as jnp
from jax import lax
from jax.experimental import pallas as pl
from jax.experimental.pallas import tpu as pltpu
from jax.sharding import PartitionSpec as P

MESH = pl.DeviceIdType.MESH
F32, BF16 = jnp.float32, jnp.bfloat16
CONTRACT_LAST = (((1,), (1,)), ((), ()))
CONTRACT_FIRST = (((0,), (0,)), ((), ()))
GELU_C = 0.7978845608028654
GELU_K = 0.044715


def mm(a, b, dims=(((1,), (0,)), ((), ()))):
    return lax.dot_general(a, b, dims, preferred_element_type=F32)


def ep_partners():
    ep = lax.axis_index("ep")
    cx, cc = ep // 2, ep % 2
    return [ep, 2 * cx + (1 - cc), 2 * (1 - cx) + cc, 2 * (1 - cx) + (1 - cc)]


def route(idx_row, capacity, n_experts, stride):
    n = idx_row.shape[1]
    expert = lax.broadcasted_iota(jnp.int32, (n_experts, n), 0)
    hot = jnp.where(expert == idx_row, 1.0, 0.0)
    earlier = lax.broadcasted_iota(jnp.int32, (n, n), 0)
    later = lax.broadcasted_iota(jnp.int32, (n, n), 1)
    upto = jnp.where(earlier <= later, 1.0, 0.0).astype(BF16)
    count = mm(hot.astype(BF16), upto)
    position = jnp.sum(hot * count, axis=0, keepdims=True) - 1.0
    slot = jnp.where(position < capacity, idx_row.astype(F32) * stride + position, -1.0)
    return hot, slot


def pick(slot, firsts, rows):
    n = slot.shape[1]
    row = lax.broadcasted_iota(jnp.int32, (rows, n), 0)
    parts = [jnp.where((row + first).astype(F32) == slot, 1.0, 0.0) for first in firsts]
    return jnp.concatenate(parts, axis=0).astype(BF16)


def gate_of(x, wgt, hot):
    n_experts = hot.shape[0]
    logits = mm(x, wgt, CONTRACT_LAST)
    e = jnp.exp(logits - jnp.max(logits, axis=1, keepdims=True))
    prob = e / jnp.sum(e, axis=1, keepdims=True)
    eye = jnp.where(
        lax.broadcasted_iota(jnp.int32, (n_experts, n_experts), 0)
        == lax.broadcasted_iota(jnp.int32, (n_experts, n_experts), 1), 1.0, 0.0)
    chosen = mm(hot.astype(BF16), eye.astype(BF16), CONTRACT_FIRST)
    gate = jnp.sum(chosen * prob, axis=1, keepdims=True)
    return prob, chosen, gate


def enter(peers, tp_peer):
    barrier = pltpu.get_barrier_semaphore()
    for r in (1, 2, 3):
        pl.semaphore_signal(barrier, inc=1, device_id={"ep": peers[r]}, device_id_type=MESH)
    pl.semaphore_signal(barrier, inc=1, device_id={"tp": tp_peer}, device_id_type=MESH)
    return barrier


def send(src, dst, ssem, rsem, device):
    copy = pltpu.make_async_remote_copy(
        src_ref=src, dst_ref=dst, send_sem=ssem, recv_sem=rsem, device_id=device, device_id_type=MESH)
    copy.start()
    return copy


def make_front(n_experts, capacity, cap):
    blk = 2 * cap

    def front(x_hbm, gy_hbm, wgt_hbm, idx_hbm, wi_hbm, wo_hbm,
              h_ref, da_ref, xs_ref, dys_ref, sfar_ref, snear_ref, sfar_own_ref, snear_own_ref, ynear_ref, yfar0_ref, yfar1_ref,
              picks_ref, prob_ref, chosen_ref,
              x_ref, gy_ref, wgt_ref, idx_ref, wi, wo, xsend, dysend, gp,
              ypeer, yown, yrecv, yback, yland,
              in_sem, wsem, x_s, x_r, d_s, d_r, y_s, y_r, b_s, b_r):
        tp = lax.axis_index("tp")
        tp_peer = 1 - tp
        peers = ep_partners()
        half = x_ref.shape[1] // 2
        mine = pl.ds(pl.multiple_of(tp * half, half), half)
        theirs = pl.ds(pl.multiple_of(tp_peer * half, half), half)
        d_ff = wi.shape[2]
        near, far, whole = slice(0, blk), slice(blk, 2 * blk), slice(0, 2 * blk)
        with jax.named_scope("enter"):
            small = [pltpu.make_async_copy(src, dst, in_sem.at[k]) for k, (src, dst) in enumerate(
                ((idx_hbm, idx_ref), (x_hbm, x_ref), (wgt_hbm, wgt_ref), (gy_hbm, gy_ref)))]
            for copy in small:
                copy.start()
            barrier = enter(peers, tp_peer)
            loads = {}
            for e in range(2):
                loads["i", e] = pltpu.make_async_copy(wi_hbm.at[e], wi.at[e], wsem.at[0, e])
                loads["o", e] = pltpu.make_async_copy(wo_hbm.at[e], wo.at[e], wsem.at[1, e])
            for e in range(2):
                loads["i", e].start()
                loads["o", e].start()

        xc, dc, yc = {}, {}, {}

        def dispatch(v, g, e, buf, rows_ref, ssem, rsem, made):
            first = [peers[2 * g + q] * blk + e * cap for q in range(2)]
            rows = mm(pick(slot, first, cap), v)
            for q in range(2):
                r = 2 * g + q
                part = rows[q * cap:(q + 1) * cap].astype(BF16)
                if r == 0:
                    rows_ref[e, 0:cap, :] = part
                else:
                    buf[r - 1, e] = part
            return lambda: [made.__setitem__((r, e), send(
                buf.at[r - 1, e], rows_ref.at[e, r * cap:(r + 1) * cap, :], ssem.at[r - 1, e], rsem.at[r - 1, e],
                {"ep": peers[r]})) for r in (2 * g, 2 * g + 1) if r]

        def dispatch_x(g, e):
            return dispatch(x_ref[...], g, e, xsend, xs_ref, x_s, x_r, xc)

        with jax.named_scope("route"):
            small[0].wait()
            hot, slot = route(idx_ref[...], capacity, n_experts, cap)
            small[1].wait()
            go = dispatch_x(0, 0)
        with jax.named_scope("barrier"):
            pl.semaphore_wait(barrier, 4)
        with jax.named_scope("dispatch_x"):
            go()
            dispatch_x(1, 0)()
            dispatch_x(0, 1)()
            dispatch_x(1, 1)()
        with jax.named_scope("gate"):
            small[2].wait()
            prob, chosen, gate = gate_of(x_ref[...], wgt_ref[...], hot)
            prob_ref[...], chosen_ref[...] = prob, chosen

        def forward(g, e):
            rows = far if g else near
            if g == 0:
                loads["i", e].wait()
            xg = xs_ref[e, rows, :]
            step = d_ff // 2
            for c in range(2):
                cols = slice(c * step, (c + 1) * step)
                a = mm(xg, wi[e, :, cols])
                t = jnp.tanh(GELU_C * (a + GELU_K * (a * a * a)))
                cdf = 0.5 * (1.0 + t)
                h_ref[e, rows, cols] = (a * cdf).astype(BF16)
                gp[e, rows, cols] = cdf + (0.5 * a) * (1.0 - t * t) * (GELU_C + (3.0 * GELU_C * GELU_K) * (a * a))
            if g == 0:
                loads["o", e].wait()
            ypeer[g, e] = mm(h_ref[e, rows, :], wo[e, :, theirs])
            yc[g, e] = send(ypeer.at[g, e], yrecv.at[g, e], y_s.at[g, e], y_r.at[g, e], {"tp": tp_peer})

        def backward(rows, e):
            dyg = dys_ref[e, rows, :]
            step = d_ff // 4
            for c in range(4):
                cols = slice(c * step, (c + 1) * step)
                dh = mm(dyg, wo[e, cols, :], CONTRACT_LAST)
                da_ref[e, rows, cols] = (dh * gp[e, rows, cols]).astype(BF16)
            dag = da_ref[e, rows, :]
            for cols, near_ref, far_ref in ((theirs, snear_ref, sfar_ref), (mine, snear_own_ref, sfar_own_ref)):
                part = mm(dag, wi[e, cols, :], CONTRACT_LAST)
                if rows is not far:
                    near_ref[e] = part[0:blk]
                if rows is not near:
                    far_ref[e] = part[part.shape[0] - blk:]

        def y_blocks(g):
            for e in range(2):
                yc[g, e].wait()
            both = [yown[e, far if g else near, :] + yrecv[g, e] for e in range(2)]
            return [jnp.concatenate([both[e][q * cap:(q + 1) * cap] for e in range(2)], axis=0).astype(BF16) for q in range(2)]

        with jax.named_scope("wait_near"):
            xc[1, 0].wait()
        with jax.named_scope("fwd#g=0#e=0"):
            forward(0, 0)
        with jax.named_scope("dispatch_dy"):
            small[3].wait()
            dy = (gate * gy_ref[...].astype(F32)).astype(BF16)
            for g in (1, 0):
                for e in range(2):
                    dispatch(dy, g, e, dysend, dys_ref, d_s, d_r, dc)()
        with jax.named_scope("fwd#g=0#e=1"):
            xc[1, 1].wait()
            forward(0, 1)
        with jax.named_scope("picks"):
            picks_ref[...] = pick(slot, [peers[r] * blk for r in range(4)], blk)
        with jax.named_scope("wait_far#e=0"):
            xc[2, 0].wait()
            xc[3, 0].wait()
        with jax.named_scope("fwd#g=1#e=0"):
            forward(1, 0)
        with jax.named_scope("bwd#near#e=0"):
            dc[1, 0].wait()
            backward(near, 0)
        with jax.named_scope("wait_far#e=1"):
            xc[2, 1].wait()
            xc[3, 1].wait()
        with jax.named_scope("fwd#g=1#e=1"):
            forward(1, 1)
        with jax.named_scope("yown"):
            for e in range(2):
                yown[e] = mm(h_ref[e], wo[e, :, mine])
        with jax.named_scope("y_near"):
            kept, away = y_blocks(0)
            ynear_ref[near, :] = kept
            yback[...] = away
            bc = send(yback, yland, b_s, b_r, {"ep": peers[1]})
        with jax.named_scope("wait_dy#e=0"):
            dc[2, 0].wait()
            dc[3, 0].wait()
        with jax.named_scope("bwd#far#e=0"):
            backward(far, 0)
        with jax.named_scope("wait_dy#e=1"):
            for r in (1, 2, 3):
                dc[r, 1].wait()
        with jax.named_scope("bwd#e=1"):
            backward(whole, 1)
        with jax.named_scope("y_far"):
            bc.wait()
            ynear_ref[far, :] = yland[...]
            yfar0_ref[...], yfar1_ref[...] = y_blocks(1)

    return front


def make_grad(steps):
    def grad(left_ref, right_ref, after_ref, out_hbm, done_ref, buf, sem):
        n_exp, _, width = left_ref.shape
        piece = width // steps
        copies = []
        for e in range(n_exp):
            right = right_ref[e]
            for c in range(steps):
                rows = slice(c * piece, (c + 1) * piece)
                buf[e, rows, :] = mm(left_ref[e, :, rows], right, CONTRACT_FIRST)
                copies.append(pltpu.make_async_copy(buf.at[e, rows, :], out_hbm.at[e, rows, :], sem.at[e, c]))
                copies[-1].start()
        done_ref[...] = jnp.zeros_like(done_ref)
        for copy in copies:
            copy.wait()

    return grad


def y_tokens(picks_ref, ynear_ref, yfar0_ref, yfar1_ref, after_ref, y_ref):
    rows = jnp.concatenate([ynear_ref[...], yfar0_ref[...], yfar1_ref[...]], axis=0)
    y_ref[...] = mm(picks_ref[...], rows, CONTRACT_FIRST).astype(BF16)


def make_blocks(cap):
    def s_blocks(own_ref, recv_ref, out_ref):
        both = [own_ref[e] + recv_ref[e] for e in range(2)]
        out_ref[...] = jnp.concatenate(
            [both[e][q * cap:(q + 1) * cap] for q in range(2) for e in range(2)], axis=0).astype(BF16)

    return s_blocks


def make_back(cap):
    blk = 2 * cap

    def back(x_ref, gy_ref, wgt_ref, picks_ref, prob_ref, chosen_ref, ymine_ref, sfar_ref, sown_ref, srecv_ref,
             dx_ref, dwgt_ref,
             sback, sland, stsend, stland, gsend, gland, dwg,
             b_s, b_r, x_s, x_r, g_s, g_r, w_s, w_r):
        tp = lax.axis_index("tp")
        ep = lax.axis_index("ep")
        tp_peer = 1 - tp
        peers = ep_partners()
        n, d_model = x_ref.shape
        half = d_model // 2
        mine = pl.ds(pl.multiple_of(tp * half, half), half)
        theirs = pl.ds(pl.multiple_of(tp_peer * half, half), half)
        with jax.named_scope("enter"):
            barrier = enter(peers, tp_peer)
            both = [sown_ref[e] + srecv_ref[e] for e in range(2)]
            kept, away = [jnp.concatenate([both[e][q * cap:(q + 1) * cap] for e in range(2)], axis=0).astype(BF16)
                          for q in range(2)]
            sback[...] = away
            dgate = jnp.sum(gy_ref[:, mine].astype(F32) * ymine_ref[...].astype(F32), axis=1, keepdims=True)
            gsend[...] = jnp.broadcast_to(dgate, (n, 128)).T[0:8]
            pl.semaphore_wait(barrier, 4)
        with jax.named_scope("s_back"):
            bc = [send(sback, sland.at[0], b_s.at[0], b_r.at[0], {"ep": peers[1]}),
                  send(sfar_ref.at[blk:2 * blk, :], sland.at[1], b_s.at[1], b_r.at[1], {"ep": peers[1]})]
            gc = send(gsend, gland, g_s, g_r, {"tp": tp_peer})
        with jax.named_scope("s_wait"):
            for copy in bc:
                copy.wait()
        with jax.named_scope("s_tok"):
            s_rows = jnp.concatenate([kept, sland[0], sfar_ref[0:blk, :], sland[1]], axis=0)
            stsend[...] = mm(picks_ref[...], s_rows, CONTRACT_FIRST).astype(BF16)
            xc = send(stsend, stland, x_s, x_r, {"tp": tp_peer})
        with jax.named_scope("gate_wait"):
            prob, chosen = prob_ref[...], chosen_ref[...]
            gate = jnp.sum(chosen * prob, axis=1, keepdims=True)
            gc.wait()
        with jax.named_scope("router"):
            dgate = dgate + jnp.broadcast_to(gland[0:1, :], (128, n)).T[:, 0:1]
            dlogits = (dgate * prob * (chosen - gate)).astype(BF16)
            dwg[ep] = mm(dlogits, x_ref[...], CONTRACT_FIRST)
            wc = {}
            for r in (2, 3, 1):
                wc[r] = send(dwg.at[ep], dwg.at[ep], w_s.at[r - 1], w_r.at[r - 1], {"ep": peers[r]})
            dx_ref[:, mine] = (stsend[...].astype(F32) + mm(dlogits, wgt_ref[:, mine])).astype(BF16)
            rgrad = mm(dlogits, wgt_ref[:, theirs])
        with jax.named_scope("dwg"):
            for r in (1, 2, 3):
                wc[r].wait()
            dwgt_ref[...] = (dwg[0] + dwg[1]) + (dwg[2] + dwg[3])
        with jax.named_scope("dx_wait"):
            xc.wait()
        with jax.named_scope("dx"):
            dx_ref[:, theirs] = (stland[...].astype(F32) + rgrad).astype(BF16)

    return back


def finish(dx_ref, dwgt_ref, ymine_ref, ytheirs_ref, prob_ref, chosen_ref, out_hbm, dx_hbm, dwgt_hbm, out_ref, sem):
    half = ymine_ref.shape[1]
    copies = [pltpu.make_async_copy(src, dst, sem.at[k]) for k, (src, dst) in enumerate(
        ((dx_ref, dx_hbm), (dwgt_ref, dwgt_hbm), (out_ref, out_hbm)))]
    copies[0].start()
    copies[1].start()
    tp = lax.axis_index("tp")
    gate = jnp.sum(chosen_ref[...] * prob_ref[...], axis=1, keepdims=True)
    for side, ref in ((tp, ymine_ref), (1 - tp, ytheirs_ref)):
        out_ref[:, pl.ds(pl.multiple_of(side * half, half), half)] = (gate * ref[...].astype(F32)).astype(BF16)
    copies[2].start()
    for copy in copies:
        copy.wait()


def solution(mesh):
    row_spec = P(("dp", "ep"), None)
    vmem = pl.BlockSpec(memory_space=pltpu.VMEM)
    hbm = pl.BlockSpec(memory_space=pltpu.HBM)

    def local_block(tokens, grad_out, w_router, w_in, w_out, expert_ids):
        n, d_model = tokens.shape
        n_experts = w_router.shape[1]
        le, _, d_ff = w_in.shape
        capacity = (6 * n + 5 * n_experts - 1) // (5 * n_experts)
        cap = -(-capacity // 8) * 8
        blk = le * cap
        rows = 4 * cap
        half = d_model // 2
        wgt = w_router.T
        idx_row = expert_ids.reshape(1, n)
        sds = jax.ShapeDtypeStruct
        dma = pltpu.SemaphoreType.DMA

        h, da, xs, dys, sfar, snear, sfar_own, snear_own, ynear, yfar0, yfar1, picks, prob, chosen = pl.pallas_call(
            make_front(n_experts, capacity, cap),
            out_shape=(sds((le, rows, d_ff), BF16), sds((le, rows, d_ff), BF16), sds((le, rows, d_model), BF16),
                       sds((le, rows, d_model), BF16), *[sds((le, blk, half), F32)] * 4,
                       sds((2 * blk, half), BF16), sds((blk, half), BF16), sds((blk, half), BF16),
                       sds((4 * blk, n), BF16), sds((n, n_experts), F32), sds((n, n_experts), F32)),
            in_specs=[hbm] * 6,
            out_specs=(vmem,) * 14,
            scratch_shapes=[
                pltpu.VMEM((n, d_model), BF16), pltpu.VMEM((n, d_model), BF16), pltpu.VMEM((n_experts, d_model), BF16),
                pltpu.VMEM((1, n), jnp.int32),
                pltpu.VMEM((le, d_model, d_ff), BF16), pltpu.VMEM((le, d_ff, d_model), BF16),
                pltpu.VMEM((3, le, cap, d_model), BF16), pltpu.VMEM((3, le, cap, d_model), BF16),
                pltpu.VMEM((le, rows, d_ff), F32),
                pltpu.VMEM((2, le, blk, half), F32), pltpu.VMEM((le, rows, half), F32), pltpu.VMEM((2, le, blk, half), F32),
                pltpu.VMEM((blk, half), BF16), pltpu.VMEM((blk, half), BF16),
                dma((4,)), dma((2, le)), dma((3, le)), dma((3, le)), dma((3, le)), dma((3, le)), dma((2, le)), dma((2, le)), dma, dma,
            ],
            compiler_params=pltpu.CompilerParams(collective_id=0, has_side_effects=True, vmem_limit_bytes=40 * 2**20),
            name="front",
        )(*[pltpu.with_memory_space_constraint(v, pltpu.HBM) for v in (tokens, grad_out, wgt, idx_row, w_in, w_out)])

        swap = [(0, 1), (1, 0)]
        across, diagonal = [(0, 2), (2, 0), (1, 3), (3, 1)], [(0, 3), (3, 0), (1, 2), (2, 1)]
        sfar_recv = lax.ppermute(sfar, "tp", swap)
        snear_recv = lax.ppermute(snear, "tp", swap)
        yland0 = lax.ppermute(yfar0, "ep", across)
        yland1 = lax.ppermute(yfar1, "ep", diagonal)

        def weight_grad(left, right, after, name):
            steps = 8
            shape = (le, left.shape[2], right.shape[2])
            return pl.pallas_call(
                make_grad(steps),
                out_shape=(sds(shape, F32), sds((8, 128), F32)),
                in_specs=[vmem] * 3, out_specs=(hbm, vmem),
                scratch_shapes=[pltpu.VMEM(shape, F32), dma((le, steps))],
                cost_estimate=pl.CostEstimate(flops=2 * rows * shape[0] * shape[1] * shape[2],
                                              bytes_accessed=4 * shape[0] * shape[1] * shape[2], transcendentals=0),
                compiler_params=pltpu.CompilerParams(vmem_limit_bytes=24 * 2**20),
                name=name,
            )(left, right, after)

        dwo, done = weight_grad(h, dys, ynear, "grad_out")
        ymine = pl.pallas_call(
            y_tokens, out_shape=sds((n, half), BF16), in_specs=[vmem] * 5, out_specs=vmem,
            compiler_params=pltpu.CompilerParams(vmem_limit_bytes=8 * 2**20), name="y_tokens",
        )(picks, ynear, yland0, yland1, done)
        ytheirs = lax.ppermute(ymine, "tp", swap)
        sblocks = pl.pallas_call(
            make_blocks(cap), out_shape=sds((2 * blk, half), BF16), in_specs=[vmem] * 2, out_specs=vmem,
            compiler_params=pltpu.CompilerParams(vmem_limit_bytes=8 * 2**20), name="s_blocks",
        )(sfar_own, sfar_recv)
        sfar_land = lax.ppermute(sblocks, "ep", across)
        dwi, _ = weight_grad(xs, da, sblocks, "grad_in")

        dx_v, dwgt_v = pl.pallas_call(
            make_back(cap),
            out_shape=(sds((n, d_model), BF16), sds((n_experts, d_model), F32)),
            in_specs=[vmem] * 10,
            out_specs=(vmem,) * 2,
            scratch_shapes=[
                pltpu.VMEM((blk, half), BF16), pltpu.VMEM((2, blk, half), BF16),
                pltpu.VMEM((n, half), BF16), pltpu.VMEM((n, half), BF16),
                pltpu.VMEM((8, n), F32), pltpu.VMEM((8, n), F32),
                pltpu.VMEM((4, n_experts, d_model), F32),
                dma((2,)), dma((2,)), dma, dma, dma, dma, dma((3,)), dma((3,)),
            ],
            compiler_params=pltpu.CompilerParams(collective_id=1, has_side_effects=True, vmem_limit_bytes=24 * 2**20),
            name="back",
        )(tokens, grad_out, wgt, picks, prob, chosen, ymine, sfar_land, snear_own, snear_recv)
        out, dx, dwgt = pl.pallas_call(
            finish, out_shape=(sds((n, d_model), BF16), sds((n, d_model), BF16), sds((n_experts, d_model), F32)),
            in_specs=[vmem] * 6, out_specs=(hbm,) * 3,
            scratch_shapes=[pltpu.VMEM((n, d_model), BF16), dma((3,))],
            compiler_params=pltpu.CompilerParams(vmem_limit_bytes=8 * 2**20), name="finish",
        )(dx_v, dwgt_v, ymine, ytheirs, prob, chosen)
        return out, dx, dwi, dwo, dwgt.T

    in_specs = (row_spec, row_spec, P(None, None), P("ep", None, "tp"), P("ep", "tp", None), P(("dp", "ep")))
    out_specs = (row_spec, row_spec, P(("dp", "ep"), None, "tp"), P(("dp", "ep"), "tp", None), P("dp", None))
    return jax.shard_map(local_block, mesh=mesh, in_specs=in_specs, out_specs=out_specs, check_vma=False)
```

```python
import jax
import jax.numpy as jnp
from jax import lax
from jax.experimental import pallas as pl
from jax.experimental.pallas import tpu as pltpu
from jax.sharding import PartitionSpec as P

MESH = pl.DeviceIdType.MESH
F32, BF16 = jnp.float32, jnp.bfloat16
CONTRACT_LAST = (((1,), (1,)), ((), ()))
CONTRACT_FIRST = (((0,), (0,)), ((), ()))
GELU_C = 0.7978845608028654
GELU_K = 0.044715


def mm(a, b, dims=(((1,), (0,)), ((), ()))):
    return lax.dot_general(a, b, dims, preferred_element_type=F32)


def ep_partners():
    ep = lax.axis_index("ep")
    cx, cc = ep // 2, ep % 2
    return [ep, 2 * cx + (1 - cc), 2 * (1 - cx) + cc, 2 * (1 - cx) + (1 - cc)]


def route(idx_row, capacity, n_experts, stride):
    n = idx_row.shape[1]
    expert = lax.broadcasted_iota(jnp.int32, (n_experts, n), 0)
    hot = jnp.where(expert == idx_row, 1.0, 0.0)
    earlier = lax.broadcasted_iota(jnp.int32, (n, n), 0)
    later = lax.broadcasted_iota(jnp.int32, (n, n), 1)
    upto = jnp.where(earlier <= later, 1.0, 0.0).astype(BF16)
    count = mm(hot.astype(BF16), upto)
    position = jnp.sum(hot * count, axis=0, keepdims=True) - 1.0
    slot = jnp.where(position < capacity, idx_row.astype(F32) * stride + position, -1.0)
    return hot, slot


def pick(slot, firsts, rows):
    n = slot.shape[1]
    row = lax.broadcasted_iota(jnp.int32, (rows, n), 0)
    parts = [jnp.where((row + first).astype(F32) == slot, 1.0, 0.0) for first in firsts]
    return jnp.concatenate(parts, axis=0).astype(BF16)


def gate_of(x, wgt, hot):
    n_experts = hot.shape[0]
    logits = mm(x, wgt, CONTRACT_LAST)
    e = jnp.exp(logits - jnp.max(logits, axis=1, keepdims=True))
    prob = e / jnp.sum(e, axis=1, keepdims=True)
    eye = jnp.where(
        lax.broadcasted_iota(jnp.int32, (n_experts, n_experts), 0)
        == lax.broadcasted_iota(jnp.int32, (n_experts, n_experts), 1), 1.0, 0.0)
    chosen = mm(hot.astype(BF16), eye.astype(BF16), CONTRACT_FIRST)
    gate = jnp.sum(chosen * prob, axis=1, keepdims=True)
    return prob, chosen, gate


def enter(peers, tp_peer):
    barrier = pltpu.get_barrier_semaphore()
    for r in (1, 2, 3):
        pl.semaphore_signal(barrier, inc=1, device_id={"ep": peers[r]}, device_id_type=MESH)
    pl.semaphore_signal(barrier, inc=1, device_id={"tp": tp_peer}, device_id_type=MESH)
    return barrier


def send(src, dst, ssem, rsem, device):
    copy = pltpu.make_async_remote_copy(
        src_ref=src, dst_ref=dst, send_sem=ssem, recv_sem=rsem, device_id=device, device_id_type=MESH)
    copy.start()
    return copy


def make_front(n_experts, capacity, cap):
    blk = 2 * cap

    def front(x_hbm, gy_hbm, wgt_hbm, idx_hbm, wi_hbm, wo_hbm,
              h_ref, da_ref, xs_ref, dys_ref, sfar_ref, snear_ref, sfar_own_ref, snear_own_ref, ynear_ref, yfar0_ref, yfar1_ref,
              picks_ref, prob_ref, chosen_ref,
              x_ref, gy_ref, wgt_ref, idx_ref, wi, wo, xsend, dysend, gp,
              ypeer, yown, yrecv, yback, yland,
              in_sem, wsem, x_s, x_r, d_s, d_r, y_s, y_r, b_s, b_r):
        tp = lax.axis_index("tp")
        tp_peer = 1 - tp
        peers = ep_partners()
        half = x_ref.shape[1] // 2
        mine = pl.ds(pl.multiple_of(tp * half, half), half)
        theirs = pl.ds(pl.multiple_of(tp_peer * half, half), half)
        d_ff = wi.shape[2]
        near, far, whole = slice(0, blk), slice(blk, 2 * blk), slice(0, 2 * blk)
        with jax.named_scope("enter"):
            small = [pltpu.make_async_copy(src, dst, in_sem.at[k]) for k, (src, dst) in enumerate(
                ((idx_hbm, idx_ref), (x_hbm, x_ref), (wgt_hbm, wgt_ref), (gy_hbm, gy_ref)))]
            for copy in small:
                copy.start()
            barrier = enter(peers, tp_peer)
            loads = {}
            for e in range(2):
                loads["i", e] = pltpu.make_async_copy(wi_hbm.at[e], wi.at[e], wsem.at[0, e])
                loads["o", e] = pltpu.make_async_copy(wo_hbm.at[e], wo.at[e], wsem.at[1, e])
            loads["i", 0].start()
            loads["o", 0].start()

        xc, dc, yc = {}, {}, {}

        def dispatch(v, g, e, buf, rows_ref, ssem, rsem, made):
            first = [peers[2 * g + q] * blk + e * cap for q in range(2)]
            rows = mm(pick(slot, first, cap), v)
            for q in range(2):
                r = 2 * g + q
                part = rows[q * cap:(q + 1) * cap].astype(BF16)
                if r == 0:
                    rows_ref[e, 0:cap, :] = part
                else:
                    buf[r - 1, e] = part
            return lambda: [made.__setitem__((r, e), send(
                buf.at[r - 1, e], rows_ref.at[e, r * cap:(r + 1) * cap, :], ssem.at[r - 1, e], rsem.at[r - 1, e],
                {"ep": peers[r]})) for r in (2 * g, 2 * g + 1) if r]

        def dispatch_x(g, e):
            return dispatch(x_ref[...], g, e, xsend, xs_ref, x_s, x_r, xc)

        with jax.named_scope("route"):
            small[0].wait()
            hot, slot = route(idx_ref[...], capacity, n_experts, cap)
            small[1].wait()
            go = dispatch_x(0, 0)
        with jax.named_scope("barrier"):
            pl.semaphore_wait(barrier, 4)
        with jax.named_scope("dispatch_x"):
            go()
            dispatch_x(1, 0)()
            dispatch_x(0, 1)()
            dispatch_x(1, 1)()
        loads["i", 1].start()
        loads["o", 1].start()

        def forward(g, e):
            rows = far if g else near
            if g == 0:
                loads["i", e].wait()
            xg = xs_ref[e, rows, :]
            step = d_ff // 2
            for c in range(2):
                cols = slice(c * step, (c + 1) * step)
                a = mm(xg, wi[e, :, cols])
                t = jnp.tanh(GELU_C * (a + GELU_K * (a * a * a)))
                cdf = 0.5 * (1.0 + t)
                h_ref[e, rows, cols] = (a * cdf).astype(BF16)
                gp[e, rows, cols] = cdf + (0.5 * a) * (1.0 - t * t) * (GELU_C + (3.0 * GELU_C * GELU_K) * (a * a))
            if g == 0:
                loads["o", e].wait()
            ypeer[g, e] = mm(h_ref[e, rows, :], wo[e, :, theirs])
            yc[g, e] = send(ypeer.at[g, e], yrecv.at[g, e], y_s.at[g, e], y_r.at[g, e], {"tp": tp_peer})

        def backward(rows, e):
            dyg = dys_ref[e, rows, :]
            step = d_ff // 4
            for c in range(4):
                cols = slice(c * step, (c + 1) * step)
                dh = mm(dyg, wo[e, cols, :], CONTRACT_LAST)
                da_ref[e, rows, cols] = (dh * gp[e, rows, cols]).astype(BF16)
            dag = da_ref[e, rows, :]
            for cols, near_ref, far_ref in ((theirs, snear_ref, sfar_ref), (mine, snear_own_ref, sfar_own_ref)):
                part = mm(dag, wi[e, cols, :], CONTRACT_LAST)
                if rows is not far:
                    near_ref[e] = part[0:blk]
                if rows is not near:
                    far_ref[e] = part[part.shape[0] - blk:]

        def y_blocks(g):
            for e in range(2):
                yc[g, e].wait()
            both = [yown[e, far if g else near, :] + yrecv[g, e] for e in range(2)]
            return [jnp.concatenate([both[e][q * cap:(q + 1) * cap] for e in range(2)], axis=0).astype(BF16) for q in range(2)]

        with jax.named_scope("wait_near"):
            xc[1, 0].wait()
        with jax.named_scope("fwd#g=0#e=0"):
            forward(0, 0)
        with jax.named_scope("dispatch_dy"):
            small[2].wait()
            small[3].wait()
            prob, chosen, gate = gate_of(x_ref[...], wgt_ref[...], hot)
            prob_ref[...], chosen_ref[...] = prob, chosen
            dy = (gate * gy_ref[...].astype(F32)).astype(BF16)
            for g in (1, 0):
                for e in range(2):
                    dispatch(dy, g, e, dysend, dys_ref, d_s, d_r, dc)()
        with jax.named_scope("fwd#g=0#e=1"):
            xc[1, 1].wait()
            forward(0, 1)
        with jax.named_scope("picks"):
            picks_ref[...] = pick(slot, [peers[r] * blk for r in range(4)], blk)
        with jax.named_scope("wait_far#e=0"):
            xc[2, 0].wait()
            xc[3, 0].wait()
        with jax.named_scope("fwd#g=1#e=0"):
            forward(1, 0)
        with jax.named_scope("bwd#near#e=0"):
            dc[1, 0].wait()
            backward(near, 0)
        with jax.named_scope("wait_far#e=1"):
            xc[2, 1].wait()
            xc[3, 1].wait()
        with jax.named_scope("fwd#g=1#e=1"):
            forward(1, 1)
        with jax.named_scope("yown"):
            for e in range(2):
                yown[e] = mm(h_ref[e], wo[e, :, mine])
        with jax.named_scope("y_near"):
            kept, away = y_blocks(0)
            ynear_ref[near, :] = kept
            yback[...] = away
            bc = send(yback, yland, b_s, b_r, {"ep": peers[1]})
        with jax.named_scope("wait_dy#e=0"):
            dc[2, 0].wait()
            dc[3, 0].wait()
        with jax.named_scope("bwd#far#e=0"):
            backward(far, 0)
        with jax.named_scope("wait_dy#e=1"):
            for r in (1, 2, 3):
                dc[r, 1].wait()
        with jax.named_scope("bwd#e=1"):
            backward(whole, 1)
        with jax.named_scope("y_far"):
            bc.wait()
            ynear_ref[far, :] = yland[...]
            yfar0_ref[...], yfar1_ref[...] = y_blocks(1)

    return front


def make_grad(steps):
    def grad(left_ref, right_ref, after_ref, out_hbm, *rest):
        buf, sem = rest[-2:]
        n_exp, _, width = left_ref.shape
        piece = width // steps
        copies = []
        with jax.named_scope("make"):
            for e in range(n_exp):
                right = right_ref[e]
                for c in range(steps):
                    rows = slice(c * piece, (c + 1) * piece)
                    buf[e, rows, :] = mm(left_ref[e, :, rows], right, CONTRACT_FIRST)
                    copies.append(pltpu.make_async_copy(buf.at[e, rows, :], out_hbm.at[e, rows, :], sem.at[e, c]))
                    copies[-1].start()
            for done_ref in rest[:-2]:
                done_ref[...] = jnp.zeros_like(done_ref)
        with jax.named_scope("drain"):
            for copy in copies:
                copy.wait()

    return grad


def y_tokens(picks_ref, ynear_ref, yfar0_ref, yfar1_ref, after_ref, y_ref):
    rows = jnp.concatenate([ynear_ref[...], yfar0_ref[...], yfar1_ref[...]], axis=0)
    y_ref[...] = mm(picks_ref[...], rows, CONTRACT_FIRST).astype(BF16)


def make_blocks(cap):
    def s_blocks(own_ref, recv_ref, out_ref):
        both = [own_ref[e] + recv_ref[e] for e in range(2)]
        out_ref[...] = jnp.concatenate(
            [both[e][q * cap:(q + 1) * cap] for q in range(2) for e in range(2)], axis=0).astype(BF16)

    return s_blocks


def make_back(cap):
    blk = 2 * cap

    def back(x_ref, gy_ref, wgt_ref, picks_ref, prob_ref, chosen_ref, ymine_ref, sfar_ref, sown_ref, srecv_ref,
             dx_ref, dwgt_ref,
             sback, sland, stsend, stland, gsend, gland, dwg,
             b_s, b_r, x_s, x_r, g_s, g_r, w_s, w_r):
        tp = lax.axis_index("tp")
        ep = lax.axis_index("ep")
        tp_peer = 1 - tp
        peers = ep_partners()
        n, d_model = x_ref.shape
        half = d_model // 2
        mine = pl.ds(pl.multiple_of(tp * half, half), half)
        theirs = pl.ds(pl.multiple_of(tp_peer * half, half), half)
        with jax.named_scope("enter"):
            barrier = enter(peers, tp_peer)
            both = [sown_ref[e] + srecv_ref[e] for e in range(2)]
            kept, away = [jnp.concatenate([both[e][q * cap:(q + 1) * cap] for e in range(2)], axis=0).astype(BF16)
                          for q in range(2)]
            sback[...] = away
            dgate = jnp.sum(gy_ref[:, mine].astype(F32) * ymine_ref[...].astype(F32), axis=1, keepdims=True)
            gsend[...] = jnp.broadcast_to(dgate, (n, 128)).T[0:8]
            pl.semaphore_wait(barrier, 4)
        with jax.named_scope("s_back"):
            bc = [send(sback, sland.at[0], b_s.at[0], b_r.at[0], {"ep": peers[1]}),
                  send(sfar_ref.at[blk:2 * blk, :], sland.at[1], b_s.at[1], b_r.at[1], {"ep": peers[1]})]
            gc = send(gsend, gland, g_s, g_r, {"tp": tp_peer})
        with jax.named_scope("s_wait"):
            for copy in bc:
                copy.wait()
        with jax.named_scope("s_tok"):
            s_rows = jnp.concatenate([kept, sland[0], sfar_ref[0:blk, :], sland[1]], axis=0)
            stsend[...] = mm(picks_ref[...], s_rows, CONTRACT_FIRST).astype(BF16)
            xc = send(stsend, stland, x_s, x_r, {"tp": tp_peer})
        with jax.named_scope("gate_wait"):
            prob, chosen = prob_ref[...], chosen_ref[...]
            gate = jnp.sum(chosen * prob, axis=1, keepdims=True)
            gc.wait()
        with jax.named_scope("router"):
            dgate = dgate + jnp.broadcast_to(gland[0:1, :], (128, n)).T[:, 0:1]
            dlogits = (dgate * prob * (chosen - gate)).astype(BF16)
            dwg[ep] = mm(dlogits, x_ref[...], CONTRACT_FIRST)
            wc = {}
            for r in (2, 3, 1):
                wc[r] = send(dwg.at[ep], dwg.at[ep], w_s.at[r - 1], w_r.at[r - 1], {"ep": peers[r]})
            dx_ref[:, mine] = (stsend[...].astype(F32) + mm(dlogits, wgt_ref[:, mine])).astype(BF16)
            rgrad = mm(dlogits, wgt_ref[:, theirs])
        with jax.named_scope("dwg"):
            for r in (1, 2, 3):
                wc[r].wait()
            dwgt_ref[...] = (dwg[0] + dwg[1]) + (dwg[2] + dwg[3])
        with jax.named_scope("dx_wait"):
            xc.wait()
        with jax.named_scope("dx"):
            dx_ref[:, theirs] = (stland[...].astype(F32) + rgrad).astype(BF16)

    return back


def finish(dx_ref, dwgt_ref, ymine_ref, ytheirs_ref, prob_ref, chosen_ref, out_hbm, dx_hbm, dwgt_hbm, out_ref, sem):
    half = ymine_ref.shape[1]
    copies = [pltpu.make_async_copy(src, dst, sem.at[k]) for k, (src, dst) in enumerate(
        ((dx_ref, dx_hbm), (dwgt_ref, dwgt_hbm), (out_ref, out_hbm)))]
    copies[0].start()
    copies[1].start()
    tp = lax.axis_index("tp")
    gate = jnp.sum(chosen_ref[...] * prob_ref[...], axis=1, keepdims=True)
    for side, ref in ((tp, ymine_ref), (1 - tp, ytheirs_ref)):
        out_ref[:, pl.ds(pl.multiple_of(side * half, half), half)] = (gate * ref[...].astype(F32)).astype(BF16)
    copies[2].start()
    for copy in copies:
        copy.wait()


def solution(mesh):
    row_spec = P(("dp", "ep"), None)
    vmem = pl.BlockSpec(memory_space=pltpu.VMEM)
    hbm = pl.BlockSpec(memory_space=pltpu.HBM)

    def local_block(tokens, grad_out, w_router, w_in, w_out, expert_ids):
        n, d_model = tokens.shape
        n_experts = w_router.shape[1]
        le, _, d_ff = w_in.shape
        capacity = (6 * n + 5 * n_experts - 1) // (5 * n_experts)
        cap = -(-capacity // 8) * 8
        blk = le * cap
        rows = 4 * cap
        half = d_model // 2
        wgt = w_router.T
        idx_row = expert_ids.reshape(1, n)
        sds = jax.ShapeDtypeStruct
        dma = pltpu.SemaphoreType.DMA

        h, da, xs, dys, sfar, snear, sfar_own, snear_own, ynear, yfar0, yfar1, picks, prob, chosen = pl.pallas_call(
            make_front(n_experts, capacity, cap),
            out_shape=(sds((le, rows, d_ff), BF16), sds((le, rows, d_ff), BF16), sds((le, rows, d_model), BF16),
                       sds((le, rows, d_model), BF16), *[sds((le, blk, half), F32)] * 4,
                       sds((2 * blk, half), BF16), sds((blk, half), BF16), sds((blk, half), BF16),
                       sds((4 * blk, n), BF16), sds((n, n_experts), F32), sds((n, n_experts), F32)),
            in_specs=[hbm] * 6,
            out_specs=(vmem,) * 14,
            scratch_shapes=[
                pltpu.VMEM((n, d_model), BF16), pltpu.VMEM((n, d_model), BF16), pltpu.VMEM((n_experts, d_model), BF16),
                pltpu.VMEM((1, n), jnp.int32),
                pltpu.VMEM((le, d_model, d_ff), BF16), pltpu.VMEM((le, d_ff, d_model), BF16),
                pltpu.VMEM((3, le, cap, d_model), BF16), pltpu.VMEM((3, le, cap, d_model), BF16),
                pltpu.VMEM((le, rows, d_ff), F32),
                pltpu.VMEM((2, le, blk, half), F32), pltpu.VMEM((le, rows, half), F32), pltpu.VMEM((2, le, blk, half), F32),
                pltpu.VMEM((blk, half), BF16), pltpu.VMEM((blk, half), BF16),
                dma((4,)), dma((2, le)), dma((3, le)), dma((3, le)), dma((3, le)), dma((3, le)), dma((2, le)), dma((2, le)), dma, dma,
            ],
            compiler_params=pltpu.CompilerParams(collective_id=0, has_side_effects=True, vmem_limit_bytes=40 * 2**20),
            name="front",
        )(*[pltpu.with_memory_space_constraint(v, pltpu.HBM) for v in (tokens, grad_out, wgt, idx_row, w_in, w_out)])

        swap = [(0, 1), (1, 0)]
        across, diagonal = [(0, 2), (2, 0), (1, 3), (3, 1)], [(0, 3), (3, 0), (1, 2), (2, 1)]
        sfar_recv = lax.ppermute(sfar, "tp", swap)
        snear_recv = lax.ppermute(snear, "tp", swap)
        yland0 = lax.ppermute(yfar0, "ep", across)
        yland1 = lax.ppermute(yfar1, "ep", diagonal)

        def weight_grad(left, right, after, name, tell):
            steps = 8
            shape = (le, left.shape[2], right.shape[2])
            return pl.pallas_call(
                make_grad(steps),
                out_shape=(sds(shape, F32), sds((8, 128), F32))[:1 + tell],
                in_specs=[vmem] * 3, out_specs=(hbm, vmem)[:1 + tell],
                scratch_shapes=[pltpu.VMEM(shape, F32), dma((le, steps))],
                cost_estimate=pl.CostEstimate(flops=2 * rows * shape[0] * shape[1] * shape[2],
                                              bytes_accessed=4 * shape[0] * shape[1] * shape[2], transcendentals=0),
                compiler_params=pltpu.CompilerParams(vmem_limit_bytes=24 * 2**20),
                name=name,
            )(left, right, after)

        dwo, done = weight_grad(h, dys, ynear, "grad_out", True)
        ymine = pl.pallas_call(
            y_tokens, out_shape=sds((n, half), BF16), in_specs=[vmem] * 5, out_specs=vmem,
            compiler_params=pltpu.CompilerParams(vmem_limit_bytes=8 * 2**20), name="y_tokens",
        )(picks, ynear, yland0, yland1, done)
        ytheirs = lax.ppermute(ymine, "tp", swap)
        sblocks = pl.pallas_call(
            make_blocks(cap), out_shape=sds((2 * blk, half), BF16), in_specs=[vmem] * 2, out_specs=vmem,
            compiler_params=pltpu.CompilerParams(vmem_limit_bytes=8 * 2**20), name="s_blocks",
        )(sfar_own, sfar_recv)
        sfar_land = lax.ppermute(sblocks, "ep", across)
        dwi, = weight_grad(xs, da, sblocks, "grad_in", False)

        dx_v, dwgt_v = pl.pallas_call(
            make_back(cap),
            out_shape=(sds((n, d_model), BF16), sds((n_experts, d_model), F32)),
            in_specs=[vmem] * 10,
            out_specs=(vmem,) * 2,
            scratch_shapes=[
                pltpu.VMEM((blk, half), BF16), pltpu.VMEM((2, blk, half), BF16),
                pltpu.VMEM((n, half), BF16), pltpu.VMEM((n, half), BF16),
                pltpu.VMEM((8, n), F32), pltpu.VMEM((8, n), F32),
                pltpu.VMEM((4, n_experts, d_model), F32),
                dma((2,)), dma((2,)), dma, dma, dma, dma, dma((3,)), dma((3,)),
            ],
            compiler_params=pltpu.CompilerParams(collective_id=1, has_side_effects=True, vmem_limit_bytes=24 * 2**20),
            name="back",
        )(tokens, grad_out, wgt, picks, prob, chosen, ymine, sfar_land, snear_own, snear_recv)
        out, dx, dwgt = pl.pallas_call(
            finish, out_shape=(sds((n, d_model), BF16), sds((n, d_model), BF16), sds((n_experts, d_model), F32)),
            in_specs=[vmem] * 6, out_specs=(hbm,) * 3,
            scratch_shapes=[pltpu.VMEM((n, d_model), BF16), dma((3,))],
            compiler_params=pltpu.CompilerParams(vmem_limit_bytes=8 * 2**20), name="finish",
        )(dx_v, dwgt_v, ymine, ytheirs, prob, chosen)
        return out, dx, dwi, dwo, dwgt.T

    in_specs = (row_spec, row_spec, P(None, None), P("ep", None, "tp"), P("ep", "tp", None), P(("dp", "ep")))
    out_specs = (row_spec, row_spec, P(("dp", "ep"), None, "tp"), P(("dp", "ep"), "tp", None), P("dp", None))
    return jax.shard_map(local_block, mesh=mesh, in_specs=in_specs, out_specs=out_specs, check_vma=False)
```

```python
import jax
import jax.numpy as jnp
from jax import lax
from jax.experimental import pallas as pl
from jax.experimental.pallas import tpu as pltpu
from jax.sharding import PartitionSpec as P


MESH = pl.DeviceIdType.MESH
F32, BF16 = jnp.float32, jnp.bfloat16
CONTRACT_LAST = (((1,), (1,)), ((), ()))
CONTRACT_FIRST = (((0,), (0,)), ((), ()))
GELU_C = 0.7978845608028654
GELU_K = 0.044715


def mm(a, b, dims=(((1,), (0,)), ((), ()))):
    return lax.dot_general(a, b, dims, preferred_element_type=F32)


def ep_partners():
    ep = lax.axis_index("ep")
    cx, cc = ep // 2, ep % 2
    return [ep, 2 * cx + (1 - cc), 2 * (1 - cx) + cc, 2 * (1 - cx) + (1 - cc)]


def route(idx_row, capacity, n_experts, stride):
    n = idx_row.shape[1]
    expert = lax.broadcasted_iota(jnp.int32, (n_experts, n), 0)
    hot = jnp.where(expert == idx_row, 1.0, 0.0)
    earlier = lax.broadcasted_iota(jnp.int32, (n, n), 0)
    later = lax.broadcasted_iota(jnp.int32, (n, n), 1)
    upto = jnp.where(earlier <= later, 1.0, 0.0).astype(BF16)
    count = mm(hot.astype(BF16), upto)
    position = jnp.sum(hot * count, axis=0, keepdims=True) - 1.0
    slot = jnp.where(position < capacity, idx_row.astype(F32) * stride + position, -1.0)
    return hot, slot


def pick(slot, firsts, rows):
    n = slot.shape[1]
    row = lax.broadcasted_iota(jnp.int32, (rows, n), 0)
    parts = [jnp.where((row + first).astype(F32) == slot, 1.0, 0.0) for first in firsts]
    return jnp.concatenate(parts, axis=0).astype(BF16)


def gate_of(x, wgt, hot):
    n_experts = hot.shape[0]
    logits = mm(x, wgt, CONTRACT_LAST)
    e = jnp.exp(logits - jnp.max(logits, axis=1, keepdims=True))
    prob = e / jnp.sum(e, axis=1, keepdims=True)
    eye = jnp.where(
        lax.broadcasted_iota(jnp.int32, (n_experts, n_experts), 0)
        == lax.broadcasted_iota(jnp.int32, (n_experts, n_experts), 1), 1.0, 0.0)
    chosen = mm(hot.astype(BF16), eye.astype(BF16), CONTRACT_FIRST)
    gate = jnp.sum(chosen * prob, axis=1, keepdims=True)
    return prob, chosen, gate


def enter(*devices):
    barrier = pltpu.get_barrier_semaphore()
    for device in devices:
        pl.semaphore_signal(barrier, inc=1, device_id=device, device_id_type=MESH)
    return barrier


def send(src, dst, ssem, rsem, device):
    copy = pltpu.make_async_remote_copy(
        src_ref=src, dst_ref=dst, send_sem=ssem, recv_sem=rsem, device_id=device, device_id_type=MESH)
    copy.start()
    return copy


def make_front(n_experts, capacity, cap):
    blk = 2 * cap

    def front(x_hbm, gy_hbm, wgt_hbm, idx_hbm, wi_hbm, wo_hbm,
              h_ref, da_ref, xs_ref, dys_ref, sfar_ref, snear_ref, sfar_own_ref, snear_own_ref, ynear_ref, yfar0_ref, yfar1_ref,
              picks_ref, prob_ref, chosen_ref,
              x_ref, gy_ref, wgt_ref, idx_ref, wi, wo, xsend, dysend, gp,
              ypeer, yown, yrecv, yback, yland,
              in_sem, wsem, x_s, x_r, d_s, d_r, y_s, y_r, b_s, b_r):
        tp = lax.axis_index("tp")
        tp_peer = 1 - tp
        peers = ep_partners()
        half = x_ref.shape[1] // 2
        mine = pl.ds(pl.multiple_of(tp * half, half), half)
        theirs = pl.ds(pl.multiple_of(tp_peer * half, half), half)
        d_ff = wi.shape[2]
        near, far, whole = slice(0, blk), slice(blk, 2 * blk), slice(0, 2 * blk)
        small = [pltpu.make_async_copy(src, dst, in_sem.at[k]) for k, (src, dst) in enumerate(
            ((idx_hbm, idx_ref), (x_hbm, x_ref), (wgt_hbm, wgt_ref), (gy_hbm, gy_ref)))]
        for copy in small:
            copy.start()
        barrier = enter({"ep": peers[1]}, {"ep": peers[2]}, {"ep": peers[3]}, {"tp": tp_peer})
        loads = {}
        for e in range(2):
            loads["i", e] = pltpu.make_async_copy(wi_hbm.at[e], wi.at[e], wsem.at[0, e])
            loads["o", e] = pltpu.make_async_copy(wo_hbm.at[e], wo.at[e], wsem.at[1, e])
        loads["i", 0].start()
        loads["o", 0].start()

        xc, dc, yc = {}, {}, {}

        def dispatch(v, g, e, buf, rows_ref, ssem, rsem, made):
            first = [peers[2 * g + q] * blk + e * cap for q in range(2)]
            rows = mm(pick(slot, first, cap), v)
            for q in range(2):
                r = 2 * g + q
                part = rows[q * cap:(q + 1) * cap].astype(BF16)
                if r == 0:
                    rows_ref[e, 0:cap, :] = part
                else:
                    buf[r - 1, e] = part
            return lambda: [made.__setitem__((r, e), send(
                buf.at[r - 1, e], rows_ref.at[e, r * cap:(r + 1) * cap, :], ssem.at[r - 1, e], rsem.at[r - 1, e],
                {"ep": peers[r]})) for r in (2 * g, 2 * g + 1) if r]

        def dispatch_x(g, e):
            return dispatch(x_ref[...], g, e, xsend, xs_ref, x_s, x_r, xc)

        small[0].wait()
        hot, slot = route(idx_ref[...], capacity, n_experts, cap)
        small[1].wait()
        go = dispatch_x(0, 0)
        pl.semaphore_wait(barrier, 4)
        go()
        dispatch_x(1, 0)()
        dispatch_x(0, 1)()
        dispatch_x(1, 1)()
        loads["i", 1].start()
        loads["o", 1].start()

        def forward(g, e):
            rows = far if g else near
            if g == 0:
                loads["i", e].wait()
            xg = xs_ref[e, rows, :]
            step = d_ff // 2
            for c in range(2):
                cols = slice(c * step, (c + 1) * step)
                a = mm(xg, wi[e, :, cols])
                t = jnp.tanh(GELU_C * (a + GELU_K * (a * a * a)))
                cdf = 0.5 * (1.0 + t)
                h_ref[e, rows, cols] = (a * cdf).astype(BF16)
                gp[e, rows, cols] = cdf + (0.5 * a) * (1.0 - t * t) * (GELU_C + (3.0 * GELU_C * GELU_K) * (a * a))
            if g == 0:
                loads["o", e].wait()
            ypeer[g, e] = mm(h_ref[e, rows, :], wo[e, :, theirs])
            yc[g, e] = send(ypeer.at[g, e], yrecv.at[g, e], y_s.at[g, e], y_r.at[g, e], {"tp": tp_peer})

        def backward(rows, e):
            dyg = dys_ref[e, rows, :]
            step = d_ff // 4
            for c in range(4):
                cols = slice(c * step, (c + 1) * step)
                dh = mm(dyg, wo[e, cols, :], CONTRACT_LAST)
                da_ref[e, rows, cols] = (dh * gp[e, rows, cols]).astype(BF16)
            dag = da_ref[e, rows, :]
            for cols, near_ref, far_ref in ((theirs, snear_ref, sfar_ref), (mine, snear_own_ref, sfar_own_ref)):
                part = mm(dag, wi[e, cols, :], CONTRACT_LAST)
                if rows is not far:
                    near_ref[e] = part[0:blk]
                if rows is not near:
                    far_ref[e] = part[part.shape[0] - blk:]

        def y_blocks(g):
            for e in range(2):
                yc[g, e].wait()
            both = [yown[e, far if g else near, :] + yrecv[g, e] for e in range(2)]
            return [jnp.concatenate([both[e][q * cap:(q + 1) * cap] for e in range(2)], axis=0).astype(BF16) for q in range(2)]

        xc[1, 0].wait()
        forward(0, 0)
        small[2].wait()
        small[3].wait()
        prob, chosen, gate = gate_of(x_ref[...], wgt_ref[...], hot)
        prob_ref[...], chosen_ref[...] = prob, chosen
        dy = (gate * gy_ref[...].astype(F32)).astype(BF16)
        for g in (1, 0):
            for e in range(2):
                dispatch(dy, g, e, dysend, dys_ref, d_s, d_r, dc)()
        xc[1, 1].wait()
        forward(0, 1)
        picks_ref[...] = pick(slot, [peers[r] * blk for r in range(4)], blk)
        xc[2, 0].wait()
        xc[3, 0].wait()
        forward(1, 0)
        dc[1, 0].wait()
        backward(near, 0)
        xc[2, 1].wait()
        xc[3, 1].wait()
        forward(1, 1)
        for e in range(2):
            yown[e] = mm(h_ref[e], wo[e, :, mine])
        kept, away = y_blocks(0)
        ynear_ref[near, :] = kept
        yback[...] = away
        bc = send(yback, yland, b_s, b_r, {"ep": peers[1]})
        dc[2, 0].wait()
        dc[3, 0].wait()
        backward(far, 0)
        for r in (1, 2, 3):
            dc[r, 1].wait()
        backward(whole, 1)
        bc.wait()
        ynear_ref[far, :] = yland[...]
        yfar0_ref[...], yfar1_ref[...] = y_blocks(1)

    return front


def make_grad(pieces, tell):
    def grad(left_ref, right_ref, after_ref, *rest):
        rest = rest[len(rest) - 3 - tell:]
        out_hbm, rest = rest[0], rest[1:]
        buf, sem = rest[-2:]
        size = buf.shape[1]
        copies = []
        for k, (e, row) in enumerate(pieces):
            rows = slice(row, row + size)
            buf[k] = mm(left_ref[e, :, rows], right_ref[e], CONTRACT_FIRST)
            copies.append(pltpu.make_async_copy(buf.at[k], out_hbm.at[e, rows, :], sem.at[k]))
            copies[-1].start()
        if tell:
            rest[0][...] = jnp.zeros_like(rest[0])
        for copy in copies:
            copy.wait()

    return grad


def y_tokens(picks_ref, ynear_ref, yfar0_ref, yfar1_ref, after_ref, y_ref):
    rows = jnp.concatenate([ynear_ref[...], yfar0_ref[...], yfar1_ref[...]], axis=0)
    y_ref[...] = mm(picks_ref[...], rows, CONTRACT_FIRST).astype(BF16)


def make_blocks(cap):
    def s_blocks(own_ref, recv_ref, after_ref, out_ref):
        both = [own_ref[e] + recv_ref[e] for e in range(2)]
        out_ref[...] = jnp.concatenate(
            [both[e][q * cap:(q + 1) * cap] for q in range(2) for e in range(2)], axis=0).astype(BF16)

    return s_blocks


def make_near_return(cap):
    blk = 2 * cap

    def near_return(picks_ref, sfar_ref, sown_ref, srecv_ref, after_ref, stok_ref, sback, sland, b_s, b_r):
        partner = {"ep": ep_partners()[1]}
        barrier = enter(partner)
        both = [sown_ref[e] + srecv_ref[e] for e in range(2)]
        kept, away = [jnp.concatenate([both[e][q * cap:(q + 1) * cap] for e in range(2)], axis=0).astype(BF16)
                      for q in range(2)]
        sback[...] = away
        pl.semaphore_wait(barrier, 1)
        copies = [send(sback, sland.at[0], b_s.at[0], b_r.at[0], partner),
                  send(sfar_ref.at[blk:2 * blk, :], sland.at[1], b_s.at[1], b_r.at[1], partner)]
        for copy in copies:
            copy.wait()
        s_rows = jnp.concatenate([kept, sland[0], sfar_ref[0:blk, :], sland[1]], axis=0)
        stok_ref[...] = mm(picks_ref[...], s_rows, CONTRACT_FIRST).astype(BF16)

    return near_return


def router_grad(x_ref, gy_ref, prob_ref, chosen_ref, ymine_ref, ytheirs_ref, after_ref, dlog_ref, dwgt_ref, dwg, w_s, w_r):
    tp = lax.axis_index("tp")
    ep = lax.axis_index("ep")
    peers = ep_partners()
    half = ymine_ref.shape[1]
    barrier = enter(*[{"ep": peers[r]} for r in (1, 2, 3)])
    sums = [jnp.sum(gy_ref[:, pl.ds(pl.multiple_of(side * half, half), half)].astype(F32) * ref[...].astype(F32),
                    axis=1, keepdims=True) for side, ref in ((tp, ymine_ref), (1 - tp, ytheirs_ref))]
    prob, chosen = prob_ref[...], chosen_ref[...]
    gate = jnp.sum(chosen * prob, axis=1, keepdims=True)
    dlogits = ((sums[0] + sums[1]) * prob * (chosen - gate)).astype(BF16)
    dlog_ref[...] = dlogits
    dwg[ep] = mm(dlogits, x_ref[...], CONTRACT_FIRST)
    pl.semaphore_wait(barrier, 3)
    copies = [send(dwg.at[ep], dwg.at[ep], w_s.at[r - 1], w_r.at[r - 1], {"ep": peers[r]}) for r in (2, 3, 1)]
    for copy in copies:
        copy.wait()
    dwgt_ref[...] = (dwg[0] + dwg[1]) + (dwg[2] + dwg[3])


def write_out(dwgt_ref, ymine_ref, ytheirs_ref, prob_ref, chosen_ref, out_hbm, dwgt_hbm, out_ref, sem):
    half = ymine_ref.shape[1]
    first = pltpu.make_async_copy(dwgt_ref, dwgt_hbm, sem.at[0])
    first.start()
    tp = lax.axis_index("tp")
    gate = jnp.sum(chosen_ref[...] * prob_ref[...], axis=1, keepdims=True)
    for side, ref in ((tp, ymine_ref), (1 - tp, ytheirs_ref)):
        out_ref[:, pl.ds(pl.multiple_of(side * half, half), half)] = (gate * ref[...].astype(F32)).astype(BF16)
    second = pltpu.make_async_copy(out_ref, out_hbm, sem.at[1])
    second.start()
    first.wait()
    second.wait()


def write_dx(dlog_ref, wgt_ref, smine_ref, stheirs_ref, after_ref, dx_hbm, dx_ref, sem):
    half = smine_ref.shape[1]
    tp = lax.axis_index("tp")
    for side, ref in ((tp, smine_ref), (1 - tp, stheirs_ref)):
        cols = pl.ds(pl.multiple_of(side * half, half), half)
        dx_ref[:, cols] = (ref[...].astype(F32) + mm(dlog_ref[...], wgt_ref[:, cols])).astype(BF16)
    copy = pltpu.make_async_copy(dx_ref, dx_hbm, sem)
    copy.start()
    copy.wait()


FIRST_PART = 12


def solution(mesh):
    row_spec = P(("dp", "ep"), None)
    vmem = pl.BlockSpec(memory_space=pltpu.VMEM)
    hbm = pl.BlockSpec(memory_space=pltpu.HBM)

    def local_block(tokens, grad_out, w_router, w_in, w_out, expert_ids):
        n, d_model = tokens.shape
        n_experts = w_router.shape[1]
        le, _, d_ff = w_in.shape
        capacity = (6 * n + 5 * n_experts - 1) // (5 * n_experts)
        cap = -(-capacity // 8) * 8
        blk = le * cap
        rows = 4 * cap
        half = d_model // 2
        wgt = w_router.T
        idx_row = expert_ids.reshape(1, n)
        sds = jax.ShapeDtypeStruct
        dma = pltpu.SemaphoreType.DMA

        h, da, xs, dys, sfar, snear, sfar_own, snear_own, ynear, yfar0, yfar1, picks, prob, chosen = pl.pallas_call(
            make_front(n_experts, capacity, cap),
            out_shape=(sds((le, rows, d_ff), BF16), sds((le, rows, d_ff), BF16), sds((le, rows, d_model), BF16),
                       sds((le, rows, d_model), BF16), *[sds((le, blk, half), F32)] * 4,
                       sds((2 * blk, half), BF16), sds((blk, half), BF16), sds((blk, half), BF16),
                       sds((4 * blk, n), BF16), sds((n, n_experts), F32), sds((n, n_experts), F32)),
            in_specs=[hbm] * 6,
            out_specs=(vmem,) * 14,
            scratch_shapes=[
                pltpu.VMEM((n, d_model), BF16), pltpu.VMEM((n, d_model), BF16), pltpu.VMEM((n_experts, d_model), BF16),
                pltpu.VMEM((1, n), jnp.int32),
                pltpu.VMEM((le, d_model, d_ff), BF16), pltpu.VMEM((le, d_ff, d_model), BF16),
                pltpu.VMEM((3, le, cap, d_model), BF16), pltpu.VMEM((3, le, cap, d_model), BF16),
                pltpu.VMEM((le, rows, d_ff), F32),
                pltpu.VMEM((2, le, blk, half), F32), pltpu.VMEM((le, rows, half), F32), pltpu.VMEM((2, le, blk, half), F32),
                pltpu.VMEM((blk, half), BF16), pltpu.VMEM((blk, half), BF16),
                dma((4,)), dma((2, le)), dma((3, le)), dma((3, le)), dma((3, le)), dma((3, le)), dma((2, le)), dma((2, le)), dma, dma,
            ],
            compiler_params=pltpu.CompilerParams(collective_id=0, has_side_effects=True, vmem_limit_bytes=40 * 2**20),
            name="front",
        )(*[pltpu.with_memory_space_constraint(v, pltpu.HBM) for v in (tokens, grad_out, wgt, idx_row, w_in, w_out)])

        swap = [(0, 1), (1, 0)]
        across, diagonal = [(0, 2), (2, 0), (1, 3), (3, 1)], [(0, 3), (3, 0), (1, 2), (2, 1)]
        sfar_recv = lax.ppermute(sfar, "tp", swap)
        snear_recv = lax.ppermute(snear, "tp", swap)
        yland0 = lax.ppermute(yfar0, "ep", across)
        yland1 = lax.ppermute(yfar1, "ep", diagonal)

        def local(kernel, out_shape, ins, outs, args, scratch=(), limit=8, **more):
            return pl.pallas_call(
                kernel, out_shape=out_shape, in_specs=ins, out_specs=outs, scratch_shapes=list(scratch),
                compiler_params=pltpu.CompilerParams(vmem_limit_bytes=limit * 2**20), **more)(*args)

        def weight_grad(left, right, after, pieces, size, tell, base=None):
            shape = (le, left.shape[2], right.shape[2])
            cost = pl.CostEstimate(flops=2 * rows * len(pieces) * size * shape[2],
                                   bytes_accessed=4 * len(pieces) * size * shape[2], transcendentals=0)
            return local(
                make_grad(pieces, tell), (sds(shape, F32), sds((8, 128), F32))[:1 + tell],
                [vmem] * 3 + [hbm] * (base is not None), (hbm, vmem)[:1 + tell],
                (left, right, after) + ((base,) if base is not None else ()),
                [pltpu.VMEM((len(pieces), size, shape[2]), F32), dma((len(pieces),))], 24, cost_estimate=cost,
                input_output_aliases={3: 0} if base is not None else {})

        out_size, in_size = d_ff // 8, d_model // 8
        out_pieces = [(e, c * out_size) for e in range(le) for c in range(8)]
        in_pieces = [(e, c * in_size) for e in range(le) for c in range(8)]
        dwo, done = weight_grad(h, dys, ynear, out_pieces, out_size, True)
        ymine = local(y_tokens, sds((n, half), BF16), [vmem] * 5, vmem, (picks, ynear, yland0, yland1, done))
        ytheirs = lax.ppermute(ymine, "tp", swap)
        sblocks = local(make_blocks(cap), sds((2 * blk, half), BF16), [vmem] * 3, vmem, (sfar_own, sfar_recv, ymine))
        sfar_land = lax.ppermute(sblocks, "ep", across)
        dwi, done = weight_grad(xs, da, sblocks, in_pieces[:FIRST_PART], in_size, True)

        smine = pl.pallas_call(
            make_near_return(cap), out_shape=sds((n, half), BF16), in_specs=[vmem] * 5, out_specs=vmem,
            scratch_shapes=[pltpu.VMEM((blk, half), BF16), pltpu.VMEM((2, blk, half), BF16), dma((2,)), dma((2,))],
            compiler_params=pltpu.CompilerParams(collective_id=1, has_side_effects=True, vmem_limit_bytes=8 * 2**20),
            name="near_return",
        )(picks, sfar_land, snear_own, snear_recv, done)
        stheirs = lax.ppermute(smine, "tp", swap)
        dwi, done = weight_grad(xs, da, smine, in_pieces[FIRST_PART:], in_size, True, dwi)
        dlog, dwgt_v = pl.pallas_call(
            router_grad, out_shape=(sds((n, n_experts), BF16), sds((n_experts, d_model), F32)),
            in_specs=[vmem] * 7, out_specs=(vmem,) * 2,
            scratch_shapes=[pltpu.VMEM((4, n_experts, d_model), F32), dma((3,)), dma((3,))],
            compiler_params=pltpu.CompilerParams(collective_id=2, has_side_effects=True, vmem_limit_bytes=8 * 2**20),
            name="router_grad",
        )(tokens, grad_out, prob, chosen, ymine, ytheirs, done)
        out, dwgt = local(write_out, (sds((n, d_model), BF16), sds((n_experts, d_model), F32)), [vmem] * 5, (hbm,) * 2,
                          (dwgt_v, ymine, ytheirs, prob, chosen), [pltpu.VMEM((n, d_model), BF16), dma((2,))])
        dx = local(write_dx, sds((n, d_model), BF16), [vmem] * 5, hbm, (dlog, wgt, smine, stheirs, dwgt_v),
                   [pltpu.VMEM((n, d_model), BF16), dma])
        return out, dx, dwi, dwo, dwgt.T

    in_specs = (row_spec, row_spec, P(None, None), P("ep", None, "tp"), P("ep", "tp", None), P(("dp", "ep")))
    out_specs = (row_spec, row_spec, P(("dp", "ep"), None, "tp"), P(("dp", "ep"), "tp", None), P("dp", None))
    return jax.shard_map(local_block, mesh=mesh, in_specs=in_specs, out_specs=out_specs, check_vma=False)
```

```python
import jax
import jax.numpy as jnp
from jax import lax
from jax.experimental import pallas as pl
from jax.experimental.pallas import tpu as pltpu
from jax.sharding import PartitionSpec as P


MESH = pl.DeviceIdType.MESH
F32, BF16 = jnp.float32, jnp.bfloat16
CONTRACT_LAST = (((1,), (1,)), ((), ()))
CONTRACT_FIRST = (((0,), (0,)), ((), ()))
GELU_C = 0.7978845608028654
GELU_K = 0.044715


def mm(a, b, dims=(((1,), (0,)), ((), ()))):
    return lax.dot_general(a, b, dims, preferred_element_type=F32)


def ep_partners():
    ep = lax.axis_index("ep")
    cx, cc = ep // 2, ep % 2
    return [ep, 2 * cx + (1 - cc), 2 * (1 - cx) + cc, 2 * (1 - cx) + (1 - cc)]


def route(idx_row, capacity, n_experts, stride):
    n = idx_row.shape[1]
    expert = lax.broadcasted_iota(jnp.int32, (n_experts, n), 0)
    hot = jnp.where(expert == idx_row, 1.0, 0.0)
    earlier = lax.broadcasted_iota(jnp.int32, (n, n), 0)
    later = lax.broadcasted_iota(jnp.int32, (n, n), 1)
    upto = jnp.where(earlier <= later, 1.0, 0.0).astype(BF16)
    count = mm(hot.astype(BF16), upto)
    position = jnp.sum(hot * count, axis=0, keepdims=True) - 1.0
    slot = jnp.where(position < capacity, idx_row.astype(F32) * stride + position, -1.0)
    return hot, slot


def pick(slot, firsts, rows):
    n = slot.shape[1]
    row = lax.broadcasted_iota(jnp.int32, (rows, n), 0)
    parts = [jnp.where((row + first).astype(F32) == slot, 1.0, 0.0) for first in firsts]
    return jnp.concatenate(parts, axis=0).astype(BF16)


def gate_of(x, wgt, hot):
    n_experts = hot.shape[0]
    logits = mm(x, wgt, CONTRACT_LAST)
    e = jnp.exp(logits - jnp.max(logits, axis=1, keepdims=True))
    prob = e / jnp.sum(e, axis=1, keepdims=True)
    eye = jnp.where(
        lax.broadcasted_iota(jnp.int32, (n_experts, n_experts), 0)
        == lax.broadcasted_iota(jnp.int32, (n_experts, n_experts), 1), 1.0, 0.0)
    chosen = mm(hot.astype(BF16), eye.astype(BF16), CONTRACT_FIRST)
    gate = jnp.sum(chosen * prob, axis=1, keepdims=True)
    return prob, chosen, gate


def enter(*devices):
    barrier = pltpu.get_barrier_semaphore()
    for device in devices:
        pl.semaphore_signal(barrier, inc=1, device_id=device, device_id_type=MESH)
    return barrier


def send(src, dst, ssem, rsem, device):
    copy = pltpu.make_async_remote_copy(
        src_ref=src, dst_ref=dst, send_sem=ssem, recv_sem=rsem, device_id=device, device_id_type=MESH)
    copy.start()
    return copy


def make_front(n_experts, capacity, cap):
    blk = 2 * cap

    def front(x_hbm, gy_hbm, wgt_hbm, idx_hbm, wi_hbm, wo_hbm,
              h_ref, da_ref, xs_ref, dys_ref, sfar_ref, snear_ref, ynear_ref, yfar0_ref, yfar1_ref,
              picks_ref, prob_ref, chosen_ref, wi,
              x_ref, gy_ref, wgt_ref, idx_ref, wo, xsend, dysend, gp,
              ypeer, yown, yrecv, yback, yland,
              in_sem, wsem, x_s, x_r, d_s, d_r, y_s, y_r, b_s, b_r):
        tp = lax.axis_index("tp")
        tp_peer = 1 - tp
        peers = ep_partners()
        half = x_ref.shape[1] // 2
        mine = pl.ds(pl.multiple_of(tp * half, half), half)
        theirs = pl.ds(pl.multiple_of(tp_peer * half, half), half)
        d_ff = wi.shape[2]
        near, far, whole = slice(0, blk), slice(blk, 2 * blk), slice(0, 2 * blk)
        small = [pltpu.make_async_copy(src, dst, in_sem.at[k]) for k, (src, dst) in enumerate(
            ((idx_hbm, idx_ref), (x_hbm, x_ref), (wgt_hbm, wgt_ref), (gy_hbm, gy_ref)))]
        for copy in small:
            copy.start()
        barrier = enter({"ep": peers[1]}, {"ep": peers[2]}, {"ep": peers[3]}, {"tp": tp_peer})
        loads = {}
        for e in range(2):
            loads["i", e] = pltpu.make_async_copy(wi_hbm.at[e], wi.at[e], wsem.at[0, e])
            for k, (name, cols) in enumerate((("theirs", theirs), ("mine", mine))):
                loads[name, e] = pltpu.make_async_copy(wo_hbm.at[e, :, cols], wo.at[e, :, cols], wsem.at[1 + k, e])
        loads["i", 0].start()

        xc, dc, yc = {}, {}, {}

        def dispatch(v, g, e, buf, rows_ref, ssem, rsem, made):
            first = [peers[2 * g + q] * blk + e * cap for q in range(2)]
            rows = mm(pick(slot, first, cap), v)
            for q in range(2):
                r = 2 * g + q
                part = rows[q * cap:(q + 1) * cap].astype(BF16)
                if r == 0:
                    rows_ref[e, 0:cap, :] = part
                else:
                    buf[r - 1, e] = part
            return lambda: [made.__setitem__((r, e), send(
                buf.at[r - 1, e], rows_ref.at[e, r * cap:(r + 1) * cap, :], ssem, rsem.at[g, e],
                {"ep": peers[r]})) for r in (2 * g, 2 * g + 1) if r]

        def arrived(g, e, rows_ref, rsem):
            part = rows_ref.at[e, far if g else slice(cap, blk), :]
            pltpu.make_async_copy(part, part, rsem.at[g, e]).wait()

        def dispatch_x(g, e):
            return dispatch(x_ref[...], g, e, xsend, xs_ref, x_s, x_r, xc)

        def forward(first, last, e):
            rows = slice(first * cap, last * cap)
            if first == 0:
                loads["i", e].wait()
            xg = xs_ref[e, rows, :]
            step = d_ff // 2
            for c in range(2):
                cols = slice(c * step, (c + 1) * step)
                a = mm(xg, wi[e, :, cols])
                t = jnp.tanh(GELU_C * (a + GELU_K * (a * a * a)))
                cdf = 0.5 * (1.0 + t)
                h_ref[e, rows, cols] = (a * cdf).astype(BF16)
                gp[e, rows, cols] = cdf + (0.5 * a) * (1.0 - t * t) * (GELU_C + (3.0 * GELU_C * GELU_K) * (a * a))
            if first == 0:
                loads["theirs", e].wait()
            ypeer[e, rows, :] = mm(h_ref[e, rows, :], wo[e, :, theirs])
            yc[e, first] = send(ypeer.at[e, rows, :], yrecv.at[e, rows, :], y_s.at[e, first], y_r.at[e, first], {"tp": tp_peer})

        small[0].wait()
        hot, slot = route(idx_ref[...], capacity, n_experts, cap)
        small[1].wait()
        go = dispatch_x(0, 0)
        loads["theirs", 0].start()
        pl.semaphore_wait(barrier, 4)
        go()
        dispatch_x(1, 0)()
        dispatch_x(0, 1)()
        dispatch_x(1, 1)()
        for copy in (loads["i", 1], loads["theirs", 1], loads["mine", 0], loads["mine", 1]):
            copy.start()

        def backward(rows, e):
            dyg = dys_ref[e, rows, :]
            step = d_ff // 4
            for c in range(4):
                cols = slice(c * step, (c + 1) * step)
                dh = mm(dyg, wo[e, cols, :], CONTRACT_LAST)
                da_ref[e, rows, cols] = (dh * gp[e, rows, cols]).astype(BF16)
            dag = da_ref[e, rows, :]
            part = mm(dag, wi[e, theirs, :], CONTRACT_LAST)
            if rows is not far:
                snear_ref[e] = part[0:blk]
            if rows is not near:
                sfar_ref[e] = part[part.shape[0] - blk:]

        def y_blocks(g):
            rows = far if g else near
            for e in range(2):
                for r in (2 * g, 2 * g + 1):
                    if (e, r) in yc:
                        yc[e, r].wait()
            both = [yown[e, rows, :] + yrecv[e, rows, :] for e in range(2)]
            return [jnp.concatenate([both[e][q * cap:(q + 1) * cap] for e in range(2)], axis=0).astype(BF16) for q in range(2)]

        arrived(0, 0, xs_ref, x_r)
        forward(0, 2, 0)
        small[2].wait()
        small[3].wait()
        prob, chosen, gate = gate_of(x_ref[...], wgt_ref[...], hot)
        prob_ref[...], chosen_ref[...] = prob, chosen
        dy = (gate * gy_ref[...].astype(F32)).astype(BF16)
        for g in (1, 0):
            for e in range(2):
                dispatch(dy, g, e, dysend, dys_ref, d_s, d_r, dc)()
        arrived(0, 1, xs_ref, x_r)
        forward(0, 2, 1)
        picks_ref[...] = pick(slot, [peers[r] * blk for r in range(4)], blk)
        arrived(1, 0, xs_ref, x_r)
        forward(2, 4, 0)
        arrived(0, 0, dys_ref, d_r)
        loads["mine", 0].wait()
        backward(near, 0)
        arrived(1, 1, xs_ref, x_r)
        forward(2, 4, 1)
        loads["mine", 1].wait()
        for e in range(2):
            yown[e] = mm(h_ref[e], wo[e, :, mine])
        kept, away = y_blocks(0)
        ynear_ref[near, :] = kept
        yback[...] = away
        bc = send(yback, yland, b_s, b_r, {"ep": peers[1]})
        arrived(1, 0, dys_ref, d_r)
        backward(far, 0)
        for g in range(2):
            arrived(g, 1, dys_ref, d_r)
        backward(whole, 1)
        bc.wait()
        ynear_ref[far, :] = yland[...]
        yfar0_ref[...], yfar1_ref[...] = y_blocks(1)
        for sent, sem in ((xsend, x_s), (dysend, d_s)):
            pltpu.make_async_copy(sent, sent, sem).wait()

    return front


def make_grad(pieces, tell):
    def grad(left_ref, right_ref, after_ref, *rest):
        rest = rest[len(rest) - 3 - tell:]
        out_hbm, rest = rest[0], rest[1:]
        buf, sem = rest[-2:]
        size = buf.shape[1]
        copies = []
        for k, (e, row) in enumerate(pieces):
            rows = slice(row, row + size)
            buf[k] = mm(left_ref[e, :, rows], right_ref[e], CONTRACT_FIRST)
            copies.append(pltpu.make_async_copy(buf.at[k], out_hbm.at[e, rows, :], sem.at[k]))
            copies[-1].start()
        if tell:
            rest[0][...] = jnp.zeros_like(rest[0])
        for copy in copies:
            copy.wait()

    return grad


def make_grad_out(pieces):
    def grad_out(h_ref, dys_ref, da_ref, wi_ref, dwo_hbm, sfar_ref, snear_ref, buf, sem):
        size = buf.shape[1]
        blk, half = sfar_ref.shape[1:]
        copies = []
        for k, (e, row) in enumerate(pieces):
            rows = slice(row, row + size)
            buf[k] = mm(h_ref[e, :, rows], dys_ref[e], CONTRACT_FIRST)
            copies.append(pltpu.make_async_copy(buf.at[k], dwo_hbm.at[e, rows, :], sem.at[k]))
            copies[-1].start()
        mine = pl.ds(pl.multiple_of(lax.axis_index("tp") * half, half), half)
        for e in range(2):
            part = mm(da_ref[e], wi_ref[e, mine, :], CONTRACT_LAST)
            snear_ref[e] = part[0:blk]
            sfar_ref[e] = part[blk:]
        for copy in copies:
            copy.wait()

    return grad_out


def y_tokens(picks_ref, ynear_ref, yfar0_ref, yfar1_ref, after_ref, y_ref):
    rows = jnp.concatenate([ynear_ref[...], yfar0_ref[...], yfar1_ref[...]], axis=0)
    y_ref[...] = mm(picks_ref[...], rows, CONTRACT_FIRST).astype(BF16)


def make_blocks(cap):
    def s_blocks(own_ref, recv_ref, after_ref, out_ref):
        both = [own_ref[e] + recv_ref[e] for e in range(2)]
        out_ref[...] = jnp.concatenate(
            [both[e][q * cap:(q + 1) * cap] for q in range(2) for e in range(2)], axis=0).astype(BF16)

    return s_blocks


def make_near_return(cap):
    blk = 2 * cap

    def near_return(picks_ref, sfar_ref, sown_ref, srecv_ref, after_ref, stok_ref, sback, sland, b_s, b_r):
        partner = {"ep": ep_partners()[1]}
        barrier = enter(partner)
        both = [sown_ref[e] + srecv_ref[e] for e in range(2)]
        kept, away = [jnp.concatenate([both[e][q * cap:(q + 1) * cap] for e in range(2)], axis=0).astype(BF16)
                      for q in range(2)]
        sback[...] = away
        pl.semaphore_wait(barrier, 1)
        copies = [send(sback, sland.at[0], b_s.at[0], b_r.at[0], partner),
                  send(sfar_ref.at[blk:2 * blk, :], sland.at[1], b_s.at[1], b_r.at[1], partner)]
        for copy in copies:
            copy.wait()
        s_rows = jnp.concatenate([kept, sland[0], sfar_ref[0:blk, :], sland[1]], axis=0)
        stok_ref[...] = mm(picks_ref[...], s_rows, CONTRACT_FIRST).astype(BF16)

    return near_return


def router_grad(x_ref, gy_ref, prob_ref, chosen_ref, ymine_ref, ytheirs_ref, after_ref, dlog_ref, dwgt_ref, dwg, w_s, w_r):
    tp = lax.axis_index("tp")
    ep = lax.axis_index("ep")
    peers = ep_partners()
    half = ymine_ref.shape[1]
    barrier = enter(*[{"ep": peers[r]} for r in (1, 2, 3)])
    sums = [jnp.sum(gy_ref[:, pl.ds(pl.multiple_of(side * half, half), half)].astype(F32) * ref[...].astype(F32),
                    axis=1, keepdims=True) for side, ref in ((tp, ymine_ref), (1 - tp, ytheirs_ref))]
    prob, chosen = prob_ref[...], chosen_ref[...]
    gate = jnp.sum(chosen * prob, axis=1, keepdims=True)
    dlogits = ((sums[0] + sums[1]) * prob * (chosen - gate)).astype(BF16)
    dlog_ref[...] = dlogits
    dwg[ep] = mm(dlogits, x_ref[...], CONTRACT_FIRST)
    pl.semaphore_wait(barrier, 3)
    copies = [send(dwg.at[ep], dwg.at[ep], w_s.at[r - 1], w_r.at[r - 1], {"ep": peers[r]}) for r in (2, 3, 1)]
    for copy in copies:
        copy.wait()
    dwgt_ref[...] = (dwg[0] + dwg[1]) + (dwg[2] + dwg[3])


def write_out(dwgt_ref, ymine_ref, ytheirs_ref, prob_ref, chosen_ref, dlog_ref, wgt_ref, smine_ref,
              out_hbm, dwgt_hbm, dx_hbm, rgrad_ref, out_ref, dx_ref, sem):
    half = ymine_ref.shape[1]
    tp = lax.axis_index("tp")
    mine, theirs = [pl.ds(pl.multiple_of(side * half, half), half) for side in (tp, 1 - tp)]
    copies = [pltpu.make_async_copy(src, dst, sem.at[k]) for k, (src, dst) in enumerate(
        ((dwgt_ref, dwgt_hbm), (out_ref, out_hbm), (dx_ref, dx_hbm.at[:, mine])))]
    copies[0].start()
    gate = jnp.sum(chosen_ref[...] * prob_ref[...], axis=1, keepdims=True)
    out_ref[:, mine] = (gate * ymine_ref[...].astype(F32)).astype(BF16)
    out_ref[:, theirs] = (gate * ytheirs_ref[...].astype(F32)).astype(BF16)
    copies[1].start()
    dx_ref[...] = (smine_ref[...].astype(F32) + mm(dlog_ref[...], wgt_ref[:, mine])).astype(BF16)
    copies[2].start()
    rgrad_ref[...] = mm(dlog_ref[...], wgt_ref[:, theirs])
    for copy in copies:
        copy.wait()


def write_dx(rgrad_ref, stheirs_ref, dx_in, dx_hbm, dx_ref, sem):
    half = stheirs_ref.shape[1]
    dx_ref[...] = (stheirs_ref[...].astype(F32) + rgrad_ref[...]).astype(BF16)
    copy = pltpu.make_async_copy(dx_ref, dx_hbm.at[:, pl.ds(pl.multiple_of((1 - lax.axis_index("tp")) * half, half), half)], sem)
    copy.start()
    copy.wait()


FIRST_PART = 14


def solution(mesh):
    row_spec = P(("dp", "ep"), None)
    vmem = pl.BlockSpec(memory_space=pltpu.VMEM)
    hbm = pl.BlockSpec(memory_space=pltpu.HBM)

    def local_block(tokens, grad_out, w_router, w_in, w_out, expert_ids):
        n, d_model = tokens.shape
        n_experts = w_router.shape[1]
        le, _, d_ff = w_in.shape
        capacity = (6 * n + 5 * n_experts - 1) // (5 * n_experts)
        cap = -(-capacity // 8) * 8
        blk = le * cap
        rows = 4 * cap
        half = d_model // 2
        wgt = w_router.T
        idx_row = expert_ids.reshape(1, n)
        sds = jax.ShapeDtypeStruct
        dma = pltpu.SemaphoreType.DMA

        h, da, xs, dys, sfar, snear, ynear, yfar0, yfar1, picks, prob, chosen, wi_v = pl.pallas_call(
            make_front(n_experts, capacity, cap),
            out_shape=(sds((le, rows, d_ff), BF16), sds((le, rows, d_ff), BF16), sds((le, rows, d_model), BF16),
                       sds((le, rows, d_model), BF16), *[sds((le, blk, half), F32)] * 2,
                       sds((2 * blk, half), BF16), sds((blk, half), BF16), sds((blk, half), BF16),
                       sds((4 * blk, n), BF16), sds((n, n_experts), F32), sds((n, n_experts), F32),
                       sds((le, d_model, d_ff), BF16)),
            in_specs=[hbm] * 6,
            out_specs=(vmem,) * 13,
            scratch_shapes=[
                pltpu.VMEM((n, d_model), BF16), pltpu.VMEM((n, d_model), BF16), pltpu.VMEM((n_experts, d_model), BF16),
                pltpu.VMEM((1, n), jnp.int32),
                pltpu.VMEM((le, d_ff, d_model), BF16),
                pltpu.VMEM((3, le, cap, d_model), BF16), pltpu.VMEM((3, le, cap, d_model), BF16),
                pltpu.VMEM((le, rows, d_ff), F32),
                *[pltpu.VMEM((le, rows, half), F32)] * 3,
                pltpu.VMEM((blk, half), BF16), pltpu.VMEM((blk, half), BF16),
                dma((4,)), dma((3, le)), dma, dma((2, le)), dma, dma((2, le)), dma((le, 3)), dma((le, 3)), dma, dma,
            ],
            compiler_params=pltpu.CompilerParams(collective_id=0, has_side_effects=True, vmem_limit_bytes=32 * 2**20),
            name="front",
        )(*[pltpu.with_memory_space_constraint(v, pltpu.HBM) for v in (tokens, grad_out, wgt, idx_row, w_in, w_out)])

        swap = [(0, 1), (1, 0)]
        across, diagonal = [(0, 2), (2, 0), (1, 3), (3, 1)], [(0, 3), (3, 0), (1, 2), (2, 1)]
        sfar_recv = lax.ppermute(sfar, "tp", swap)
        snear_recv = lax.ppermute(snear, "tp", swap)
        yland0 = lax.ppermute(yfar0, "ep", across)
        yland1 = lax.ppermute(yfar1, "ep", diagonal)

        def local(kernel, out_shape, ins, outs, args, scratch=(), limit=8, **more):
            return pl.pallas_call(
                kernel, out_shape=out_shape, in_specs=ins, out_specs=outs, scratch_shapes=list(scratch),
                compiler_params=pltpu.CompilerParams(vmem_limit_bytes=limit * 2**20), **more)(*args)

        def weight_grad(left, right, after, pieces, size, tell, base=None):
            shape = (le, left.shape[2], right.shape[2])
            cost = pl.CostEstimate(flops=2 * rows * len(pieces) * size * shape[2],
                                   bytes_accessed=4 * len(pieces) * size * shape[2], transcendentals=0)
            return local(
                make_grad(pieces, tell), (sds(shape, F32), sds((8, 128), F32))[:1 + tell],
                [vmem] * 3 + [hbm] * (base is not None), (hbm, vmem)[:1 + tell],
                (left, right, after) + ((base,) if base is not None else ()),
                [pltpu.VMEM((len(pieces), size, shape[2]), F32), dma((len(pieces),))], 24, cost_estimate=cost,
                input_output_aliases={3: 0} if base is not None else {})

        out_size, in_size = d_ff // 8, d_model // 8
        out_pieces = [(e, c * out_size) for e in range(le) for c in range(8)]
        in_pieces = [(e, c * in_size) for e in range(le) for c in range(8)]
        dwo, sfar_own, snear_own = local(
            make_grad_out(out_pieces), (sds((le, d_ff, d_model), F32), *[sds((le, blk, half), F32)] * 2), [vmem] * 4,
            (hbm, vmem, vmem), (h, dys, da, wi_v),
            [pltpu.VMEM((len(out_pieces), out_size, d_model), F32), dma((len(out_pieces),))], 24,
            cost_estimate=pl.CostEstimate(flops=2 * rows * le * d_ff * d_model, bytes_accessed=4 * le * d_ff * d_model,
                                          transcendentals=0))
        ymine = local(y_tokens, sds((n, half), BF16), [vmem] * 5, vmem, (picks, ynear, yland0, yland1, sfar_own))
        ytheirs = lax.ppermute(ymine, "tp", swap)
        sblocks = local(make_blocks(cap), sds((2 * blk, half), BF16), [vmem] * 3, vmem, (sfar_own, sfar_recv, ymine))
        sfar_land = lax.ppermute(sblocks, "ep", across)
        dwi, done = weight_grad(xs, da, sblocks, in_pieces[:FIRST_PART], in_size, True)

        smine = pl.pallas_call(
            make_near_return(cap), out_shape=sds((n, half), BF16), in_specs=[vmem] * 5, out_specs=vmem,
            scratch_shapes=[pltpu.VMEM((blk, half), BF16), pltpu.VMEM((2, blk, half), BF16), dma((2,)), dma((2,))],
            compiler_params=pltpu.CompilerParams(collective_id=1, has_side_effects=True, vmem_limit_bytes=8 * 2**20),
            name="near_return",
        )(picks, sfar_land, snear_own, snear_recv, done)
        stheirs = lax.ppermute(smine, "tp", swap)
        dwi, done = weight_grad(xs, da, smine, in_pieces[FIRST_PART:], in_size, True, dwi)
        dlog, dwgt_v = pl.pallas_call(
            router_grad, out_shape=(sds((n, n_experts), BF16), sds((n_experts, d_model), F32)),
            in_specs=[vmem] * 7, out_specs=(vmem,) * 2,
            scratch_shapes=[pltpu.VMEM((4, n_experts, d_model), F32), dma((3,)), dma((3,))],
            compiler_params=pltpu.CompilerParams(collective_id=2, has_side_effects=True, vmem_limit_bytes=8 * 2**20),
            name="router_grad",
        )(tokens, grad_out, prob, chosen, ymine, ytheirs, done)
        tok = sds((n, d_model), BF16)
        out, dwgt, dx, rgrad = local(
            write_out, (tok, sds((n_experts, d_model), F32), tok, sds((n, half), F32)), [vmem] * 8, (hbm, hbm, hbm, vmem),
            (dwgt_v, ymine, ytheirs, prob, chosen, dlog, wgt, smine),
            [pltpu.VMEM((n, d_model), BF16), pltpu.VMEM((n, half), BF16), dma((3,))])
        dx = local(write_dx, tok, [vmem, vmem, hbm], hbm, (rgrad, stheirs, dx),
                   [pltpu.VMEM((n, half), BF16), dma], input_output_aliases={2: 0})
        return out, dx, dwi, dwo, dwgt.T

    in_specs = (row_spec, row_spec, P(None, None), P("ep", None, "tp"), P("ep", "tp", None), P(("dp", "ep")))
    out_specs = (row_spec, row_spec, P(("dp", "ep"), None, "tp"), P(("dp", "ep"), "tp", None), P("dp", None))
    return jax.shard_map(local_block, mesh=mesh, in_specs=in_specs, out_specs=out_specs, check_vma=False)
```

```python
import jax
import jax.numpy as jnp
from jax import lax
from jax.experimental import pallas as pl
from jax.experimental.pallas import tpu as pltpu
from jax.sharding import PartitionSpec as P


MESH = pl.DeviceIdType.MESH
F32, BF16 = jnp.float32, jnp.bfloat16
CONTRACT_LAST = (((1,), (1,)), ((), ()))
CONTRACT_FIRST = (((0,), (0,)), ((), ()))
GELU_C = 0.7978845608028654
GELU_K = 0.044715


def mm(a, b, dims=(((1,), (0,)), ((), ()))):
    return lax.dot_general(a, b, dims, preferred_element_type=F32)


def ep_partners():
    ep = lax.axis_index("ep")
    cx, cc = ep // 2, ep % 2
    return [ep, 2 * cx + (1 - cc), 2 * (1 - cx) + cc, 2 * (1 - cx) + (1 - cc)]


def route(idx_row, capacity, n_experts, stride):
    n = idx_row.shape[1]
    expert = lax.broadcasted_iota(jnp.int32, (n_experts, n), 0)
    hot = jnp.where(expert == idx_row, 1.0, 0.0)
    earlier = lax.broadcasted_iota(jnp.int32, (n, n), 0)
    later = lax.broadcasted_iota(jnp.int32, (n, n), 1)
    upto = jnp.where(earlier <= later, 1.0, 0.0).astype(BF16)
    count = mm(hot.astype(BF16), upto)
    position = jnp.sum(hot * count, axis=0, keepdims=True) - 1.0
    slot = jnp.where(position < capacity, idx_row.astype(F32) * stride + position, -1.0)
    return hot, slot


def pick(slot, firsts, rows):
    n = slot.shape[1]
    row = lax.broadcasted_iota(jnp.int32, (rows, n), 0)
    parts = [jnp.where((row + first).astype(F32) == slot, 1.0, 0.0) for first in firsts]
    return jnp.concatenate(parts, axis=0).astype(BF16)


def gate_of(x, wgt, hot):
    n_experts = hot.shape[0]
    logits = mm(x, wgt, CONTRACT_LAST)
    e = jnp.exp(logits - jnp.max(logits, axis=1, keepdims=True))
    prob = e / jnp.sum(e, axis=1, keepdims=True)
    eye = jnp.where(
        lax.broadcasted_iota(jnp.int32, (n_experts, n_experts), 0)
        == lax.broadcasted_iota(jnp.int32, (n_experts, n_experts), 1), 1.0, 0.0)
    chosen = mm(hot.astype(BF16), eye.astype(BF16), CONTRACT_FIRST)
    gate = jnp.sum(chosen * prob, axis=1, keepdims=True)
    return prob, chosen, gate


def enter(*devices):
    barrier = pltpu.get_barrier_semaphore()
    for device in devices:
        pl.semaphore_signal(barrier, inc=1, device_id=device, device_id_type=MESH)
    return barrier


def send(src, dst, ssem, rsem, device):
    copy = pltpu.make_async_remote_copy(
        src_ref=src, dst_ref=dst, send_sem=ssem, recv_sem=rsem, device_id=device, device_id_type=MESH)
    copy.start()
    return copy


def make_front(n_experts, capacity, cap):
    blk = 2 * cap

    def front(x_hbm, gy_hbm, wgt_hbm, idx_hbm, wi_hbm, wo_hbm,
              h_ref, da_ref, xs_ref, dys_ref, sfar_ref, snear_ref, ynear_ref, yfar0_ref, yfar1_ref,
              picks_ref, prob_ref, chosen_ref, wi,
              x_ref, gy_ref, wgt_ref, idx_ref, wo, xsend, dysend, gp,
              ypeer, yown, yrecv, yback, yland,
              in_sem, wsem, x_s, x_r, d_s, d_r, y_s, y_r, b_s, b_r):
        tp = lax.axis_index("tp")
        tp_peer = 1 - tp
        peers = ep_partners()
        half = x_ref.shape[1] // 2
        mine = pl.ds(pl.multiple_of(tp * half, half), half)
        theirs = pl.ds(pl.multiple_of(tp_peer * half, half), half)
        d_ff = wi.shape[2]
        near, far, whole = slice(0, blk), slice(blk, 2 * blk), slice(0, 2 * blk)
        small = [pltpu.make_async_copy(src, dst, in_sem.at[k]) for k, (src, dst) in enumerate(
            ((idx_hbm, idx_ref), (x_hbm, x_ref), (wgt_hbm, wgt_ref), (gy_hbm, gy_ref)))]
        for copy in small:
            copy.start()
        barrier = enter({"ep": peers[1]}, {"ep": peers[2]}, {"ep": peers[3]}, {"tp": tp_peer})
        loads = {}
        for e in range(2):
            loads["i", e] = pltpu.make_async_copy(wi_hbm.at[e], wi.at[e], wsem.at[0, e])
            for k, (name, cols) in enumerate((("theirs", theirs), ("mine", mine))):
                loads[name, e] = pltpu.make_async_copy(wo_hbm.at[e, :, cols], wo.at[e, :, cols], wsem.at[1 + k, e])
        loads["i", 0].start()

        xc, dc = {}, {}

        def dispatch(v, g, e, buf, rows_ref, ssem, rsem, made):
            first = [peers[2 * g + q] * blk + e * cap for q in range(2)]
            rows = mm(pick(slot, first, cap), v)
            for q in range(2):
                r = 2 * g + q
                part = rows[q * cap:(q + 1) * cap].astype(BF16)
                if r == 0:
                    rows_ref[e, 0:cap, :] = part
                else:
                    buf[r - 1, e] = part
            return lambda: [made.__setitem__((r, e), send(
                buf.at[r - 1, e], rows_ref.at[e, r * cap:(r + 1) * cap, :], ssem, rsem.at[g, e],
                {"ep": peers[r]})) for r in (2 * g, 2 * g + 1) if r]

        def arrived(g, e, rows_ref, rsem):
            part = rows_ref.at[e, far if g else slice(cap, blk), :]
            pltpu.make_async_copy(part, part, rsem.at[g, e]).wait()

        def dispatch_x(g, e):
            return dispatch(x_ref[...], g, e, xsend, xs_ref, x_s, x_r, xc)

        def forward(first, last, e):
            rows = slice(first * cap, last * cap)
            if first == 0:
                loads["i", e].wait()
            xg = xs_ref[e, rows, :]
            step = d_ff // 2
            for c in range(2):
                cols = slice(c * step, (c + 1) * step)
                a = mm(xg, wi[e, :, cols])
                t = jnp.tanh(GELU_C * (a + GELU_K * (a * a * a)))
                cdf = 0.5 * (1.0 + t)
                h_ref[e, rows, cols] = (a * cdf).astype(BF16)
                gp[e, rows, cols] = cdf + (0.5 * a) * (1.0 - t * t) * (GELU_C + (3.0 * GELU_C * GELU_K) * (a * a))
            if first == 0:
                loads["theirs", e].wait()
            ypeer[e, rows, :] = mm(h_ref[e, rows, :], wo[e, :, theirs])
            send(ypeer.at[e, rows, :], yrecv.at[e, rows, :], y_s, y_r.at[e, first // 2], {"tp": tp_peer})

        small[0].wait()
        hot, slot = route(idx_ref[...], capacity, n_experts, cap)
        small[1].wait()
        go = dispatch_x(0, 0)
        loads["theirs", 0].start()
        pl.semaphore_wait(barrier, 4)
        go()
        dispatch_x(1, 0)()
        dispatch_x(0, 1)()
        dispatch_x(1, 1)()
        for copy in (loads["i", 1], loads["theirs", 1], loads["mine", 0], loads["mine", 1]):
            copy.start()

        def backward(rows, e):
            dyg = dys_ref[e, rows, :]
            step = d_ff // 4
            for c in range(4):
                cols = slice(c * step, (c + 1) * step)
                dh = mm(dyg, wo[e, cols, :], CONTRACT_LAST)
                da_ref[e, rows, cols] = (dh * gp[e, rows, cols]).astype(BF16)
            dag = da_ref[e, rows, :]
            part = mm(dag, wi[e, theirs, :], CONTRACT_LAST)
            if rows is not far:
                snear_ref[e] = part[0:blk]
            if rows is not near:
                sfar_ref[e] = part[part.shape[0] - blk:]

        def y_blocks(g):
            rows = far if g else near
            for e in range(2):
                part = yrecv.at[e, rows, :]
                pltpu.make_async_copy(part, part, y_r.at[e, g]).wait()
            both = [yown[e, rows, :] + yrecv[e, rows, :] for e in range(2)]
            return [jnp.concatenate([both[e][q * cap:(q + 1) * cap] for e in range(2)], axis=0).astype(BF16) for q in range(2)]

        arrived(0, 0, xs_ref, x_r)
        forward(0, 2, 0)
        small[2].wait()
        small[3].wait()
        prob, chosen, gate = gate_of(x_ref[...], wgt_ref[...], hot)
        prob_ref[...], chosen_ref[...] = prob, chosen
        dy = (gate * gy_ref[...].astype(F32)).astype(BF16)
        for g in (1, 0):
            for e in range(2):
                dispatch(dy, g, e, dysend, dys_ref, d_s, d_r, dc)()
        arrived(0, 1, xs_ref, x_r)
        forward(0, 2, 1)
        picks_ref[...] = pick(slot, [peers[r] * blk for r in range(4)], blk)
        arrived(1, 0, xs_ref, x_r)
        forward(2, 4, 0)
        arrived(0, 0, dys_ref, d_r)
        loads["mine", 0].wait()
        backward(near, 0)
        arrived(1, 1, xs_ref, x_r)
        forward(2, 4, 1)
        loads["mine", 1].wait()
        for e in range(2):
            yown[e] = mm(h_ref[e], wo[e, :, mine])
        kept, away = y_blocks(0)
        ynear_ref[near, :] = kept
        yback[...] = away
        bc = send(yback, yland, b_s, b_r, {"ep": peers[1]})
        arrived(1, 0, dys_ref, d_r)
        backward(far, 0)
        for g in range(2):
            arrived(g, 1, dys_ref, d_r)
        backward(whole, 1)
        bc.wait()
        ynear_ref[far, :] = yland[...]
        yfar0_ref[...], yfar1_ref[...] = y_blocks(1)
        for sent, sem in ((xsend, x_s), (dysend, d_s), (ypeer, y_s)):
            pltpu.make_async_copy(sent, sent, sem).wait()

    return front


def make_grad(pieces, tell):
    def grad(left_ref, right_ref, after_ref, *rest):
        rest = rest[len(rest) - 3 - tell:]
        out_hbm, rest = rest[0], rest[1:]
        buf, sem = rest[-2:]
        size = buf.shape[1]
        copies = []
        for k, (e, row) in enumerate(pieces):
            rows = slice(row, row + size)
            buf[k] = mm(left_ref[e, :, rows], right_ref[e], CONTRACT_FIRST)
            copies.append(pltpu.make_async_copy(buf.at[k], out_hbm.at[e, rows, :], sem.at[k]))
            copies[-1].start()
        if tell:
            rest[0][...] = jnp.zeros_like(rest[0])
        for copy in copies:
            copy.wait()

    return grad


def make_grad_out(pieces):
    def grad_out(h_ref, dys_ref, da_ref, wi_ref, dwo_hbm, sfar_ref, snear_ref, buf, sem):
        size = buf.shape[1]
        blk, half = sfar_ref.shape[1:]
        copies = []
        for k, (e, row) in enumerate(pieces):
            rows = slice(row, row + size)
            buf[k] = mm(h_ref[e, :, rows], dys_ref[e], CONTRACT_FIRST)
            copies.append(pltpu.make_async_copy(buf.at[k], dwo_hbm.at[e, rows, :], sem.at[k]))
            copies[-1].start()
        mine = pl.ds(pl.multiple_of(lax.axis_index("tp") * half, half), half)
        for e in range(2):
            part = mm(da_ref[e], wi_ref[e, mine, :], CONTRACT_LAST)
            snear_ref[e] = part[0:blk]
            sfar_ref[e] = part[blk:]
        for copy in copies:
            copy.wait()

    return grad_out


def y_tokens(picks_ref, ynear_ref, yfar0_ref, yfar1_ref, after_ref, y_ref):
    rows = jnp.concatenate([ynear_ref[...], yfar0_ref[...], yfar1_ref[...]], axis=0)
    y_ref[...] = mm(picks_ref[...], rows, CONTRACT_FIRST).astype(BF16)


def make_blocks(cap):
    def s_blocks(own_ref, recv_ref, after_ref, out_ref):
        both = [own_ref[e] + recv_ref[e] for e in range(2)]
        out_ref[...] = jnp.concatenate(
            [both[e][q * cap:(q + 1) * cap] for q in range(2) for e in range(2)], axis=0).astype(BF16)

    return s_blocks


def make_near_return(cap):
    blk = 2 * cap

    def near_return(picks_ref, sfar_ref, sown_ref, srecv_ref, after_ref, stok_ref, sback, sland, b_s, b_r):
        partner = {"ep": ep_partners()[1]}
        barrier = enter(partner)
        both = [sown_ref[e] + srecv_ref[e] for e in range(2)]
        kept, away = [jnp.concatenate([both[e][q * cap:(q + 1) * cap] for e in range(2)], axis=0).astype(BF16)
                      for q in range(2)]
        sback[...] = away
        pl.semaphore_wait(barrier, 1)
        copies = [send(sback, sland.at[0], b_s.at[0], b_r.at[0], partner),
                  send(sfar_ref.at[blk:2 * blk, :], sland.at[1], b_s.at[1], b_r.at[1], partner)]
        for copy in copies:
            copy.wait()
        s_rows = jnp.concatenate([kept, sland[0], sfar_ref[0:blk, :], sland[1]], axis=0)
        stok_ref[...] = mm(picks_ref[...], s_rows, CONTRACT_FIRST).astype(BF16)

    return near_return


def router_grad(x_ref, gy_ref, prob_ref, chosen_ref, ymine_ref, ytheirs_ref, after_ref, dlog_ref, dwgt_ref, dwg, w_s, w_r):
    tp = lax.axis_index("tp")
    ep = lax.axis_index("ep")
    peers = ep_partners()
    half = ymine_ref.shape[1]
    barrier = enter(*[{"ep": peers[r]} for r in (1, 2, 3)])
    sums = [jnp.sum(gy_ref[:, pl.ds(pl.multiple_of(side * half, half), half)].astype(F32) * ref[...].astype(F32),
                    axis=1, keepdims=True) for side, ref in ((tp, ymine_ref), (1 - tp, ytheirs_ref))]
    prob, chosen = prob_ref[...], chosen_ref[...]
    gate = jnp.sum(chosen * prob, axis=1, keepdims=True)
    dlogits = ((sums[0] + sums[1]) * prob * (chosen - gate)).astype(BF16)
    dlog_ref[...] = dlogits
    dwg[ep] = mm(dlogits, x_ref[...], CONTRACT_FIRST)
    pl.semaphore_wait(barrier, 3)
    copies = [send(dwg.at[ep], dwg.at[ep], w_s.at[r - 1], w_r.at[r - 1], {"ep": peers[r]}) for r in (2, 3, 1)]
    for copy in copies:
        copy.wait()
    dwgt_ref[...] = (dwg[0] + dwg[1]) + (dwg[2] + dwg[3])


def write_out(dwgt_ref, ymine_ref, ytheirs_ref, prob_ref, chosen_ref, dlog_ref, wgt_ref, smine_ref,
              out_hbm, dwgt_hbm, dx_hbm, rgrad_ref, out_ref, dx_ref, sem):
    half = ymine_ref.shape[1]
    tp = lax.axis_index("tp")
    mine, theirs = [pl.ds(pl.multiple_of(side * half, half), half) for side in (tp, 1 - tp)]
    copies = [pltpu.make_async_copy(src, dst, sem.at[k]) for k, (src, dst) in enumerate(
        ((dwgt_ref, dwgt_hbm), (out_ref, out_hbm), (dx_ref, dx_hbm.at[:, mine])))]
    copies[0].start()
    gate = jnp.sum(chosen_ref[...] * prob_ref[...], axis=1, keepdims=True)
    out_ref[:, mine] = (gate * ymine_ref[...].astype(F32)).astype(BF16)
    out_ref[:, theirs] = (gate * ytheirs_ref[...].astype(F32)).astype(BF16)
    copies[1].start()
    dx_ref[...] = (smine_ref[...].astype(F32) + mm(dlog_ref[...], wgt_ref[:, mine])).astype(BF16)
    copies[2].start()
    rgrad_ref[...] = mm(dlog_ref[...], wgt_ref[:, theirs])
    for copy in copies:
        copy.wait()


def write_dx(rgrad_ref, stheirs_ref, dx_in, dx_hbm, dx_ref, sem):
    half = stheirs_ref.shape[1]
    dx_ref[...] = (stheirs_ref[...].astype(F32) + rgrad_ref[...]).astype(BF16)
    copy = pltpu.make_async_copy(dx_ref, dx_hbm.at[:, pl.ds(pl.multiple_of((1 - lax.axis_index("tp")) * half, half), half)], sem)
    copy.start()
    copy.wait()


FIRST_PART = 14


def solution(mesh):
    row_spec = P(("dp", "ep"), None)
    vmem = pl.BlockSpec(memory_space=pltpu.VMEM)
    hbm = pl.BlockSpec(memory_space=pltpu.HBM)

    def local_block(tokens, grad_out, w_router, w_in, w_out, expert_ids):
        n, d_model = tokens.shape
        n_experts = w_router.shape[1]
        le, _, d_ff = w_in.shape
        capacity = (6 * n + 5 * n_experts - 1) // (5 * n_experts)
        cap = -(-capacity // 8) * 8
        blk = le * cap
        rows = 4 * cap
        half = d_model // 2
        wgt = w_router.T
        idx_row = expert_ids.reshape(1, n)
        sds = jax.ShapeDtypeStruct
        dma = pltpu.SemaphoreType.DMA

        h, da, xs, dys, sfar, snear, ynear, yfar0, yfar1, picks, prob, chosen, wi_v = pl.pallas_call(
            make_front(n_experts, capacity, cap),
            out_shape=(sds((le, rows, d_ff), BF16), sds((le, rows, d_ff), BF16), sds((le, rows, d_model), BF16),
                       sds((le, rows, d_model), BF16), *[sds((le, blk, half), F32)] * 2,
                       sds((2 * blk, half), BF16), sds((blk, half), BF16), sds((blk, half), BF16),
                       sds((4 * blk, n), BF16), sds((n, n_experts), F32), sds((n, n_experts), F32),
                       sds((le, d_model, d_ff), BF16)),
            in_specs=[hbm] * 6,
            out_specs=(vmem,) * 13,
            scratch_shapes=[
                pltpu.VMEM((n, d_model), BF16), pltpu.VMEM((n, d_model), BF16), pltpu.VMEM((n_experts, d_model), BF16),
                pltpu.VMEM((1, n), jnp.int32),
                pltpu.VMEM((le, d_ff, d_model), BF16),
                pltpu.VMEM((3, le, cap, d_model), BF16), pltpu.VMEM((3, le, cap, d_model), BF16),
                pltpu.VMEM((le, rows, d_ff), F32),
                *[pltpu.VMEM((le, rows, half), F32)] * 3,
                pltpu.VMEM((blk, half), BF16), pltpu.VMEM((blk, half), BF16),
                dma((4,)), dma((3, le)), dma, dma((2, le)), dma, dma((2, le)), dma, dma((le, 2)), dma, dma,
            ],
            compiler_params=pltpu.CompilerParams(collective_id=0, has_side_effects=True, vmem_limit_bytes=32 * 2**20),
            name="front",
        )(*[pltpu.with_memory_space_constraint(v, pltpu.HBM) for v in (tokens, grad_out, wgt, idx_row, w_in, w_out)])

        swap = [(0, 1), (1, 0)]
        across, diagonal = [(0, 2), (2, 0), (1, 3), (3, 1)], [(0, 3), (3, 0), (1, 2), (2, 1)]
        sfar_recv = lax.ppermute(sfar, "tp", swap)
        snear_recv = lax.ppermute(snear, "tp", swap)
        yland0 = lax.ppermute(yfar0, "ep", across)
        yland1 = lax.ppermute(yfar1, "ep", diagonal)

        def local(kernel, out_shape, ins, outs, args, scratch=(), limit=8, **more):
            return pl.pallas_call(
                kernel, out_shape=out_shape, in_specs=ins, out_specs=outs, scratch_shapes=list(scratch),
                compiler_params=pltpu.CompilerParams(vmem_limit_bytes=limit * 2**20), **more)(*args)

        def weight_grad(left, right, after, pieces, size, tell, base=None):
            shape = (le, left.shape[2], right.shape[2])
            cost = pl.CostEstimate(flops=2 * rows * len(pieces) * size * shape[2],
                                   bytes_accessed=4 * len(pieces) * size * shape[2], transcendentals=0)
            return local(
                make_grad(pieces, tell), (sds(shape, F32), sds((8, 128), F32))[:1 + tell],
                [vmem] * 3 + [hbm] * (base is not None), (hbm, vmem)[:1 + tell],
                (left, right, after) + ((base,) if base is not None else ()),
                [pltpu.VMEM((len(pieces), size, shape[2]), F32), dma((len(pieces),))], 24, cost_estimate=cost,
                input_output_aliases={3: 0} if base is not None else {})

        out_size, in_size = d_ff // 8, d_model // 8
        out_pieces = [(e, c * out_size) for e in range(le) for c in range(8)]
        in_pieces = [(e, c * in_size) for e in range(le) for c in range(8)]
        dwo, sfar_own, snear_own = local(
            make_grad_out(out_pieces), (sds((le, d_ff, d_model), F32), *[sds((le, blk, half), F32)] * 2), [vmem] * 4,
            (hbm, vmem, vmem), (h, dys, da, wi_v),
            [pltpu.VMEM((len(out_pieces), out_size, d_model), F32), dma((len(out_pieces),))], 24,
            cost_estimate=pl.CostEstimate(flops=2 * rows * le * d_ff * d_model, bytes_accessed=4 * le * d_ff * d_model,
                                          transcendentals=0))
        ymine = local(y_tokens, sds((n, half), BF16), [vmem] * 5, vmem, (picks, ynear, yland0, yland1, sfar_own))
        ytheirs = lax.ppermute(ymine, "tp", swap)
        sblocks = local(make_blocks(cap), sds((2 * blk, half), BF16), [vmem] * 3, vmem, (sfar_own, sfar_recv, ymine))
        sfar_land = lax.ppermute(sblocks, "ep", across)
        dwi, done = weight_grad(xs, da, sblocks, in_pieces[:FIRST_PART], in_size, True)

        smine = pl.pallas_call(
            make_near_return(cap), out_shape=sds((n, half), BF16), in_specs=[vmem] * 5, out_specs=vmem,
            scratch_shapes=[pltpu.VMEM((blk, half), BF16), pltpu.VMEM((2, blk, half), BF16), dma((2,)), dma((2,))],
            compiler_params=pltpu.CompilerParams(collective_id=1, has_side_effects=True, vmem_limit_bytes=8 * 2**20),
            name="near_return",
        )(picks, sfar_land, snear_own, snear_recv, done)
        stheirs = lax.ppermute(smine, "tp", swap)
        dwi, done = weight_grad(xs, da, smine, in_pieces[FIRST_PART:], in_size, True, dwi)
        dlog, dwgt_v = pl.pallas_call(
            router_grad, out_shape=(sds((n, n_experts), BF16), sds((n_experts, d_model), F32)),
            in_specs=[vmem] * 7, out_specs=(vmem,) * 2,
            scratch_shapes=[pltpu.VMEM((4, n_experts, d_model), F32), dma((3,)), dma((3,))],
            compiler_params=pltpu.CompilerParams(collective_id=2, has_side_effects=True, vmem_limit_bytes=8 * 2**20),
            name="router_grad",
        )(tokens, grad_out, prob, chosen, ymine, ytheirs, done)
        tok = sds((n, d_model), BF16)
        out, dwgt, dx, rgrad = local(
            write_out, (tok, sds((n_experts, d_model), F32), tok, sds((n, half), F32)), [vmem] * 8, (hbm, hbm, hbm, vmem),
            (dwgt_v, ymine, ytheirs, prob, chosen, dlog, wgt, smine),
            [pltpu.VMEM((n, d_model), BF16), pltpu.VMEM((n, half), BF16), dma((3,))])
        dx = local(write_dx, tok, [vmem, vmem, hbm], hbm, (rgrad, stheirs, dx),
                   [pltpu.VMEM((n, half), BF16), dma], input_output_aliases={2: 0})
        return out, dx, dwi, dwo, dwgt.T

    in_specs = (row_spec, row_spec, P(None, None), P("ep", None, "tp"), P("ep", "tp", None), P(("dp", "ep")))
    out_specs = (row_spec, row_spec, P(("dp", "ep"), None, "tp"), P(("dp", "ep"), "tp", None), P("dp", None))
    return jax.shard_map(local_block, mesh=mesh, in_specs=in_specs, out_specs=out_specs, check_vma=False)
```

```python
import jax
import jax.numpy as jnp
from jax import lax
from jax.experimental import pallas as pl
from jax.experimental.pallas import tpu as pltpu
from jax.sharding import PartitionSpec as P


MESH = pl.DeviceIdType.MESH
F32, BF16 = jnp.float32, jnp.bfloat16
CONTRACT_LAST = (((1,), (1,)), ((), ()))
CONTRACT_FIRST = (((0,), (0,)), ((), ()))
GELU_C = 0.7978845608028654
GELU_K = 0.044715


def mm(a, b, dims=(((1,), (0,)), ((), ()))):
    return lax.dot_general(a, b, dims, preferred_element_type=F32)


def ep_partners():
    ep = lax.axis_index("ep")
    cx, cc = ep // 2, ep % 2
    return [ep, 2 * cx + (1 - cc), 2 * (1 - cx) + cc, 2 * (1 - cx) + (1 - cc)]


def route(idx_row, capacity, n_experts, stride):
    n = idx_row.shape[1]
    expert = lax.broadcasted_iota(jnp.int32, (n_experts, n), 0)
    hot = jnp.where(expert == idx_row, 1.0, 0.0)
    earlier = lax.broadcasted_iota(jnp.int32, (n, n), 0)
    later = lax.broadcasted_iota(jnp.int32, (n, n), 1)
    upto = jnp.where(earlier <= later, 1.0, 0.0).astype(BF16)
    count = mm(hot.astype(BF16), upto)
    position = jnp.sum(hot * count, axis=0, keepdims=True) - 1.0
    slot = jnp.where(position < capacity, idx_row.astype(F32) * stride + position, -1.0)
    return hot, slot


def pick(slot, firsts, rows):
    n = slot.shape[1]
    row = lax.broadcasted_iota(jnp.int32, (rows, n), 0)
    parts = [jnp.where((row + first).astype(F32) == slot, 1.0, 0.0) for first in firsts]
    return jnp.concatenate(parts, axis=0).astype(BF16)


def gate_of(x, wgt, hot):
    n_experts = hot.shape[0]
    logits = mm(x, wgt, CONTRACT_LAST)
    e = jnp.exp(logits - jnp.max(logits, axis=1, keepdims=True))
    prob = e / jnp.sum(e, axis=1, keepdims=True)
    eye = jnp.where(
        lax.broadcasted_iota(jnp.int32, (n_experts, n_experts), 0)
        == lax.broadcasted_iota(jnp.int32, (n_experts, n_experts), 1), 1.0, 0.0)
    chosen = mm(hot.astype(BF16), eye.astype(BF16), CONTRACT_FIRST)
    gate = jnp.sum(chosen * prob, axis=1, keepdims=True)
    return prob, chosen, gate


def enter(*devices):
    barrier = pltpu.get_barrier_semaphore()
    for device in devices:
        pl.semaphore_signal(barrier, inc=1, device_id=device, device_id_type=MESH)
    return barrier


def send(src, dst, ssem, rsem, device):
    copy = pltpu.make_async_remote_copy(
        src_ref=src, dst_ref=dst, send_sem=ssem, recv_sem=rsem, device_id=device, device_id_type=MESH)
    copy.start()
    return copy


def make_front(n_experts, capacity, cap):
    blk = 2 * cap

    def front(x_hbm, gy_hbm, wgt_hbm, idx_hbm, wi_hbm, wo_hbm,
              h_ref, da_ref, xs_ref, dys_ref, sfar_ref, snear_ref, ynear_ref, yfar0_ref, yfar1_ref,
              picks_ref, prob_ref, chosen_ref, wi,
              x_ref, gy_ref, wgt_ref, idx_ref, wo, xsend, dysend, gp,
              ypeer, yown, yrecv, yback, yland,
              in_sem, wsem, x_s, x_r, d_s, d_r, y_s, y_r, b_s, b_r):
        tp = lax.axis_index("tp")
        tp_peer = 1 - tp
        peers = ep_partners()
        half = x_ref.shape[1] // 2
        mine = pl.ds(pl.multiple_of(tp * half, half), half)
        theirs = pl.ds(pl.multiple_of(tp_peer * half, half), half)
        d_ff = wi.shape[2]
        near, far, whole = slice(0, blk), slice(blk, 2 * blk), slice(0, 2 * blk)
        small = [pltpu.make_async_copy(src, dst, in_sem.at[k]) for k, (src, dst) in enumerate(
            ((idx_hbm, idx_ref), (x_hbm, x_ref), (wgt_hbm, wgt_ref), (gy_hbm, gy_ref)))]
        small[0].start()
        small[1].start()
        barrier = enter({"ep": peers[1]}, {"ep": peers[2]}, {"ep": peers[3]}, {"tp": tp_peer})
        loads = {}
        for e in range(2):
            loads["i", e] = pltpu.make_async_copy(wi_hbm.at[e], wi.at[e], wsem.at[0, e])
            for k, (name, cols) in enumerate((("theirs", theirs), ("mine", mine))):
                loads[name, e] = pltpu.make_async_copy(wo_hbm.at[e, :, cols], wo.at[e, :, cols], wsem.at[1 + k, e])
        loads["i", 0].start()

        xc, dc = {}, {}

        def dispatch(v, g, e, buf, rows_ref, ssem, rsem, made):
            first = [peers[2 * g + q] * blk + e * cap for q in range(2)]
            rows = mm(pick(slot, first, cap), v)
            for q in range(2):
                r = 2 * g + q
                part = rows[q * cap:(q + 1) * cap].astype(BF16)
                if r == 0:
                    rows_ref[e, 0:cap, :] = part
                else:
                    buf[r - 1, e] = part
            return lambda: [made.__setitem__((r, e), send(
                buf.at[r - 1, e], rows_ref.at[e, r * cap:(r + 1) * cap, :], ssem, rsem.at[g, e],
                {"ep": peers[r]})) for r in (2 * g, 2 * g + 1) if r]

        def arrived(g, e, rows_ref, rsem):
            part = rows_ref.at[e, far if g else slice(cap, blk), :]
            pltpu.make_async_copy(part, part, rsem.at[g, e]).wait()

        def dispatch_x(g, e):
            return dispatch(x_ref[...], g, e, xsend, xs_ref, x_s, x_r, xc)

        def forward(first, last, e):
            rows = slice(first * cap, last * cap)
            if first == 0:
                loads["i", e].wait()
            xg = xs_ref[e, rows, :]
            step = d_ff // 2
            for c in range(2):
                cols = slice(c * step, (c + 1) * step)
                a = mm(xg, wi[e, :, cols])
                t = jnp.tanh(GELU_C * (a + GELU_K * (a * a * a)))
                cdf = 0.5 * (1.0 + t)
                h_ref[e, rows, cols] = (a * cdf).astype(BF16)
                gp[e, rows, cols] = cdf + (0.5 * a) * (1.0 - t * t) * (GELU_C + (3.0 * GELU_C * GELU_K) * (a * a))
            if first == 0:
                loads["theirs", e].wait()
            ypeer[e, rows, :] = mm(h_ref[e, rows, :], wo[e, :, theirs])
            send(ypeer.at[e, rows, :], yrecv.at[e, rows, :], y_s, y_r.at[e, first // 2], {"tp": tp_peer})

        small[0].wait()
        hot, slot = route(idx_ref[...], capacity, n_experts, cap)
        small[1].wait()
        go = dispatch_x(0, 0)
        loads["theirs", 0].start()
        pl.semaphore_wait(barrier, 4)
        go()
        dispatch_x(1, 0)()
        dispatch_x(0, 1)()
        dispatch_x(1, 1)()
        small[2].start()
        small[3].start()

        def backward(rows, e):
            dyg = dys_ref[e, rows, :]
            step = d_ff // 4
            for c in range(4):
                cols = slice(c * step, (c + 1) * step)
                dh = mm(dyg, wo[e, cols, :], CONTRACT_LAST)
                da_ref[e, rows, cols] = (dh * gp[e, rows, cols]).astype(BF16)
            dag = da_ref[e, rows, :]
            part = mm(dag, wi[e, theirs, :], CONTRACT_LAST)
            if rows is not far:
                snear_ref[e] = part[0:blk]
            if rows is not near:
                sfar_ref[e] = part[part.shape[0] - blk:]

        def y_blocks(g):
            rows = far if g else near
            for e in range(2):
                part = yrecv.at[e, rows, :]
                pltpu.make_async_copy(part, part, y_r.at[e, g]).wait()
            both = [yown[e, rows, :] + yrecv[e, rows, :] for e in range(2)]
            return [jnp.concatenate([both[e][q * cap:(q + 1) * cap] for e in range(2)], axis=0).astype(BF16) for q in range(2)]

        arrived(0, 0, xs_ref, x_r)
        loads["i", 1].start()
        forward(0, 2, 0)
        for copy in (loads["theirs", 1], loads["mine", 0], loads["mine", 1]):
            copy.start()
        small[2].wait()
        small[3].wait()
        prob, chosen, gate = gate_of(x_ref[...], wgt_ref[...], hot)
        prob_ref[...], chosen_ref[...] = prob, chosen
        dy = (gate * gy_ref[...].astype(F32)).astype(BF16)
        for g in (1, 0):
            for e in range(2):
                dispatch(dy, g, e, dysend, dys_ref, d_s, d_r, dc)()
        arrived(0, 1, xs_ref, x_r)
        forward(0, 2, 1)
        picks_ref[...] = pick(slot, [peers[r] * blk for r in range(4)], blk)
        arrived(1, 0, xs_ref, x_r)
        forward(2, 4, 0)
        arrived(0, 0, dys_ref, d_r)
        loads["mine", 0].wait()
        backward(near, 0)
        arrived(1, 1, xs_ref, x_r)
        forward(2, 4, 1)
        loads["mine", 1].wait()
        for e in range(2):
            yown[e] = mm(h_ref[e], wo[e, :, mine])
        kept, away = y_blocks(0)
        ynear_ref[near, :] = kept
        yback[...] = away
        bc = send(yback, yland, b_s, b_r, {"ep": peers[1]})
        arrived(1, 0, dys_ref, d_r)
        backward(far, 0)
        for g in range(2):
            arrived(g, 1, dys_ref, d_r)
        backward(whole, 1)
        bc.wait()
        ynear_ref[far, :] = yland[...]
        yfar0_ref[...], yfar1_ref[...] = y_blocks(1)
        for sent, sem in ((xsend, x_s), (dysend, d_s), (ypeer, y_s)):
            pltpu.make_async_copy(sent, sent, sem).wait()

    return front


def make_grad(pieces, tell):
    def grad(left_ref, right_ref, after_ref, *rest):
        rest = rest[len(rest) - 3 - tell:]
        out_hbm, rest = rest[0], rest[1:]
        buf, sem = rest[-2:]
        size = buf.shape[1]
        copies = []
        for k, (e, row) in enumerate(pieces):
            rows = slice(row, row + size)
            buf[k] = mm(left_ref[e, :, rows], right_ref[e], CONTRACT_FIRST)
            copies.append(pltpu.make_async_copy(buf.at[k], out_hbm.at[e, rows, :], sem.at[k]))
            copies[-1].start()
        if tell:
            rest[0][...] = jnp.zeros_like(rest[0])
        for copy in copies:
            copy.wait()

    return grad


def make_grad_out(pieces):
    def grad_out(h_ref, dys_ref, da_ref, wi_ref, dwo_hbm, sfar_ref, snear_ref, buf, sem):
        size = buf.shape[1]
        blk, half = sfar_ref.shape[1:]
        copies = []
        for k, (e, row) in enumerate(pieces):
            rows = slice(row, row + size)
            buf[k] = mm(h_ref[e, :, rows], dys_ref[e], CONTRACT_FIRST)
            copies.append(pltpu.make_async_copy(buf.at[k], dwo_hbm.at[e, rows, :], sem.at[k]))
            copies[-1].start()
        mine = pl.ds(pl.multiple_of(lax.axis_index("tp") * half, half), half)
        for e in range(2):
            part = mm(da_ref[e], wi_ref[e, mine, :], CONTRACT_LAST)
            snear_ref[e] = part[0:blk]
            sfar_ref[e] = part[blk:]
        for copy in copies:
            copy.wait()

    return grad_out


def y_tokens(picks_ref, ynear_ref, yfar0_ref, yfar1_ref, after_ref, y_ref):
    rows = jnp.concatenate([ynear_ref[...], yfar0_ref[...], yfar1_ref[...]], axis=0)
    y_ref[...] = mm(picks_ref[...], rows, CONTRACT_FIRST).astype(BF16)


def make_blocks(cap):
    def s_blocks(own_ref, recv_ref, after_ref, out_ref):
        both = [own_ref[e] + recv_ref[e] for e in range(2)]
        out_ref[...] = jnp.concatenate(
            [both[e][q * cap:(q + 1) * cap] for q in range(2) for e in range(2)], axis=0).astype(BF16)

    return s_blocks


def make_near_return(cap):
    blk = 2 * cap

    def near_return(picks_ref, sfar_ref, sown_ref, srecv_ref, after_ref, stok_ref, sback, sland, b_s, b_r):
        partner = {"ep": ep_partners()[1]}
        barrier = enter(partner)
        both = [sown_ref[e] + srecv_ref[e] for e in range(2)]
        kept, away = [jnp.concatenate([both[e][q * cap:(q + 1) * cap] for e in range(2)], axis=0).astype(BF16)
                      for q in range(2)]
        sback[...] = away
        pl.semaphore_wait(barrier, 1)
        copies = [send(sback, sland.at[0], b_s.at[0], b_r.at[0], partner),
                  send(sfar_ref.at[blk:2 * blk, :], sland.at[1], b_s.at[1], b_r.at[1], partner)]
        for copy in copies:
            copy.wait()
        s_rows = jnp.concatenate([kept, sland[0], sfar_ref[0:blk, :], sland[1]], axis=0)
        stok_ref[...] = mm(picks_ref[...], s_rows, CONTRACT_FIRST).astype(BF16)

    return near_return


def router_grad(x_ref, gy_ref, prob_ref, chosen_ref, ymine_ref, ytheirs_ref, after_ref, dlog_ref, dwgt_ref, dwg, w_s, w_r):
    tp = lax.axis_index("tp")
    ep = lax.axis_index("ep")
    peers = ep_partners()
    half = ymine_ref.shape[1]
    barrier = enter(*[{"ep": peers[r]} for r in (1, 2, 3)])
    sums = [jnp.sum(gy_ref[:, pl.ds(pl.multiple_of(side * half, half), half)].astype(F32) * ref[...].astype(F32),
                    axis=1, keepdims=True) for side, ref in ((tp, ymine_ref), (1 - tp, ytheirs_ref))]
    prob, chosen = prob_ref[...], chosen_ref[...]
    gate = jnp.sum(chosen * prob, axis=1, keepdims=True)
    dlogits = ((sums[0] + sums[1]) * prob * (chosen - gate)).astype(BF16)
    dlog_ref[...] = dlogits
    dwg[ep] = mm(dlogits, x_ref[...], CONTRACT_FIRST)
    pl.semaphore_wait(barrier, 3)
    copies = [send(dwg.at[ep], dwg.at[ep], w_s.at[r - 1], w_r.at[r - 1], {"ep": peers[r]}) for r in (2, 3, 1)]
    for copy in copies:
        copy.wait()
    dwgt_ref[...] = (dwg[0] + dwg[1]) + (dwg[2] + dwg[3])


def write_out(dwgt_ref, ymine_ref, ytheirs_ref, prob_ref, chosen_ref, dlog_ref, wgt_ref, smine_ref,
              out_hbm, dwgt_hbm, dx_hbm, rgrad_ref, out_ref, dx_ref, sem):
    half = ymine_ref.shape[1]
    tp = lax.axis_index("tp")
    mine, theirs = [pl.ds(pl.multiple_of(side * half, half), half) for side in (tp, 1 - tp)]
    copies = [pltpu.make_async_copy(src, dst, sem.at[k]) for k, (src, dst) in enumerate(
        ((dwgt_ref, dwgt_hbm), (out_ref, out_hbm), (dx_ref, dx_hbm.at[:, mine])))]
    copies[0].start()
    gate = jnp.sum(chosen_ref[...] * prob_ref[...], axis=1, keepdims=True)
    out_ref[:, mine] = (gate * ymine_ref[...].astype(F32)).astype(BF16)
    out_ref[:, theirs] = (gate * ytheirs_ref[...].astype(F32)).astype(BF16)
    copies[1].start()
    dx_ref[...] = (smine_ref[...].astype(F32) + mm(dlog_ref[...], wgt_ref[:, mine])).astype(BF16)
    copies[2].start()
    rgrad_ref[...] = mm(dlog_ref[...], wgt_ref[:, theirs])
    for copy in copies:
        copy.wait()


def write_dx(rgrad_ref, stheirs_ref, dx_in, dx_hbm, dx_ref, sem):
    half = stheirs_ref.shape[1]
    dx_ref[...] = (stheirs_ref[...].astype(F32) + rgrad_ref[...]).astype(BF16)
    copy = pltpu.make_async_copy(dx_ref, dx_hbm.at[:, pl.ds(pl.multiple_of((1 - lax.axis_index("tp")) * half, half), half)], sem)
    copy.start()
    copy.wait()


FIRST_PART = 14


def solution(mesh):
    row_spec = P(("dp", "ep"), None)
    vmem = pl.BlockSpec(memory_space=pltpu.VMEM)
    hbm = pl.BlockSpec(memory_space=pltpu.HBM)

    def local_block(tokens, grad_out, w_router, w_in, w_out, expert_ids):
        n, d_model = tokens.shape
        n_experts = w_router.shape[1]
        le, _, d_ff = w_in.shape
        capacity = (6 * n + 5 * n_experts - 1) // (5 * n_experts)
        cap = -(-capacity // 8) * 8
        blk = le * cap
        rows = 4 * cap
        half = d_model // 2
        wgt = w_router.T
        idx_row = expert_ids.reshape(1, n)
        sds = jax.ShapeDtypeStruct
        dma = pltpu.SemaphoreType.DMA

        h, da, xs, dys, sfar, snear, ynear, yfar0, yfar1, picks, prob, chosen, wi_v = pl.pallas_call(
            make_front(n_experts, capacity, cap),
            out_shape=(sds((le, rows, d_ff), BF16), sds((le, rows, d_ff), BF16), sds((le, rows, d_model), BF16),
                       sds((le, rows, d_model), BF16), *[sds((le, blk, half), F32)] * 2,
                       sds((2 * blk, half), BF16), sds((blk, half), BF16), sds((blk, half), BF16),
                       sds((4 * blk, n), BF16), sds((n, n_experts), F32), sds((n, n_experts), F32),
                       sds((le, d_model, d_ff), BF16)),
            in_specs=[hbm] * 6,
            out_specs=(vmem,) * 13,
            scratch_shapes=[
                pltpu.VMEM((n, d_model), BF16), pltpu.VMEM((n, d_model), BF16), pltpu.VMEM((n_experts, d_model), BF16),
                pltpu.VMEM((1, n), jnp.int32),
                pltpu.VMEM((le, d_ff, d_model), BF16),
                pltpu.VMEM((3, le, cap, d_model), BF16), pltpu.VMEM((3, le, cap, d_model), BF16),
                pltpu.VMEM((le, rows, d_ff), F32),
                *[pltpu.VMEM((le, rows, half), F32)] * 3,
                pltpu.VMEM((blk, half), BF16), pltpu.VMEM((blk, half), BF16),
                dma((4,)), dma((3, le)), dma, dma((2, le)), dma, dma((2, le)), dma, dma((le, 2)), dma, dma,
            ],
            compiler_params=pltpu.CompilerParams(collective_id=0, has_side_effects=True, vmem_limit_bytes=32 * 2**20),
            name="front",
        )(*[pltpu.with_memory_space_constraint(v, pltpu.HBM) for v in (tokens, grad_out, wgt, idx_row, w_in, w_out)])

        swap = [(0, 1), (1, 0)]
        across, diagonal = [(0, 2), (2, 0), (1, 3), (3, 1)], [(0, 3), (3, 0), (1, 2), (2, 1)]
        sfar_recv = lax.ppermute(sfar, "tp", swap)
        snear_recv = lax.ppermute(snear, "tp", swap)
        yland0 = lax.ppermute(yfar0, "ep", across)
        yland1 = lax.ppermute(yfar1, "ep", diagonal)

        def local(kernel, out_shape, ins, outs, args, scratch=(), limit=8, **more):
            return pl.pallas_call(
                kernel, out_shape=out_shape, in_specs=ins, out_specs=outs, scratch_shapes=list(scratch),
                compiler_params=pltpu.CompilerParams(vmem_limit_bytes=limit * 2**20), **more)(*args)

        def weight_grad(left, right, after, pieces, size, tell, base=None):
            shape = (le, left.shape[2], right.shape[2])
            cost = pl.CostEstimate(flops=2 * rows * len(pieces) * size * shape[2],
                                   bytes_accessed=4 * len(pieces) * size * shape[2], transcendentals=0)
            return local(
                make_grad(pieces, tell), (sds(shape, F32), sds((8, 128), F32))[:1 + tell],
                [vmem] * 3 + [hbm] * (base is not None), (hbm, vmem)[:1 + tell],
                (left, right, after) + ((base,) if base is not None else ()),
                [pltpu.VMEM((len(pieces), size, shape[2]), F32), dma((len(pieces),))], 24, cost_estimate=cost,
                input_output_aliases={3: 0} if base is not None else {})

        out_size, in_size = d_ff // 8, d_model // 8
        out_pieces = [(e, c * out_size) for e in range(le) for c in range(8)]
        in_pieces = [(e, c * in_size) for e in range(le) for c in range(8)]
        dwo, sfar_own, snear_own = local(
            make_grad_out(out_pieces), (sds((le, d_ff, d_model), F32), *[sds((le, blk, half), F32)] * 2), [vmem] * 4,
            (hbm, vmem, vmem), (h, dys, da, wi_v),
            [pltpu.VMEM((len(out_pieces), out_size, d_model), F32), dma((len(out_pieces),))], 24,
            cost_estimate=pl.CostEstimate(flops=2 * rows * le * d_ff * d_model, bytes_accessed=4 * le * d_ff * d_model,
                                          transcendentals=0))
        ymine = local(y_tokens, sds((n, half), BF16), [vmem] * 5, vmem, (picks, ynear, yland0, yland1, sfar_own))
        ytheirs = lax.ppermute(ymine, "tp", swap)
        sblocks = local(make_blocks(cap), sds((2 * blk, half), BF16), [vmem] * 3, vmem, (sfar_own, sfar_recv, ymine))
        sfar_land = lax.ppermute(sblocks, "ep", across)
        dwi, done = weight_grad(xs, da, sblocks, in_pieces[:FIRST_PART], in_size, True)

        smine = pl.pallas_call(
            make_near_return(cap), out_shape=sds((n, half), BF16), in_specs=[vmem] * 5, out_specs=vmem,
            scratch_shapes=[pltpu.VMEM((blk, half), BF16), pltpu.VMEM((2, blk, half), BF16), dma((2,)), dma((2,))],
            compiler_params=pltpu.CompilerParams(collective_id=1, has_side_effects=True, vmem_limit_bytes=8 * 2**20),
            name="near_return",
        )(picks, sfar_land, snear_own, snear_recv, done)
        stheirs = lax.ppermute(smine, "tp", swap)
        dwi, done = weight_grad(xs, da, smine, in_pieces[FIRST_PART:], in_size, True, dwi)
        dlog, dwgt_v = pl.pallas_call(
            router_grad, out_shape=(sds((n, n_experts), BF16), sds((n_experts, d_model), F32)),
            in_specs=[vmem] * 7, out_specs=(vmem,) * 2,
            scratch_shapes=[pltpu.VMEM((4, n_experts, d_model), F32), dma((3,)), dma((3,))],
            compiler_params=pltpu.CompilerParams(collective_id=2, has_side_effects=True, vmem_limit_bytes=8 * 2**20),
            name="router_grad",
        )(tokens, grad_out, prob, chosen, ymine, ytheirs, done)
        tok = sds((n, d_model), BF16)
        out, dwgt, dx, rgrad = local(
            write_out, (tok, sds((n_experts, d_model), F32), tok, sds((n, half), F32)), [vmem] * 8, (hbm, hbm, hbm, vmem),
            (dwgt_v, ymine, ytheirs, prob, chosen, dlog, wgt, smine),
            [pltpu.VMEM((n, d_model), BF16), pltpu.VMEM((n, half), BF16), dma((3,))])
        dx = local(write_dx, tok, [vmem, vmem, hbm], hbm, (rgrad, stheirs, dx),
                   [pltpu.VMEM((n, half), BF16), dma], input_output_aliases={2: 0})
        return out, dx, dwi, dwo, dwgt.T

    in_specs = (row_spec, row_spec, P(None, None), P("ep", None, "tp"), P("ep", "tp", None), P(("dp", "ep")))
    out_specs = (row_spec, row_spec, P(("dp", "ep"), None, "tp"), P(("dp", "ep"), "tp", None), P("dp", None))
    return jax.shard_map(local_block, mesh=mesh, in_specs=in_specs, out_specs=out_specs, check_vma=False)
```
